256 devices in a mesh: gx: 8 (over z), gy: 4 (over y), gz: 8 (over x, core).
Axes of the slice: x: 4, y: 4, z: 8, core: 2. Of those that a mesh axis runs over, the one named last changes fastest.
Arguments:
- point_data: float32 [1, 6, 131072], P(None, None, ('gx', 'gy', 'gz')), may hold values from -1 to 1
- neighbours: int32 [1, 64, 64, 64, 32], P(None, 'gx', 'gy', 'gz'), may hold values from 0 to 131071, as said below
- counts: int32 [1, 64, 64, 64], P(None, 'gx', 'gy', 'gz'), may hold values from 1 to 32, as said below
- kernel_in: bfloat16 [6, 80], replicated, may hold values from -2.5 to 2.5
- kernel_mid: bfloat16 [80, 80], replicated, may hold values from -0.625 to 0.625
- kernel_out: bfloat16 [80, 64], replicated, may hold values from -0.625 to 0.625
- spectral: bfloat16 [2, 16, 16, 16, 64, 64], P(None, 'gz', 'gx', 'gy'), may hold values from -48 to 48
- skip_weight: bfloat16 [64, 64], replicated, may hold values from -0.75 to 0.75
Outputs:
- latent_out: float32 [1, 64, 64, 64, 64], P(None, 'gx', 'gy', 'gz')
The draws below stay inside these ranges and needn't reach their ends.
Inputs may be any that keep to these rules, and one draw needn't show every extreme that they name: `neighbours`: points are owned by location: point j of a geometry belongs to the device at position j // 512 in the order gx, gy, gz. Every neighbour of a node is owned by the node's own device or by a device whose gx, gy and gz indices each differ from it by at most one. Slots s >= counts of the node are padding that names some point all the same. `counts`: on every device some node of every geometry has all 32 slots valid.
All inputs are finite; a program needn't handle non-finite values.
Results may differ from the reference program's by a relative error of at most 0.02.
Values may be sent and summed in bfloat16 or wider, within the bound.
A program may use at most 64 MiB of HBM per device.

```python
import math
import jax
import jax.numpy as jnp
from jax import lax

GRID = 64
CH = 64
MODES = 16
KH = 80
NB = 32
PT_DEV = 512
GEOMS = 1
LX = 8
LY = 16
LZ = 8
POINTS = 131072


def draw_neighbours(key, part):
    code_key, slot_key = jax.random.split(jax.random.fold_in(key, 11))
    shape = (GEOMS, GRID, GRID, GRID, NB)
    codes = jax.random.randint(code_key, shape, 0, 54)
    codes = jnp.where(codes >= 27, 13, codes)
    count_x = GRID // LX
    count_y = GRID // LY
    count_z = GRID // LZ
    home_x = (jnp.arange(GRID, dtype=jnp.int32) // LX).reshape(1, GRID, 1, 1, 1)
    home_y = (jnp.arange(GRID, dtype=jnp.int32) // LY).reshape(1, 1, GRID, 1, 1)
    home_z = (jnp.arange(GRID, dtype=jnp.int32) // LZ).reshape(1, 1, 1, GRID, 1)
    owner_x = jnp.clip(home_x + codes // 9 - 1, 0, count_x - 1)
    owner_y = jnp.clip(home_y + codes // 3 % 3 - 1, 0, count_y - 1)
    owner_z = jnp.clip(home_z + codes % 3 - 1, 0, count_z - 1)
    slots = jax.random.randint(slot_key, shape, 0, PT_DEV)
    return (((owner_x * count_y + owner_y) * count_z + owner_z) * PT_DEV + slots).astype(jnp.int32)


def draw_counts(key, part):
    values = jax.random.randint(jax.random.fold_in(key, 12), (GEOMS, GRID, GRID, GRID), 1, NB + 1)
    return values.at[:, ::LX, ::LY, ::LZ].set(NB).astype(jnp.int32)


def block_scale(own_key, extent, cuts, low, high):
    def one(dim, parts):
        draws = jax.random.uniform(jax.random.fold_in(jax.random.fold_in(own_key, 6), dim), (parts,), jnp.float32, low / len(cuts), high / len(cuts))
        return jnp.repeat(jnp.exp(draws), extent[dim] // parts).reshape((-1,) + (1,) * (len(extent) - dim - 1))

    level = one(*cuts[0])
    for cut in cuts[1:]:
        level = level * one(*cut)
    return level


def normal_values(key, shape, deviation, most, pieces=(), kind=jnp.bfloat16):
    drawn = deviation * jax.random.normal(key, shape, jnp.float32)
    if pieces:
        drawn = drawn * block_scale(key, shape, pieces, -0.22, 0.18)
    return jnp.clip(drawn, -most, most).astype(kind)


def setup_inputs(seed: int = 0) -> dict:
    key_list = jax.random.split(jax.random.key(seed), 9)
    return {
        "point_data": jnp.clip(jax.random.uniform(key_list[0], (GEOMS, 6, POINTS), jnp.float32, -1.0, 1.0) * block_scale(key_list[0], (GEOMS, 6, POINTS), ((2, 256),), -0.4, 0.0), -1.0, 1.0),
        "neighbours": draw_neighbours(jax.random.fold_in(key_list[8], 71), 0),
        "counts": draw_counts(jax.random.fold_in(key_list[8], 71), 0),
        "kernel_in": normal_values(key_list[3], (6, KH), 6 ** -0.5, 2.5),
        "kernel_mid": normal_values(key_list[4], (KH, KH), KH ** -0.5, 0.625),
        "kernel_out": normal_values(key_list[5], (KH, CH), KH ** -0.5, 0.625),
        "spectral": normal_values(key_list[6], (2, MODES, MODES, MODES, CH, CH), 8.0, 48.0, ((1, 8), (2, 8), (3, 4))),
        "skip_weight": normal_values(key_list[7], (CH, CH), CH ** -0.5, 0.75),
    }


HIGHEST = lax.Precision.HIGHEST
NORM_FLOOR = 1.0

def tables(length, keep_count, centred):
    position = jnp.arange(length, dtype=jnp.int32)
    frequency = jnp.arange(keep_count, dtype=jnp.int32)
    if centred:
        frequency = jnp.where(frequency < keep_count // 2, frequency, frequency + length - keep_count)
    phases = frequency[:, None] * position[None, :] % length
    angles = phases.astype(jnp.float32) * (2.0 * math.pi / length)
    return (jnp.cos(angles), jnp.sin(angles))

def third_weights(cos_table, sin_table, length):
    factor = jnp.where(jnp.arange(cos_table.shape[0]) == 0, 1.0, 2.0).astype(jnp.float32)[:, None] / length ** 3
    return (cos_table * factor, sin_table * factor)

def contract(pattern, operand, table):
    return jnp.einsum(pattern, operand, table, precision=HIGHEST)

def forward_real(values, cos_table, sin_table, pattern):
    return (contract(pattern, values, cos_table), -contract(pattern, values, sin_table))

def forward_complex(real_part, imag_part, cos_table, sin_table, pattern):
    new_real = contract(pattern, real_part, cos_table) + contract(pattern, imag_part, sin_table)
    new_imag = contract(pattern, imag_part, cos_table) - contract(pattern, real_part, sin_table)
    return (new_real, new_imag)

def inverse_complex(real_part, imag_part, cos_table, sin_table, pattern):
    new_real = contract(pattern, real_part, cos_table) - contract(pattern, imag_part, sin_table)
    new_imag = contract(pattern, real_part, sin_table) + contract(pattern, imag_part, cos_table)
    return (new_real, new_imag)

def inverse_real(real_part, imag_part, cos_table, sin_table, pattern):
    return contract(pattern, real_part, cos_table) - contract(pattern, imag_part, sin_table)

def kernel_mean(pair, valid, kernel_in, kernel_mid, kernel_out):
    hidden_one = jax.nn.gelu(jnp.dot(kernel_in.T, pair, preferred_element_type=jnp.float32), approximate=True).astype(jnp.bfloat16)
    hidden_two = jax.nn.gelu(jnp.dot(kernel_mid.T, hidden_one, preferred_element_type=jnp.float32), approximate=True).astype(jnp.bfloat16)
    values = jnp.dot(kernel_out.T, hidden_two, preferred_element_type=jnp.float32)
    values = values.reshape(values.shape[0], -1, NB)
    slots = jnp.arange(NB, dtype=jnp.int32)
    used = (slots[None, :] < valid[:, None]).astype(jnp.float32)
    total = lax.optimization_barrier(jnp.sum(values * used[None], axis=2))
    return (total / valid.astype(jnp.float32)[None]).T.astype(jnp.bfloat16)

def reference(point_data, neighbours, counts, kernel_in, kernel_mid, kernel_out, spectral, skip_weight):
    centres = (jnp.arange(GRID, dtype=jnp.int32).astype(jnp.float32) + 0.5) / GRID
    row_y = jnp.broadcast_to(centres[:, None, None], (GRID, GRID, NB)).reshape(1, -1)
    row_z = jnp.broadcast_to(centres[None, :, None], (GRID, GRID, NB)).reshape(1, -1)

    def one_slab(step):
        geometry = step // GRID
        slab = step % GRID
        points = lax.dynamic_index_in_dim(point_data, geometry, 0, keepdims=False)
        near = lax.dynamic_index_in_dim(lax.dynamic_index_in_dim(neighbours, geometry, 0, keepdims=False), slab, 0, keepdims=False).reshape(-1)
        valid = lax.dynamic_index_in_dim(lax.dynamic_index_in_dim(counts, geometry, 0, keepdims=False), slab, 0, keepdims=False).reshape(-1)
        picked = jnp.take(points, near, axis=1)
        row_x = (slab.astype(jnp.float32) + 0.5) / GRID
        pair = jnp.concatenate([picked[0:1] - row_x, picked[1:2] - row_y, picked[2:3] - row_z, picked[3:6]], axis=0).astype(jnp.bfloat16)
        return kernel_mean(pair, valid, kernel_in, kernel_mid, kernel_out)
    latent = lax.map(one_slab, jnp.arange(GEOMS * GRID, dtype=jnp.int32)).reshape(GEOMS, GRID, GRID, GRID, CH)
    cos_centred, sin_centred = tables(GRID, MODES, True)
    cos_third, sin_third = tables(GRID, MODES, False)
    back_cos, back_sin = third_weights(cos_third, sin_third, GRID)
    latent_wide = latent.astype(jnp.float32)
    real_part, imag_part = forward_real(latent_wide, cos_third, sin_third, 'gxyzc,kz->gxykc')
    real_part, imag_part = forward_complex(real_part, imag_part, cos_centred, sin_centred, 'gxykc,jy->gxjkc')
    real_part, imag_part = forward_complex(real_part, imag_part, cos_centred, sin_centred, 'gxjkc,ix->gijkc')
    spec_real = lax.optimization_barrier(real_part.astype(jnp.bfloat16)).astype(jnp.float32)
    spec_imag = lax.optimization_barrier(imag_part.astype(jnp.bfloat16)).astype(jnp.float32)
    mix_real = spectral[0].astype(jnp.float32)
    mix_imag = spectral[1].astype(jnp.float32)
    mixed_real = jnp.einsum('gijkc,ijkco->gijko', spec_real, mix_real) - jnp.einsum('gijkc,ijkco->gijko', spec_imag, mix_imag)
    mixed_imag = jnp.einsum('gijkc,ijkco->gijko', spec_real, mix_imag) + jnp.einsum('gijkc,ijkco->gijko', spec_imag, mix_real)
    mixed_real = lax.optimization_barrier(mixed_real.astype(jnp.bfloat16)).astype(jnp.float32)
    mixed_imag = lax.optimization_barrier(mixed_imag.astype(jnp.bfloat16)).astype(jnp.float32)
    real_part, imag_part = inverse_complex(mixed_real, mixed_imag, cos_centred, sin_centred, 'gijkc,ix->gxjkc')
    real_part, imag_part = inverse_complex(real_part, imag_part, cos_centred, sin_centred, 'gxjkc,jy->gxykc')
    branch = inverse_real(real_part, imag_part, back_cos, back_sin, 'gxykc,kz->gxyzc')
    cells_total = float(GRID ** 3)
    mean = lax.optimization_barrier(jnp.sum(branch, axis=(1, 2, 3))) / cells_total
    centred_branch = branch - mean[:, None, None, None, :]
    variance = lax.optimization_barrier(jnp.sum(centred_branch * centred_branch, axis=(1, 2, 3))) / cells_total
    skip = jnp.dot(latent.reshape(-1, CH), skip_weight, preferred_element_type=jnp.float32).reshape(GEOMS, GRID, GRID, GRID, CH)
    normed = centred_branch / jnp.sqrt(variance + NORM_FLOOR)[:, None, None, None, :]
    return jax.nn.gelu(normed + skip, approximate=True)
```

```python
import functools
import math

import jax
import jax.numpy as jnp
import ml_dtypes
import numpy as np
from jax import lax
from jax.experimental import pallas as pl
from jax.experimental.pallas import tpu as pltpu
from jax.sharding import PartitionSpec as P

GRID = 64
MODES = 16
NB = 32
NORM_FLOOR = 1.0
GX, GY, GZ = 8, 4, 8
F32 = jnp.float32
BF16 = jnp.bfloat16
MESH = pl.DeviceIdType.MESH


def extended(cells, sides, width):
    for axis, dim in sides:
        count = lax.axis_size(axis)
        ends = count - 1
        head = lax.slice_in_dim(cells, 0, width, axis=dim)
        tail = lax.slice_in_dim(cells, cells.shape[dim] - width, cells.shape[dim], axis=dim)
        cells = jnp.concatenate(
            [
                lax.ppermute(tail, axis, [(i, (i + 1) % count) for i in range(ends)]),
                cells,
                lax.ppermute(head, axis, [((i + 1) % count, i) for i in range(ends)]),
            ],
            axis=dim,
        )
    return cells


def gelu(v):
    inner = v * (0.7978845608028654 + 0.035677408136300125 * (v * v))
    half = 0.5 * v
    return half + half * jnp.tanh(inner)


def encoder_kernel(
    blocks, slots_ref, blocks_ref, counts_ref, centres_ref, table_ref, first_ref, mid_ref, last_ref, out_ref, total
):
    width = slots_ref.shape[1]
    per_device = table_ref.shape[1]
    rest_rows = table_ref.shape[0] - 8 * blocks
    slot_ids = lax.broadcasted_iota(jnp.int32, (per_device, width), 0).astype(jnp.int16)
    rest_ids = lax.broadcasted_iota(jnp.int32, (rest_rows, width), 0)
    rows = lax.broadcasted_iota(jnp.int32, (8, width), 0)
    counts = counts_ref[...]
    centres = centres_ref[...]
    total[...] = jnp.zeros_like(total)

    def step(s, carry):
        slot = jnp.broadcast_to(slots_ref[pl.ds(s, 1), :], (16, width)).astype(jnp.int16)
        slot = jnp.concatenate([slot] * (per_device // 16), axis=0)
        hot = jnp.where(slot_ids == slot, jnp.bfloat16(1), jnp.bfloat16(0))
        found = jnp.dot(table_ref[...], hot, preferred_element_type=jnp.float32)
        block = blocks_ref[pl.ds(s, 1), :]
        wide = jnp.broadcast_to(block, (8, width))
        picked = found[0:8]
        for b in range(1, blocks):
            picked = jnp.where(wide == b, found[8 * b : 8 * b + 8], picked)
        third = jnp.sum(jnp.where(rest_ids == block, found[8 * blocks :], 0.0), axis=0, keepdims=True)
        place = picked + pltpu.roll(picked, 4, 0) - centres
        pair = jnp.where(rows < 3, place, jnp.where(rows == 4, third, picked)).astype(jnp.bfloat16)
        hidden = gelu(jnp.dot(first_ref[...], pair, preferred_element_type=jnp.float32))
        hidden = gelu(
            jnp.dot(mid_ref[...], hidden.astype(jnp.bfloat16), preferred_element_type=jnp.float32)
        )
        hidden = hidden.astype(jnp.bfloat16).astype(jnp.float32)
        total[...] += jnp.where(s < counts, hidden, 0.0)
        return carry

    lax.fori_loop(0, slots_ref.shape[0], step, 0, unroll=8)
    mean = total[...] / counts.astype(jnp.float32)
    upper = mean.astype(jnp.bfloat16)
    lower = (mean - upper.astype(jnp.float32)).astype(jnp.bfloat16)
    last = last_ref[...]
    values = jnp.dot(last, upper, preferred_element_type=jnp.float32) + jnp.dot(
        last, lower, preferred_element_type=jnp.float32
    )
    tiles = width // 128
    parts = [values[:, 128 * t : 128 * t + 128].reshape(8, 8, 128) for t in range(tiles)]
    out_ref[...] = jnp.stack(parts, axis=1).reshape(8, 8 * tiles, 128).astype(jnp.bfloat16)


def encode(slots, block_ids, counts, centres, table, first, mid, last):
    nodes = slots.shape[1]
    width = min(512, nodes)
    tile = lambda rows: pl.BlockSpec((rows, width), lambda i: (0, i))
    whole = lambda array: pl.BlockSpec(array.shape, lambda i: (0, 0))
    return pl.pallas_call(
        functools.partial(encoder_kernel, 27),
        grid=(nodes // width,),
        out_shape=jax.ShapeDtypeStruct((8, nodes // 16, 128), jnp.bfloat16),
        in_specs=[tile(NB), tile(NB), tile(1), tile(8), whole(table), whole(first), whole(mid), whole(last)],
        out_specs=pl.BlockSpec((8, width // 16, 128), lambda i: (0, i, 0)),
        scratch_shapes=[pltpu.VMEM((mid.shape[0], width), jnp.float32)],
    )(slots, block_ids, counts, centres, table, first, mid, last)


def packed_table(table):
    upper = table.astype(jnp.bfloat16)
    lower = (table - upper.astype(jnp.float32)).astype(jnp.bfloat16)
    main = jnp.concatenate([upper[0:3], upper[3:4], lower[0:3], upper[4:5]], axis=0)
    main = jnp.transpose(main, (1, 0, 2)).reshape(-1, table.shape[2])
    rows = jnp.concatenate([main, upper[5]], axis=0)
    return jnp.pad(rows, ((0, -rows.shape[0] % 128), (0, 0)))


def halves(values):
    upper = values.astype(np.float32).astype(ml_dtypes.bfloat16)
    lower = (values - upper.astype(np.float64)).astype(np.float32).astype(ml_dtypes.bfloat16)
    return np.stack([upper, lower])


def turn(frequency, position):
    angle = 2.0 * math.pi * ((frequency * position) % GRID) / GRID
    return np.cos(angle), np.sin(angle)


def centred(index):
    return np.where(index < MODES // 2, index, index - MODES)


def complex_block(cos, sin):
    return np.stack([np.stack([cos, sin], -1), np.stack([-sin, cos], -1)], -2)


@functools.lru_cache(None)
def third_table():
    cos, sin = turn(np.arange(16)[:, None], np.arange(64)[None, :])
    parts = np.stack([cos, -sin]).reshape(2, 4, 4, 64).transpose(1, 0, 2, 3)
    full = np.einsum("arkz,cd->arkczd", parts, np.eye(8))
    return full.reshape(256, 512)


@functools.lru_cache(None)
def second_table():
    j = np.arange(16)
    cos, sin = turn(centred(j)[:, None], np.arange(64)[None, :])
    both = complex_block(cos, sin).reshape(8, 2, 4, 16, 2, 2)
    full = np.einsum("gleyab,xw->lgaxebwy", both, np.eye(8))
    return full.reshape(2, 128, 1024)


@functools.lru_cache(None)
def first_table():
    i = np.arange(16)
    cos, sin = turn(centred(i)[:, None], np.arange(64)[None, :])
    both = complex_block(cos, sin).reshape(8, 2, 8, 8, 2, 2)
    full = np.einsum("hltxab,gf->tlghafbx", both, np.eye(8))
    return full.reshape(8, 2, 128, 128)


@functools.lru_cache(None)
def pair_table():
    out = np.zeros((4, 8, 8, 2, 8, 8, 2))
    for il in range(2):
        for jl in range(2):
            for h in range(8):
                for g in range(8):
                    i, j = 2 * h + il, 2 * g + jl
                    if i == 8 or j == 8:
                        continue
                    ni, nj = (16 - i) % 16, (16 - j) % 16
                    assert ni % 2 == il and nj % 2 == jl
                    for a in range(2):
                        out[2 * il + jl, g, h, a, nj // 2, ni // 2, a] = 1.0 - 2.0 * a
    return out.reshape(4, 128, 128)


def dotf(a, b):
    return jnp.dot(a, b, preferred_element_type=F32)


def dott(a, b):
    return lax.dot_general(a, b, (((1,), (1,)), ((), ())), preferred_element_type=F32)


def split(values):
    upper = values.astype(BF16)
    return upper, (values - upper.astype(F32)).astype(BF16)


def spectral_kernel(
    latent_ref, skip_ref, weight_ref, third_ref, back_ref, second_ref, first_ref, firstt_ref, pair_ref,
    out_ref,
    r1, z_msg, r2, s_msg, r3, t_msg, r4, mixing, n_msg, r5, g_msg, r6, f_msg, v_msg, r7, rv, b_msg, r8, skip,
    send, recv,
):
    me_x = lax.axis_index("gx")
    me_y = lax.axis_index("gy")
    me_z = lax.axis_index("gz")
    mine = {"gx": me_x, "gy": me_y, "gz": me_z}
    sizes = {"gx": GX, "gy": GY, "gz": GZ}

    barrier = pltpu.get_barrier_semaphore()
    total = 0
    for axis in ("gz", "gy", "gx"):
        for o in range(1, sizes[axis]):
            pl.semaphore_signal(
                barrier, inc=1, device_id={axis: lax.rem(mine[axis] + o, sizes[axis])}, device_id_type=MESH
            )
            total += 1
    pl.semaphore_wait(barrier, total)

    def start(stage, axis, source, target):
        copies = []
        size = sizes[axis]
        for o in range(1, size):
            peer = lax.rem(mine[axis] + o, size)
            copy = pltpu.make_async_remote_copy(
                src_ref=source(peer),
                dst_ref=target.at[mine[axis]],
                send_sem=send.at[stage, o],
                recv_sem=recv.at[stage, o],
                device_id={axis: peer},
                device_id_type=MESH,
            )
            copy.start()
            copies.append(copy)
        return copies

    def finish(copies):
        for copy in copies:
            copy.wait_recv()

    waiting = []

    first = start(0, "gz", lambda p: latent_ref.at[p], r1)
    waiting += first
    r1[me_z] = latent_ref[me_z]
    for z in range(8):
        here = latent_ref[:, 8 * z : 8 * z + 8, :].reshape(64, 128)
        skip[z] = dotf(skip_ref[...], here)
    for s in range(8):
        halves_of = []
        for b in range(2):
            halves_of.append(weight_ref[b, :, 8 * s : 8 * s + 8, :].astype(F32).reshape(128, 64))
        mixing[128 * s : 128 * s + 128, :] = jnp.concatenate(halves_of, axis=1).astype(BF16)
    finish(first)
    values = r1[...].reshape(512, 128)
    spectrum = dotf(third_ref[0], values) + dotf(third_ref[1], values)
    z_msg[...] = spectrum.astype(BF16).reshape(4, 64, 128)

    second = start(1, "gy", lambda p: z_msg.at[p], r2)
    waiting += second
    r2[me_y] = z_msg[me_y]
    finish(second)
    wide = jnp.concatenate(
        [r2[e, 32 * b : 32 * b + 32, :] for e in range(4) for b in range(2)], axis=1
    )
    rows = jnp.concatenate(
        [dott(second_ref[0, l], wide) + dott(second_ref[1, l], wide) for l in range(2)], axis=1
    )
    upper, lower = split(rows)
    partial = jnp.concatenate(
        [
            dotf(first_ref[0, l], upper) + dotf(first_ref[0, l], lower) + dotf(first_ref[1, l], upper)
            for l in range(2)
        ],
        axis=1,
    )
    s_msg[...] = partial.astype(BF16).reshape(8, 16, 128)

    third = start(2, "gx", lambda p: s_msg.at[p], r3)
    waiting += third
    r3[me_x] = s_msg[me_x]
    finish(third)
    modes = jnp.sum(r3[...].astype(F32), axis=0)
    for h in range(8):
        t_msg[h] = modes[2 * h : 2 * h + 2, :]

    fourth = start(3, "gz", lambda p: t_msg.at[p], r4)
    waiting += fourth
    r4[me_z] = t_msg[me_z]
    finish(fourth)
    mode_rows = lax.broadcasted_iota(jnp.int32, (16, 128), 0)
    lanes16 = lax.broadcasted_iota(jnp.int32, (16, 128), 1)
    own = mode_rows == lanes16 // 8
    expanded = jnp.concatenate(
        [
            jnp.concatenate(
                [
                    jnp.where(own, jnp.broadcast_to(r4[s, a : a + 1, :], (16, 128)), 0.0)
                    for s in range(8)
                ],
                axis=1,
            )
            for a in range(2)
        ],
        axis=0,
    ).astype(BF16)
    product = dotf(expanded, mixing[...])
    sign = jnp.where(lanes16 < 64, -1.0, 1.0)
    mixed = product[0:16] + pltpu.roll(product[16:32], 64, 1) * sign
    first_place = (me_x + me_y + me_z) == 0
    mixed = jnp.where((mode_rows == 0) & first_place, 0.0, mixed)
    spread = jnp.where(own, 1.0, 0.0).astype(BF16)
    tall = lax.dot_general(
        mixed.astype(BF16), spread, (((0,), (0,)), ((), ())), preferred_element_type=F32
    )
    tall_rows = lax.broadcasted_iota(jnp.int32, (128, 128), 0)
    tall_lanes = lax.broadcasted_iota(jnp.int32, (128, 128), 1)
    tall = jnp.where(tall_rows % 8 == tall_lanes % 8, tall, 0.0).astype(BF16)
    gather = (mode_rows % 2) * 8 + mode_rows // 2 == lanes16 // 8
    turned = dotf(jnp.where(gather, 1.0, 0.0).astype(BF16), tall)
    for h in range(8):
        n_msg[h] = turned[2 * h : 2 * h + 2, :]

    fifth = start(4, "gz", lambda p: n_msg.at[p], r5)
    waiting += fifth
    r5[me_z] = n_msg[me_z]
    finish(fifth)
    g_msg[...] = jnp.concatenate([r5[h] for h in range(8)], axis=0).astype(BF16)

    sixth = start(5, "gx", lambda p: g_msg, r6)
    waiting += sixth
    r6[me_x] = g_msg[...]
    finish(sixth)
    field = r6[...].reshape(128, 128)
    along = (
        dotf(firstt_ref[0, 0], field[:, 0:64])
        + dotf(firstt_ref[1, 0], field[:, 0:64])
        + dotf(firstt_ref[0, 1], field[:, 64:128])
        + dotf(firstt_ref[1, 1], field[:, 64:128])
    )
    upper, lower = split(along.T)
    plane = (
        dotf(upper[0:32], second_ref[0, 0])
        + dotf(lower[0:32], second_ref[0, 0])
        + dotf(upper[0:32], second_ref[1, 0])
        + dotf(upper[32:64], second_ref[0, 1])
        + dotf(lower[32:64], second_ref[0, 1])
        + dotf(upper[32:64], second_ref[1, 1])
    )
    zero_rows = lax.broadcasted_iota(jnp.int32, (32, 1024), 0)
    scale = 1.0 / GRID**3
    plane = plane * jnp.where((zero_rows < 8) & (me_y == 0), scale, 2.0 * scale)
    for e in range(4):
        for b in range(2):
            part = plane[:, (2 * e + b) * 128 : (2 * e + b + 1) * 128]
            f_msg[e, 32 * b : 32 * b + 32, :] = part.astype(BF16)

    seventh = start(6, "gy", lambda p: f_msg.at[p], r7)
    waiting += seventh
    r7[me_y] = f_msg[me_y]
    wide_field = field.astype(F32)
    lane_group = tall_lanes // 32
    paired = jnp.zeros((128, 128), F32)
    for p in range(4):
        paired = jnp.where(lane_group == p, dotf(pair_ref[p], field), paired)
    low = ((tall_lanes // 8) % 4 == 0) & (me_y == 0)
    power = jnp.where(low, 0.5 * wide_field * (wide_field + paired), 2.0 * wide_field * wide_field)
    power = jnp.sum(power, axis=0, keepdims=True)
    power = power + pltpu.roll(power, 64, 1)
    power = power + pltpu.roll(power, 32, 1)
    power = power + pltpu.roll(power, 16, 1)
    power = power + pltpu.roll(power, 8, 1)
    tall_power = jnp.broadcast_to(power, (128, 128)).T
    v_msg[...] = tall_power[0:8, :] * (scale * scale)
    eighth = start(7, "gy", lambda p: v_msg, rv)
    waiting += eighth
    rv[me_y] = v_msg[...]
    finish(seventh)
    grid_part = r7[...].reshape(256, 128)
    branch = dotf(back_ref[0], grid_part) + dotf(back_ref[1], grid_part)
    finish(eighth)
    variance = (rv[0] + rv[1]) + (rv[2] + rv[3])
    inverse = 1.0 / jnp.sqrt(variance + NORM_FLOOR)
    branch = branch.reshape(64, 8, 128) * inverse[None]
    b_msg[...] = branch.reshape(8, 64, 128).astype(BF16)

    ninth = start(8, "gz", lambda p: b_msg.at[p], r8)
    waiting += ninth
    r8[me_z] = b_msg[me_z]
    finish(ninth)
    for z in range(8):
        normed = r8[:, 8 * z : 8 * z + 8, :].astype(F32).reshape(64, 128)
        out_ref[:, z, :] = gelu(normed + skip[z]).T
    for copy in waiting:
        copy.wait_send()


def spectral_layer(latent, skip_t, weight, third, back, second, first, firstt, pair):
    vmem = pl.BlockSpec(memory_space=pltpu.VMEM)
    return pl.pallas_call(
        spectral_kernel,
        out_shape=jax.ShapeDtypeStruct((128, 8, 64), F32),
        in_specs=[vmem] * 9,
        out_specs=vmem,
        scratch_shapes=[
            pltpu.VMEM((8, 64, 128), BF16),
            pltpu.VMEM((4, 64, 128), BF16),
            pltpu.VMEM((4, 64, 128), BF16),
            pltpu.VMEM((8, 16, 128), BF16),
            pltpu.VMEM((8, 16, 128), BF16),
            pltpu.VMEM((8, 2, 128), F32),
            pltpu.VMEM((8, 2, 128), F32),
            pltpu.VMEM((1024, 128), BF16),
            pltpu.VMEM((8, 2, 128), F32),
            pltpu.VMEM((8, 2, 128), F32),
            pltpu.VMEM((16, 128), BF16),
            pltpu.VMEM((8, 16, 128), BF16),
            pltpu.VMEM((4, 64, 128), BF16),
            pltpu.VMEM((8, 128), F32),
            pltpu.VMEM((4, 64, 128), BF16),
            pltpu.VMEM((4, 8, 128), F32),
            pltpu.VMEM((8, 64, 128), BF16),
            pltpu.VMEM((8, 64, 128), BF16),
            pltpu.VMEM((8, 64, 128), F32),
            pltpu.SemaphoreType.DMA((9, 8)),
            pltpu.SemaphoreType.DMA((9, 8)),
        ],
        compiler_params=pltpu.CompilerParams(collective_id=0, has_side_effects=True),
    )(latent, skip_t, weight, third, back, second, first, firstt, pair)


def body(point_data, neighbours, counts, kernel_in, kernel_mid, kernel_out, spectral, skip_weight):
    count_y = lax.axis_size("gy")
    count_z = lax.axis_size("gz")
    place_x = lax.axis_index("gx")
    place_y = lax.axis_index("gy")
    place_z = lax.axis_index("gz")
    geometry_count, cells_x, cells_y, cells_z = neighbours.shape[0:4]
    per_device = point_data.shape[2]
    beside_all = extended(point_data[None, None, None], (("gx", 0), ("gy", 1), ("gz", 2)), 1)
    table = jnp.transpose(beside_all, (3, 4, 0, 1, 2, 5)).reshape(
        geometry_count, point_data.shape[1], 27, per_device
    )
    turned = jnp.transpose(neighbours[0], (3, 2, 0, 1)).reshape(NB, -1)
    owner = turned // per_device
    offset_z = owner % count_z - place_z + 1
    offset_y = owner // count_z % count_y - place_y + 1
    offset_x = owner // (count_z * count_y) - place_x + 1
    block_index = (offset_x * 3 + offset_y) * 3 + offset_z
    slot_index = turned % per_device
    centre_y = (
        (place_y * cells_y + jnp.arange(cells_y, dtype=jnp.int32)).astype(jnp.float32) + 0.5
    ) / GRID
    centre_z = (
        (place_z * cells_z + jnp.arange(cells_z, dtype=jnp.int32)).astype(jnp.float32) + 0.5
    ) / GRID
    centre_x = (
        (place_x * cells_x + jnp.arange(cells_x, dtype=jnp.int32)).astype(jnp.float32) + 0.5
    ) / GRID
    shape = (cells_z, cells_x, cells_y)
    centres = jnp.stack(
        [
            jnp.broadcast_to(centre_x[None, :, None], shape).reshape(-1),
            jnp.broadcast_to(centre_y[None, None, :], shape).reshape(-1),
            jnp.broadcast_to(centre_z[:, None, None], shape).reshape(-1),
        ]
    )
    centres = jnp.pad(centres, ((0, 5), (0, 0)))
    first = jnp.stack(
        [kernel_in[0], kernel_in[1], kernel_in[2], kernel_in[3], kernel_in[5]]
        + [jnp.zeros_like(kernel_in[0])] * 2
        + [kernel_in[4]],
        axis=1,
    )
    latent = encode(
        slot_index,
        block_index,
        jnp.transpose(counts[0], (2, 0, 1)).reshape(1, -1),
        centres,
        packed_table(table[0]),
        first,
        kernel_mid.T,
        kernel_out.T,
    )
    third = third_table()
    by_place = first_table()
    pick = lambda values: lax.dynamic_index_in_dim(jnp.asarray(halves(values)), place_x, 1, keepdims=False)
    out = spectral_layer(
        latent,
        skip_weight.T,
        spectral.reshape(2, 16, 64, 64),
        jnp.asarray(halves(third)),
        jnp.asarray(halves(third.T)),
        jnp.asarray(halves(second_table())),
        pick(by_place),
        pick(np.swapaxes(by_place, 2, 3)),
        jnp.asarray(pair_table().astype(ml_dtypes.bfloat16)),
    )
    return out.reshape(1, cells_x, cells_y, cells_z, -1)


def solution(mesh):
    in_specs = (
        P(None, None, ("gx", "gy", "gz")),
        P(None, "gx", "gy", "gz", None),
        P(None, "gx", "gy", "gz"),
        P(),
        P(),
        P(),
        P(None, "gz", "gx", "gy", None, None),
        P(),
    )
    out_specs = P(None, "gx", "gy", "gz", None)
    return jax.shard_map(body, mesh=mesh, in_specs=in_specs, out_specs=out_specs, check_vma=False)
```

```python
import functools
import math

import jax
import jax.numpy as jnp
import ml_dtypes
import numpy as np
from jax import lax
from jax.experimental import pallas as pl
from jax.experimental.pallas import tpu as pltpu
from jax.sharding import PartitionSpec as P

GRID = 64
MODES = 16
NB = 32
NORM_FLOOR = 1.0
GX, GY, GZ = 8, 4, 8
F32 = jnp.float32
BF16 = jnp.bfloat16
MESH = pl.DeviceIdType.MESH


def gelu(v):
    inner = v * (0.7978845608028654 + 0.035677408136300125 * (v * v))
    half = 0.5 * v
    return half + half * jnp.tanh(inner)


def twice_gelu(v):
    return v + v * jnp.tanh(v * (0.7978845608028654 + 0.035677408136300125 * (v * v)))


SLOTS = 4
ROWS = 256
OFFSETS = [(dx, dy, dz) for dx in (-1, 0, 1) for dy in (-1, 0, 1) for dz in (-1, 0, 1)]


def halo_kernel(
    points_ref, near_ref, counts_ref, table_ref, slots_ref, blocks_ref, info_ref, rank_ref,
    main, rest, send, recv,
):
    me_x = lax.axis_index("gx")
    me_y = lax.axis_index("gy")
    me_z = lax.axis_index("gz")

    def device(offset):
        dx, dy, dz = offset
        return {
            "gx": lax.rem(me_x + dx + GX, GX),
            "gy": lax.rem(me_y + dy + GY, GY),
            "gz": lax.rem(me_z + dz + GZ, GZ),
        }

    barrier = pltpu.get_barrier_semaphore()
    peers = [o for o in OFFSETS if o != (0, 0, 0)]
    for offset in peers:
        pl.semaphore_signal(barrier, inc=1, device_id=device(offset), device_id_type=MESH)

    points = points_ref[...]
    upper = points.astype(BF16).astype(F32)
    lower = points - upper
    main[13] = jnp.concatenate([upper[0:4], lower[0:3], upper[4:5]], axis=0).astype(BF16)
    rest[13] = upper[5:6]
    pl.semaphore_wait(barrier, len(peers))
    copies = []
    for n, offset in enumerate(peers):
        slot = 26 - OFFSETS.index(offset)
        for k, buffer in enumerate((main, rest)):
            copy = pltpu.make_async_remote_copy(
                src_ref=buffer.at[13],
                dst_ref=buffer.at[slot],
                send_sem=send.at[k, n],
                recv_sem=recv.at[k, n],
                device_id=device(offset),
                device_id_type=MESH,
            )
            copy.start()
            copies.append(copy)

    lane = lax.broadcasted_iota(jnp.int32, (1, 1024), 1)
    counts = counts_ref[...].astype(F32)
    key = counts * 1024.0 + (1023 - lane).astype(F32)
    ones = jnp.ones((8, 128), BF16)
    rank = jnp.zeros((8, 1024), F32)
    for m in range(8):
        tall = jnp.broadcast_to(key[:, 128 * m : 128 * m + 128], (128, 128)).T
        ahead = jnp.concatenate(
            [
                jnp.where(tall > key[:, 128 * n : 128 * n + 128], 1.0, 0.0).astype(BF16)
                for n in range(8)
            ],
            axis=1,
        )
        rank = rank + jnp.dot(ones, ahead, preferred_element_type=F32)
    rank_ref[...] = rank
    near = jnp.concatenate(
        [near_ref[pl.ds(z, 128, stride=8), :].astype(F32).T for z in range(8)], axis=1
    ).astype(jnp.int32)
    owner = near >> 9
    part = near & 511
    block = ((((owner >> 5) - me_x + 1) * 3) + ((owner >> 3) & 3) - me_y + 1) * 3 + (owner & 7) - me_z + 1
    code = jnp.clip(block, 0, 26) * 2 + (part >> 8)
    place_y = (me_y * 16 + (lane & 15)).astype(F32)
    place_x = (me_x * 8 + ((lane >> 4) & 7)).astype(F32)
    place_z = (me_z * 8 + (lane >> 7)).astype(F32)
    centres = [-(place + 0.5) / GRID for place in (place_x, place_y, place_z)]
    rows = jnp.concatenate(
        [(part & 255).astype(F32), code.astype(F32), counts] + centres + [jnp.zeros((12, 1024), F32)], axis=0
    ).astype(BF16)
    order = lax.broadcasted_iota(jnp.int32, (128, 1024), 0).astype(F32)
    wide_rank = rank[0:1]
    for t in range(8):
        moved = jnp.where(order + 128.0 * t == wide_rank, 1.0, 0.0).astype(BF16)
        moved = lax.dot_general(rows, moved, (((1,), (1,)), ((), ())), preferred_element_type=F32)
        code = moved[32:64].astype(jnp.int32)
        slots_ref[t] = moved[0:32].astype(jnp.int32) + 256 * (code & 1)
        blocks_ref[t] = code >> 1
        info_ref[t] = moved[64:72]

    for copy in copies:
        copy.wait_recv()
    table_ref[0:216, :] = main[...].astype(F32).reshape(216, 512).astype(BF16)
    tail = jnp.concatenate([rest[b] for b in range(27)] + [jnp.zeros((13, 512), F32)], axis=0)
    table_ref[216:256, :] = tail.astype(BF16)
    for copy in copies:
        copy.wait_send()


def halo(points, near, counts):
    vmem = pl.BlockSpec(memory_space=pltpu.VMEM)
    return pl.pallas_call(
        halo_kernel,
        out_shape=[
            jax.ShapeDtypeStruct((ROWS, 512), BF16),
            jax.ShapeDtypeStruct((8, NB, 128), jnp.int32),
            jax.ShapeDtypeStruct((8, NB, 128), jnp.int32),
            jax.ShapeDtypeStruct((8, 8, 128), F32),
            jax.ShapeDtypeStruct((8, 1024), F32),
        ],
        in_specs=[vmem] * 3,
        out_specs=[vmem] * 5,
        scratch_shapes=[
            pltpu.VMEM((27, 8, 512), BF16),
            pltpu.VMEM((27, 1, 512), F32),
            pltpu.SemaphoreType.DMA((2, 26)),
            pltpu.SemaphoreType.DMA((2, 26)),
        ],
        compiler_params=pltpu.CompilerParams(collective_id=1, has_side_effects=True),
    )(points, near, counts)


def encoder_kernel(
    table_ref, slots_ref, blocks_ref, info_ref, rank_ref, in_ref, mid_ref, last_ref, out_ref,
    first_scr, mid_scr, last_scr, ordered,
):
    column = lax.broadcasted_iota(jnp.int32, (6, ROWS), 1)
    feature = lax.broadcasted_iota(jnp.int32, (6, ROWS), 0)
    value = column % 8
    wanted = jnp.where(value < 4, value, jnp.where(value == 7, 4, value - 4))
    wanted = jnp.where(column >= 243, column - 243, jnp.where(column >= 216, 5, wanted))
    chosen = jnp.where((feature == wanted) & (column < 246), 1.0, 0.0).astype(BF16)
    turn = (((0,), (0,)), ((), ()))
    first_scr[...] = lax.dot_general(in_ref[...], chosen, turn, preferred_element_type=F32).astype(BF16)
    mid_scr[...] = (mid_ref[...].astype(F32).T * 0.5).astype(BF16)
    last_scr[...] = last_ref[...].astype(F32).T.astype(BF16)

    slot_ids = lax.broadcasted_iota(jnp.int32, (512, 128), 0).astype(jnp.int16)
    row = lax.broadcasted_iota(jnp.int32, (ROWS, 128), 0)
    row_block = jnp.where(row < 216, row // 8, jnp.where(row < 243, row - 216, -1)).astype(jnp.int16)
    zero = jnp.zeros((240, 128), BF16)
    last_rows = lax.broadcasted_iota(jnp.int32, (16, 128), 0)

    def chunk(c, carry):
        lanes = pl.ds(pl.multiple_of(c * 128, 128), 128)
        info = info_ref[c]
        counts = info[0:1]
        most = jnp.max(counts).astype(jnp.int32)
        centre = jnp.zeros((16, 128), F32)
        for d in range(3):
            centre = jnp.where(last_rows == 3 + d, info[1 + d : 2 + d], centre)
        base = jnp.concatenate([zero, centre.astype(BF16)], axis=0)

        def step(t, total):
            hot = []
            for u in range(SLOTS):
                slot = jnp.broadcast_to(slots_ref[c, pl.ds(SLOTS * t + u, 1), :], (16, 128)).astype(jnp.int16)
                slot = jnp.concatenate([slot] * 32, axis=0)
                hot.append(jnp.where(slot_ids == slot, BF16(1), BF16(0)))
            found = jnp.dot(table_ref[...], jnp.concatenate(hot, axis=1), preferred_element_type=F32)
            found = found.astype(BF16)
            kept = []
            for u in range(SLOTS):
                block = jnp.broadcast_to(blocks_ref[c, pl.ds(SLOTS * t + u, 1), :], (16, 128)).astype(jnp.int16)
                block = jnp.concatenate([block] * (ROWS // 16), axis=0)
                kept.append(jnp.where(row_block == block, found[:, 128 * u : 128 * u + 128], base))
            hidden = jnp.dot(first_scr[...], jnp.concatenate(kept, axis=1), preferred_element_type=F32)
            hidden = twice_gelu(hidden).astype(BF16)
            hidden = twice_gelu(jnp.dot(mid_scr[...], hidden, preferred_element_type=F32))
            for u in range(SLOTS):
                used = (SLOTS * t + u).astype(F32) < counts
                total = total + jnp.where(used, hidden[:, 128 * u : 128 * u + 128], 0.0)
            return total

        total = lax.fori_loop(0, (most + SLOTS - 1) // SLOTS, step, jnp.zeros((80, 128), F32))
        mean = total * (0.5 / counts)
        upper = mean.astype(BF16)
        lower = (mean - upper.astype(F32)).astype(BF16)
        last = last_scr[...]
        values = jnp.dot(last, upper, preferred_element_type=F32) + jnp.dot(
            last, lower, preferred_element_type=F32
        )
        ordered[:, lanes] = values.astype(BF16)
        return carry

    lax.fori_loop(0, 8, chunk, 0)
    order = lax.broadcasted_iota(jnp.int32, (1024, 128), 0).astype(F32)
    parts = []
    for t in range(8):
        moved = jnp.where(order == rank_ref[0:1, 128 * t : 128 * t + 128], 1.0, 0.0).astype(BF16)
        part = jnp.dot(ordered[...], moved, preferred_element_type=F32)
        parts.append(part.reshape(8, 8, 128))
    out_ref[...] = jnp.stack(parts, axis=1).reshape(8, 64, 128).astype(BF16)


def encode(table, slots, blocks, info, rank, kernel_in, kernel_mid, kernel_out):
    vmem = pl.BlockSpec(memory_space=pltpu.VMEM)
    return pl.pallas_call(
        encoder_kernel,
        out_shape=jax.ShapeDtypeStruct((8, 64, 128), BF16),
        in_specs=[vmem] * 8,
        out_specs=vmem,
        scratch_shapes=[
            pltpu.VMEM((80, ROWS), BF16),
            pltpu.VMEM((80, 80), BF16),
            pltpu.VMEM((64, 80), BF16),
            pltpu.VMEM((64, 1024), BF16),
        ],
    )(table, slots, blocks, info, rank, kernel_in, kernel_mid, kernel_out)


def halves(values):
    upper = values.astype(np.float32).astype(ml_dtypes.bfloat16)
    lower = (values - upper.astype(np.float64)).astype(np.float32).astype(ml_dtypes.bfloat16)
    return np.stack([upper, lower])


def turn(frequency, position):
    angle = 2.0 * math.pi * ((frequency * position) % GRID) / GRID
    return np.cos(angle), np.sin(angle)


def centred(index):
    return np.where(index < MODES // 2, index, index - MODES)


def complex_block(cos, sin):
    return np.stack([np.stack([cos, sin], -1), np.stack([-sin, cos], -1)], -2)


@functools.lru_cache(None)
def third_table():
    cos, sin = turn(np.arange(16)[:, None], np.arange(64)[None, :])
    parts = np.stack([cos, -sin]).reshape(2, 4, 4, 64).transpose(1, 0, 2, 3)
    full = np.einsum("arkz,cd->arkczd", parts, np.eye(8))
    return full.reshape(256, 512)


@functools.lru_cache(None)
def second_table():
    j = np.arange(16)
    cos, sin = turn(centred(j)[:, None], np.arange(64)[None, :])
    both = complex_block(cos, sin).reshape(8, 2, 4, 16, 2, 2)
    full = np.einsum("gleyab,xw->lgaxebwy", both, np.eye(8))
    return full.reshape(2, 128, 1024)


@functools.lru_cache(None)
def first_table():
    i = np.arange(16)
    cos, sin = turn(centred(i)[:, None], np.arange(64)[None, :])
    both = complex_block(cos, sin).reshape(8, 2, 8, 8, 2, 2)
    return np.einsum("hltxab->tlhabx", both).reshape(8, 2, 16, 16)


def placed(values):
    return np.tile(np.moveaxis(halves(values), 0, 1), (1, 1, 1, 1, 8))


@functools.lru_cache(None)
def pair_table():
    out = np.zeros((4, 8, 8, 2, 8, 8, 2))
    for il in range(2):
        for jl in range(2):
            for h in range(8):
                for g in range(8):
                    i, j = 2 * h + il, 2 * g + jl
                    if i == 8 or j == 8:
                        continue
                    ni, nj = (16 - i) % 16, (16 - j) % 16
                    assert ni % 2 == il and nj % 2 == jl
                    for a in range(2):
                        out[2 * il + jl, g, h, a, nj // 2, ni // 2, a] = 1.0 - 2.0 * a
    return out.reshape(4, 128, 128)


def dotf(a, b):
    return jnp.dot(a, b, preferred_element_type=F32)


def dott(a, b):
    return lax.dot_general(a, b, (((1,), (1,)), ((), ())), preferred_element_type=F32)


def split(values):
    upper = values.astype(BF16)
    return upper, (values - upper.astype(F32)).astype(BF16)


def spectral_kernel(
    latent_ref, skip_ref, weight_ref, third_ref, back_ref, second_ref, first_ref, firstt_ref, pair_ref,
    out_ref,
    r1, z_msg, r2, s_msg, r3, t_msg, r4, mixing, n_msg, r5, g_msg, r6, f_msg, v_msg, r7, rv, b_msg, r8, skip,
    send, recv,
):
    me_x = lax.axis_index("gx")
    me_y = lax.axis_index("gy")
    me_z = lax.axis_index("gz")
    mine = {"gx": me_x, "gy": me_y, "gz": me_z}
    sizes = {"gx": GX, "gy": GY, "gz": GZ}

    barrier = pltpu.get_barrier_semaphore()
    total = 0
    for axis in ("gz", "gy", "gx"):
        for o in range(1, sizes[axis]):
            pl.semaphore_signal(
                barrier, inc=1, device_id={axis: lax.rem(mine[axis] + o, sizes[axis])}, device_id_type=MESH
            )
            total += 1
    pl.semaphore_wait(barrier, total)

    same = lax.broadcasted_iota(jnp.int32, (128, 128), 0) // 16 == lax.broadcasted_iota(jnp.int32, (128, 128), 1) // 16

    def spread_blocks(ref, part, l):
        small = ref[me_x, part, l].astype(F32)
        return jnp.where(same, jnp.concatenate([small] * 8, axis=0), 0.0).astype(BF16)

    def start(stage, axis, source, target):
        copies = []
        size = sizes[axis]
        for o in range(1, size):
            peer = lax.rem(mine[axis] + o, size)
            copy = pltpu.make_async_remote_copy(
                src_ref=source(peer),
                dst_ref=target.at[mine[axis]],
                send_sem=send.at[stage, o],
                recv_sem=recv.at[stage, o],
                device_id={axis: peer},
                device_id_type=MESH,
            )
            copy.start()
            copies.append(copy)
        return copies

    def finish(copies):
        for copy in copies:
            copy.wait_recv()

    waiting = []

    first = start(0, "gz", lambda p: latent_ref.at[p], r1)
    waiting += first
    r1[me_z] = latent_ref[me_z]
    first_tab = [[spread_blocks(first_ref, p, l) for l in range(2)] for p in range(2)]
    back_tab = [[spread_blocks(firstt_ref, p, l) for l in range(2)] for p in range(2)]
    skip_t = skip_ref[...].astype(F32).T.astype(BF16)
    for z in range(8):
        here = latent_ref[:, 8 * z : 8 * z + 8, :].reshape(64, 128)
        skip[z] = dotf(skip_t, here)
    for s in range(8):
        halves_of = []
        for b in range(2):
            halves_of.append(weight_ref[b, :, 8 * s : 8 * s + 8, :].astype(F32).reshape(128, 64))
        mixing[128 * s : 128 * s + 128, :] = jnp.concatenate(halves_of, axis=1).astype(BF16)
    finish(first)
    values = r1[...].reshape(512, 128)
    spectrum = dotf(third_ref[0], values) + dotf(third_ref[1], values)
    z_msg[...] = spectrum.astype(BF16).reshape(4, 64, 128)

    second = start(1, "gy", lambda p: z_msg.at[p], r2)
    waiting += second
    r2[me_y] = z_msg[me_y]
    finish(second)
    wide = jnp.concatenate(
        [r2[e, 32 * b : 32 * b + 32, :] for e in range(4) for b in range(2)], axis=1
    )
    rows = jnp.concatenate(
        [dott(second_ref[0, l], wide) + dott(second_ref[1, l], wide) for l in range(2)], axis=1
    )
    upper, lower = split(rows)
    partial = jnp.concatenate(
        [
            dotf(first_tab[0][l], upper) + dotf(first_tab[0][l], lower) + dotf(first_tab[1][l], upper)
            for l in range(2)
        ],
        axis=1,
    )
    s_msg[...] = partial.astype(BF16).reshape(8, 16, 128)

    third = start(2, "gx", lambda p: s_msg.at[p], r3)
    waiting += third
    r3[me_x] = s_msg[me_x]
    finish(third)
    modes = jnp.sum(r3[...].astype(F32), axis=0)
    for h in range(8):
        t_msg[h] = modes[2 * h : 2 * h + 2, :]

    fourth = start(3, "gz", lambda p: t_msg.at[p], r4)
    waiting += fourth
    r4[me_z] = t_msg[me_z]
    finish(fourth)
    mode_rows = lax.broadcasted_iota(jnp.int32, (16, 128), 0)
    lanes16 = lax.broadcasted_iota(jnp.int32, (16, 128), 1)
    own = mode_rows == lanes16 // 8
    expanded = jnp.concatenate(
        [
            jnp.concatenate(
                [
                    jnp.where(own, jnp.broadcast_to(r4[s, a : a + 1, :], (16, 128)), 0.0)
                    for s in range(8)
                ],
                axis=1,
            )
            for a in range(2)
        ],
        axis=0,
    ).astype(BF16)
    product = dotf(expanded, mixing[...])
    sign = jnp.where(lanes16 < 64, -1.0, 1.0)
    mixed = product[0:16] + pltpu.roll(product[16:32], 64, 1) * sign
    first_place = (me_x + me_y + me_z) == 0
    mixed = jnp.where((mode_rows == 0) & first_place, 0.0, mixed)
    spread = jnp.where(own, 1.0, 0.0).astype(BF16)
    tall = lax.dot_general(
        mixed.astype(BF16), spread, (((0,), (0,)), ((), ())), preferred_element_type=F32
    )
    tall_rows = lax.broadcasted_iota(jnp.int32, (128, 128), 0)
    tall_lanes = lax.broadcasted_iota(jnp.int32, (128, 128), 1)
    tall = jnp.where(tall_rows % 8 == tall_lanes % 8, tall, 0.0).astype(BF16)
    gather = (mode_rows % 2) * 8 + mode_rows // 2 == lanes16 // 8
    turned = dotf(jnp.where(gather, 1.0, 0.0).astype(BF16), tall)
    for h in range(8):
        n_msg[h] = turned[2 * h : 2 * h + 2, :]

    fifth = start(4, "gz", lambda p: n_msg.at[p], r5)
    waiting += fifth
    r5[me_z] = n_msg[me_z]
    finish(fifth)
    g_msg[...] = jnp.concatenate([r5[h] for h in range(8)], axis=0).astype(BF16)

    sixth = start(5, "gx", lambda p: g_msg, r6)
    waiting += sixth
    r6[me_x] = g_msg[...]
    finish(sixth)
    field = r6[...].reshape(128, 128)
    along = (
        dotf(back_tab[0][0], field[:, 0:64])
        + dotf(back_tab[1][0], field[:, 0:64])
        + dotf(back_tab[0][1], field[:, 64:128])
        + dotf(back_tab[1][1], field[:, 64:128])
    )
    upper, lower = split(along.T)
    plane = (
        dotf(upper[0:32], second_ref[0, 0])
        + dotf(lower[0:32], second_ref[0, 0])
        + dotf(upper[0:32], second_ref[1, 0])
        + dotf(upper[32:64], second_ref[0, 1])
        + dotf(lower[32:64], second_ref[0, 1])
        + dotf(upper[32:64], second_ref[1, 1])
    )
    zero_rows = lax.broadcasted_iota(jnp.int32, (32, 1024), 0)
    scale = 1.0 / GRID**3
    plane = plane * jnp.where((zero_rows < 8) & (me_y == 0), scale, 2.0 * scale)
    for e in range(4):
        for b in range(2):
            part = plane[:, (2 * e + b) * 128 : (2 * e + b + 1) * 128]
            f_msg[e, 32 * b : 32 * b + 32, :] = part.astype(BF16)

    seventh = start(6, "gy", lambda p: f_msg.at[p], r7)
    waiting += seventh
    r7[me_y] = f_msg[me_y]
    wide_field = field.astype(F32)
    lane_group = tall_lanes // 32
    paired = jnp.zeros((128, 128), F32)
    for p in range(4):
        paired = jnp.where(lane_group == p, dotf(pair_ref[p], field), paired)
    low = ((tall_lanes // 8) % 4 == 0) & (me_y == 0)
    power = jnp.where(low, 0.5 * wide_field * (wide_field + paired), 2.0 * wide_field * wide_field)
    power = jnp.sum(power, axis=0, keepdims=True)
    power = power + pltpu.roll(power, 64, 1)
    power = power + pltpu.roll(power, 32, 1)
    power = power + pltpu.roll(power, 16, 1)
    power = power + pltpu.roll(power, 8, 1)
    tall_power = jnp.broadcast_to(power, (128, 128)).T
    v_msg[...] = tall_power[0:8, :] * (scale * scale)
    eighth = start(7, "gy", lambda p: v_msg, rv)
    waiting += eighth
    rv[me_y] = v_msg[...]
    finish(seventh)
    grid_part = r7[...].reshape(256, 128)
    branch = dotf(back_ref[0], grid_part) + dotf(back_ref[1], grid_part)
    finish(eighth)
    variance = (rv[0] + rv[1]) + (rv[2] + rv[3])
    inverse = 1.0 / jnp.sqrt(variance + NORM_FLOOR)
    branch = branch.reshape(64, 8, 128) * inverse[None]
    b_msg[...] = branch.reshape(8, 64, 128).astype(BF16)

    ninth = start(8, "gz", lambda p: b_msg.at[p], r8)
    waiting += ninth
    r8[me_z] = b_msg[me_z]
    finish(ninth)
    for z in range(8):
        normed = r8[:, 8 * z : 8 * z + 8, :].astype(F32).reshape(64, 128)
        out_ref[:, z, :] = gelu(normed + skip[z]).T
    for copy in waiting:
        copy.wait_send()


def spectral_layer(latent, skip_t, weight, third, back, second, first, firstt, pair):
    vmem = pl.BlockSpec(memory_space=pltpu.VMEM)
    return pl.pallas_call(
        spectral_kernel,
        out_shape=jax.ShapeDtypeStruct((128, 8, 64), F32),
        in_specs=[vmem] * 9,
        out_specs=vmem,
        scratch_shapes=[
            pltpu.VMEM((8, 64, 128), BF16),
            pltpu.VMEM((4, 64, 128), BF16),
            pltpu.VMEM((4, 64, 128), BF16),
            pltpu.VMEM((8, 16, 128), BF16),
            pltpu.VMEM((8, 16, 128), BF16),
            pltpu.VMEM((8, 2, 128), F32),
            pltpu.VMEM((8, 2, 128), F32),
            pltpu.VMEM((1024, 128), BF16),
            pltpu.VMEM((8, 2, 128), F32),
            pltpu.VMEM((8, 2, 128), F32),
            pltpu.VMEM((16, 128), BF16),
            pltpu.VMEM((8, 16, 128), BF16),
            pltpu.VMEM((4, 64, 128), BF16),
            pltpu.VMEM((8, 128), F32),
            pltpu.VMEM((4, 64, 128), BF16),
            pltpu.VMEM((4, 8, 128), F32),
            pltpu.VMEM((8, 64, 128), BF16),
            pltpu.VMEM((8, 64, 128), BF16),
            pltpu.VMEM((8, 64, 128), F32),
            pltpu.SemaphoreType.DMA((9, 8)),
            pltpu.SemaphoreType.DMA((9, 8)),
        ],
        compiler_params=pltpu.CompilerParams(collective_id=0, has_side_effects=True),
    )(latent, skip_t, weight, third, back, second, first, firstt, pair)


def body(point_data, neighbours, counts, kernel_in, kernel_mid, kernel_out, spectral, skip_weight):
    cells_x, cells_y, cells_z = neighbours.shape[1:4]
    made = halo(
        point_data[0],
        neighbours.reshape(-1, NB),
        jnp.transpose(counts[0], (2, 0, 1)).reshape(1, -1),
    )
    latent = encode(*made, kernel_in, kernel_mid, kernel_out)
    third = third_table()
    by_place = first_table()
    out = spectral_layer(
        latent,
        skip_weight,
        spectral.reshape(2, 16, 64, 64),
        jnp.asarray(halves(third)),
        jnp.asarray(halves(third.T)),
        jnp.asarray(halves(second_table())),
        jnp.asarray(placed(by_place)),
        jnp.asarray(placed(np.swapaxes(by_place, 2, 3))),
        jnp.asarray(pair_table().astype(ml_dtypes.bfloat16)),
    )
    return out.reshape(1, cells_x, cells_y, cells_z, -1)


def solution(mesh):
    in_specs = (
        P(None, None, ("gx", "gy", "gz")),
        P(None, "gx", "gy", "gz", None),
        P(None, "gx", "gy", "gz"),
        P(),
        P(),
        P(),
        P(None, "gz", "gx", "gy", None, None),
        P(),
    )
    out_specs = P(None, "gx", "gy", "gz", None)
    return jax.shard_map(body, mesh=mesh, in_specs=in_specs, out_specs=out_specs, check_vma=False)
```

```python
import functools
import math

import jax
import jax.numpy as jnp
import ml_dtypes
import numpy as np
from jax import lax
from jax.experimental import pallas as pl
from jax.experimental.pallas import tpu as pltpu
from jax.sharding import PartitionSpec as P

GRID = 64
MODES = 16
NB = 32
NORM_FLOOR = 1.0
GX, GY, GZ = 8, 4, 8
F32 = jnp.float32
BF16 = jnp.bfloat16
MESH = pl.DeviceIdType.MESH


def gelu(v):
    inner = v * (0.7978845608028654 + 0.035677408136300125 * (v * v))
    half = 0.5 * v
    return half + half * jnp.tanh(inner)


def twice_gelu(v):
    if not GELU16:
        return v + v * jnp.tanh(v * (0.7978845608028654 + 0.035677408136300125 * (v * v)))
    v = v.astype(BF16)
    inner = v * (BF16(0.7978845608028654) + BF16(0.035677408136300125) * (v * v))
    return v + v * jnp.tanh(inner)


SLOTS = 4
ROWS = 176
FOUR, SIX = 108, 162
GELU16 = True
OFFSETS = [(dx, dy, dz) for dx in (-1, 0, 1) for dy in (-1, 0, 1) for dz in (-1, 0, 1)]


def halo_kernel(
    points_ref, near_ref, counts_ref, table_ref, slots_ref, blocks_ref, info_ref, rank_ref,
    main, send, recv,
):
    me_x = lax.axis_index("gx")
    me_y = lax.axis_index("gy")
    me_z = lax.axis_index("gz")

    def device(offset):
        dx, dy, dz = offset
        return {
            "gx": lax.rem(me_x + dx + GX, GX),
            "gy": lax.rem(me_y + dy + GY, GY),
            "gz": lax.rem(me_z + dz + GZ, GZ),
        }

    barrier = pltpu.get_barrier_semaphore()
    peers = [o for o in OFFSETS if o != (0, 0, 0)]
    for offset in peers:
        pl.semaphore_signal(barrier, inc=1, device_id=device(offset), device_id_type=MESH)

    points = points_ref[...]
    main[13] = jnp.concatenate([points, jnp.zeros((2, 512), F32)], axis=0).astype(BF16)
    pl.semaphore_wait(barrier, len(peers))
    copies = []
    for n, offset in enumerate(peers):
        slot = 26 - OFFSETS.index(offset)
        for k, buffer in enumerate((main,)):
            copy = pltpu.make_async_remote_copy(
                src_ref=buffer.at[13],
                dst_ref=buffer.at[slot],
                send_sem=send.at[k, n],
                recv_sem=recv.at[k, n],
                device_id=device(offset),
                device_id_type=MESH,
            )
            copy.start()
            copies.append(copy)

    lane = lax.broadcasted_iota(jnp.int32, (1, 1024), 1)
    counts = counts_ref[...].astype(F32)
    key = counts * 1024.0 + (1023 - lane).astype(F32)
    ones = jnp.ones((8, 128), BF16)
    rank = jnp.zeros((8, 1024), F32)
    for m in range(8):
        tall = jnp.broadcast_to(key[:, 128 * m : 128 * m + 128], (128, 128)).T
        ahead = jnp.concatenate(
            [
                jnp.where(tall > key[:, 128 * n : 128 * n + 128], 1.0, 0.0).astype(BF16)
                for n in range(8)
            ],
            axis=1,
        )
        rank = rank + jnp.dot(ones, ahead, preferred_element_type=F32)
    rank_ref[...] = rank
    near = jnp.concatenate(
        [near_ref[pl.ds(z, 128, stride=8), :].astype(F32).T for z in range(8)], axis=1
    ).astype(jnp.int32)
    owner = near >> 9
    part = near & 511
    block = ((((owner >> 5) - me_x + 1) * 3) + ((owner >> 3) & 3) - me_y + 1) * 3 + (owner & 7) - me_z + 1
    code = jnp.clip(block, 0, 26) * 2 + (part >> 8)
    place_y = (me_y * 16 + (lane & 15)).astype(F32)
    place_x = (me_x * 8 + ((lane >> 4) & 7)).astype(F32)
    place_z = (me_z * 8 + (lane >> 7)).astype(F32)
    centres = [-(place + 0.5) / GRID for place in (place_x, place_y, place_z)]
    rows = jnp.concatenate(
        [(part & 255).astype(F32), code.astype(F32), counts] + centres + [jnp.zeros((12, 1024), F32)], axis=0
    ).astype(BF16)
    order = lax.broadcasted_iota(jnp.int32, (128, 1024), 0).astype(F32)
    wide_rank = rank[0:1]
    for t in range(8):
        moved = jnp.where(order + 128.0 * t == wide_rank, 1.0, 0.0).astype(BF16)
        moved = lax.dot_general(rows, moved, (((1,), (1,)), ((), ())), preferred_element_type=F32)
        slots_ref[t] = moved[0:32].astype(jnp.int32)
        blocks_ref[t] = moved[32:64].astype(jnp.int32)
        info_ref[t] = moved[64:72]

    for copy in copies:
        copy.wait_recv()
    blocks = [main[b].astype(F32) for b in range(27)]
    rows = [block[0:4] for block in blocks] + [block[4:6] for block in blocks]
    rows.append(jnp.zeros((ROWS - SIX, 512), F32))
    rows = jnp.concatenate(rows, axis=0).astype(BF16)
    table_ref[0:ROWS, :] = rows[:, 0:256]
    table_ref[ROWS : 2 * ROWS, :] = rows[:, 256:512]
    for copy in copies:
        copy.wait_send()


def halo(points, near, counts):
    vmem = pl.BlockSpec(memory_space=pltpu.VMEM)
    return pl.pallas_call(
        halo_kernel,
        out_shape=[
            jax.ShapeDtypeStruct((2 * ROWS, 256), BF16),
            jax.ShapeDtypeStruct((8, NB, 128), jnp.int32),
            jax.ShapeDtypeStruct((8, NB, 128), jnp.int32),
            jax.ShapeDtypeStruct((8, 8, 128), F32),
            jax.ShapeDtypeStruct((8, 1024), F32),
        ],
        in_specs=[vmem] * 3,
        out_specs=[vmem] * 5,
        scratch_shapes=[
            pltpu.VMEM((27, 8, 512), BF16),
            pltpu.SemaphoreType.DMA((1, 26)),
            pltpu.SemaphoreType.DMA((1, 26)),
        ],
        compiler_params=pltpu.CompilerParams(collective_id=1, has_side_effects=True),
    )(points, near, counts)


def encoder_kernel(
    table_ref, slots_ref, blocks_ref, info_ref, rank_ref, in_ref, mid_ref, last_ref, out_ref,
    first_scr, mid_scr, last_scr, kept_scr, hidden_scr, base_scr, totals, trips,
):
    column = lax.broadcasted_iota(jnp.int32, (6, ROWS), 1)
    feature = lax.broadcasted_iota(jnp.int32, (6, ROWS), 0)
    wanted = jnp.where(column < FOUR, column % 4, 4 + column % 2)
    wanted = jnp.where(column >= SIX, column - SIX, wanted)
    chosen = jnp.where((feature == wanted) & (column < SIX + 3), 1.0, 0.0).astype(BF16)
    turn = (((0,), (0,)), ((), ()))
    first_scr[...] = lax.dot_general(in_ref[...], chosen, turn, preferred_element_type=F32).astype(BF16)
    half_mid = (mid_ref[...].astype(F32).T * 0.5).astype(BF16)
    mid_scr[...] = jnp.zeros(mid_scr.shape, BF16)
    mid_scr[0:80, 0:80] = half_mid
    mid_scr[80:160, 80:160] = half_mid
    last_scr[...] = last_ref[...].astype(F32).T.astype(BF16)

    slot_ids = lax.broadcasted_iota(jnp.int32, (256, 128), 0).astype(jnp.int16)
    row = lax.broadcasted_iota(jnp.int32, (ROWS, 128), 0)
    row_block = jnp.where(row < FOUR, row // 4, jnp.where(row < SIX, (row - FOUR) // 2, -1)).astype(jnp.int16)
    last_rows = lax.broadcasted_iota(jnp.int32, (16, 128), 0)
    steps = 0
    for c in range(8):
        info = info_ref[c]
        trip = (jnp.max(info[0:1]).astype(jnp.int32) + SLOTS - 1) // SLOTS
        trips[c] = trip
        steps += trip
        centre = jnp.zeros((16, 128), F32)
        for d in range(3):
            centre = jnp.where(last_rows == SIX - ROWS + 16 + d, info[1 + d : 2 + d], centre)
        base_scr[c] = centre.astype(BF16)
        totals[c] = jnp.zeros((80, 128), F32)
    totals[8] = jnp.zeros((80, 128), F32)
    kept_scr[...] = jnp.zeros(kept_scr.shape, BF16)
    hidden_scr[...] = jnp.zeros(hidden_scr.shape, BF16)

    def step(n, places):
        (c0, t0), (c1, t1), (c2, t2) = places
        hidden = twice_gelu(jnp.dot(mid_scr[...], hidden_scr[...], preferred_element_type=F32))
        counts = info_ref[jnp.minimum(c2, 7), 0:1, :]
        total = totals[c2]
        for u in range(SLOTS):
            used = (SLOTS * t2 + u).astype(F32) < counts
            here = hidden[80 * (u // 2) : 80 * (u // 2) + 80, 128 * (u % 2) : 128 * (u % 2) + 128]
            total = total + jnp.where(used, here.astype(F32), 0.0)
        totals[c2] = total
        hidden = jnp.dot(first_scr[...], kept_scr[...], preferred_element_type=F32)
        hidden = twice_gelu(hidden).astype(BF16)
        for u in range(SLOTS // 2):
            hidden_scr[80 * u : 80 * u + 80, :] = hidden[:, 256 * u : 256 * u + 256]
        hot = []
        for u in range(SLOTS):
            slot = jnp.broadcast_to(slots_ref[c0, pl.ds(SLOTS * t0 + u, 1), :], (16, 128)).astype(jnp.int16)
            slot = jnp.concatenate([slot] * 16, axis=0)
            hot.append(jnp.where(slot_ids == slot, BF16(1), BF16(0)))
        found = jnp.dot(table_ref[...], jnp.concatenate(hot, axis=1), preferred_element_type=F32)
        found = found.astype(BF16)
        for u in range(SLOTS):
            code = jnp.broadcast_to(blocks_ref[c0, pl.ds(SLOTS * t0 + u, 1), :], (16, 128))
            block = (code >> 1).astype(jnp.int16)
            odd = (code & 1).astype(jnp.int16)
            same = row_block == jnp.concatenate([block] * (ROWS // 16), axis=0)
            odd = jnp.concatenate([odd] * (ROWS // 16), axis=0) == 1
            here = found[:, 128 * u : 128 * u + 128]
            here = jnp.where(odd, here[ROWS : 2 * ROWS], here[0:ROWS])
            kept_scr[0 : ROWS - 16, 128 * u : 128 * u + 128] = jnp.where(same[0 : ROWS - 16], here[0 : ROWS - 16], BF16(0))
            kept_scr[ROWS - 16 : ROWS, 128 * u : 128 * u + 128] = jnp.where(same[ROWS - 16 : ROWS], here[ROWS - 16 : ROWS], base_scr[c0])
        ended = t0 + 1 >= trips[c0]
        following = (
            jnp.minimum(jnp.where(ended, c0 + 1, c0), 7),
            jnp.where(ended, jnp.where(c0 == 7, t0, 0), t0 + 1),
        )
        return following, (c0, t0), (c1, t1)

    start = (jnp.int32(0), jnp.int32(0))
    spare = (jnp.int32(8), jnp.int32(0))
    lax.fori_loop(0, steps + 2, step, (start, spare, spare))
    last = last_scr[...]
    ordered = []
    for c in range(8):
        mean = totals[c] * (0.5 / info_ref[c, 0:1, :])
        upper = mean.astype(BF16)
        lower = (mean - upper.astype(F32)).astype(BF16)
        values = jnp.dot(last, upper, preferred_element_type=F32) + jnp.dot(
            last, lower, preferred_element_type=F32
        )
        ordered.append(values.astype(BF16))
    ordered = jnp.concatenate(ordered, axis=1)
    order = lax.broadcasted_iota(jnp.int32, (1024, 128), 0).astype(F32)
    parts = []
    for t in range(8):
        moved = jnp.where(order == rank_ref[0:1, 128 * t : 128 * t + 128], 1.0, 0.0).astype(BF16)
        part = jnp.dot(ordered, moved, preferred_element_type=F32)
        parts.append(part.reshape(8, 8, 128))
    out_ref[...] = jnp.stack(parts, axis=1).reshape(8, 64, 128).astype(BF16)


def encode(table, slots, blocks, info, rank, kernel_in, kernel_mid, kernel_out):
    vmem = pl.BlockSpec(memory_space=pltpu.VMEM)
    return pl.pallas_call(
        encoder_kernel,
        out_shape=jax.ShapeDtypeStruct((8, 64, 128), BF16),
        in_specs=[vmem] * 8,
        out_specs=vmem,
        scratch_shapes=[
            pltpu.VMEM((80, ROWS), BF16),
            pltpu.VMEM((160, 160), BF16),
            pltpu.VMEM((64, 80), BF16),
            pltpu.VMEM((ROWS, 128 * SLOTS), BF16),
            pltpu.VMEM((160, 256), BF16),
            pltpu.VMEM((8, 16, 128), BF16),
            pltpu.VMEM((9, 80, 128), F32),
            pltpu.SMEM((8,), jnp.int32),
        ],
    )(table, slots, blocks, info, rank, kernel_in, kernel_mid, kernel_out)


def halves(values):
    upper = values.astype(np.float32).astype(ml_dtypes.bfloat16)
    lower = (values - upper.astype(np.float64)).astype(np.float32).astype(ml_dtypes.bfloat16)
    return np.stack([upper, lower])


def turn(frequency, position):
    angle = 2.0 * math.pi * ((frequency * position) % GRID) / GRID
    return np.cos(angle), np.sin(angle)


def centred(index):
    return np.where(index < MODES // 2, index, index - MODES)


def complex_block(cos, sin):
    return np.stack([np.stack([cos, sin], -1), np.stack([-sin, cos], -1)], -2)


@functools.lru_cache(None)
def third_table():
    cos, sin = turn(np.arange(16)[:, None], np.arange(64)[None, :])
    parts = np.stack([cos, -sin]).reshape(2, 4, 4, 64).transpose(1, 0, 2, 3)
    full = np.einsum("arkz,cd->arkczd", parts, np.eye(8))
    return full.reshape(256, 512)


@functools.lru_cache(None)
def second_table():
    j = np.arange(16)
    cos, sin = turn(centred(j)[:, None], np.arange(64)[None, :])
    both = complex_block(cos, sin).reshape(8, 2, 4, 16, 2, 2)
    full = np.einsum("gleyab,xw->lgaxebwy", both, np.eye(8))
    return full.reshape(2, 128, 1024)


@functools.lru_cache(None)
def first_table():
    i = np.arange(16)
    cos, sin = turn(centred(i)[:, None], np.arange(64)[None, :])
    both = complex_block(cos, sin).reshape(8, 2, 8, 8, 2, 2)
    return np.einsum("hltxab->tlhabx", both).reshape(8, 2, 16, 16)


def placed(values):
    return np.tile(np.moveaxis(halves(values), 0, 1), (1, 1, 1, 1, 8))


@functools.lru_cache(None)
def pair_table():
    out = np.zeros((4, 8, 8, 2, 8, 8, 2))
    for il in range(2):
        for jl in range(2):
            for h in range(8):
                for g in range(8):
                    i, j = 2 * h + il, 2 * g + jl
                    if i == 8 or j == 8:
                        continue
                    ni, nj = (16 - i) % 16, (16 - j) % 16
                    assert ni % 2 == il and nj % 2 == jl
                    for a in range(2):
                        out[2 * il + jl, g, h, a, nj // 2, ni // 2, a] = 1.0 - 2.0 * a
    return out.reshape(4, 128, 128)


def dotf(a, b):
    return jnp.dot(a, b, preferred_element_type=F32)


def dott(a, b):
    return lax.dot_general(a, b, (((1,), (1,)), ((), ())), preferred_element_type=F32)


def split(values):
    upper = values.astype(BF16)
    return upper, (values - upper.astype(F32)).astype(BF16)


def spectral_kernel(
    latent_ref, skip_ref, weight_ref, third_ref, back_ref, second_ref, first_ref, firstt_ref, pair_ref,
    out_ref,
    r1, z_msg, r2, s_msg, r3, t_msg, r4, mixing, n_msg, r5, g_msg, r6, f_msg, v_msg, r7, rv, b_msg, r8, skip,
    send, recv,
):
    me_x = lax.axis_index("gx")
    me_y = lax.axis_index("gy")
    me_z = lax.axis_index("gz")
    mine = {"gx": me_x, "gy": me_y, "gz": me_z}
    sizes = {"gx": GX, "gy": GY, "gz": GZ}

    barrier = pltpu.get_barrier_semaphore()
    total = 0
    for axis in ("gz", "gy", "gx"):
        for o in range(1, sizes[axis]):
            pl.semaphore_signal(
                barrier, inc=1, device_id={axis: lax.rem(mine[axis] + o, sizes[axis])}, device_id_type=MESH
            )
            total += 1
    pl.semaphore_wait(barrier, total)

    same = lax.broadcasted_iota(jnp.int32, (128, 128), 0) // 16 == lax.broadcasted_iota(jnp.int32, (128, 128), 1) // 16

    def spread_blocks(ref, part, l):
        small = ref[me_x, part, l].astype(F32)
        return jnp.where(same, jnp.concatenate([small] * 8, axis=0), 0.0).astype(BF16)

    def start(stage, axis, source, target):
        copies = []
        size = sizes[axis]
        for o in range(1, size):
            peer = lax.rem(mine[axis] + o, size)
            copy = pltpu.make_async_remote_copy(
                src_ref=source(peer),
                dst_ref=target.at[mine[axis]],
                send_sem=send.at[stage, o],
                recv_sem=recv.at[stage, o],
                device_id={axis: peer},
                device_id_type=MESH,
            )
            copy.start()
            copies.append(copy)
        return copies

    def finish(copies):
        for copy in copies:
            copy.wait_recv()

    waiting = []

    first = start(0, "gz", lambda p: latent_ref.at[p], r1)
    waiting += first
    r1[me_z] = latent_ref[me_z]
    first_tab = [[spread_blocks(first_ref, p, l) for l in range(2)] for p in range(2)]
    back_tab = [[spread_blocks(firstt_ref, p, l) for l in range(2)] for p in range(2)]
    skip_t = skip_ref[...].astype(F32).T.astype(BF16)
    for z in range(8):
        here = latent_ref[:, 8 * z : 8 * z + 8, :].reshape(64, 128)
        skip[z] = dotf(skip_t, here)
    for s in range(8):
        halves_of = []
        for b in range(2):
            halves_of.append(weight_ref[b, :, 8 * s : 8 * s + 8, :].astype(F32).reshape(128, 64))
        mixing[128 * s : 128 * s + 128, :] = jnp.concatenate(halves_of, axis=1).astype(BF16)
    finish(first)
    values = r1[...].reshape(512, 128)
    spectrum = dotf(third_ref[0], values) + dotf(third_ref[1], values)
    z_msg[...] = spectrum.astype(BF16).reshape(4, 64, 128)

    second = start(1, "gy", lambda p: z_msg.at[p], r2)
    waiting += second
    r2[me_y] = z_msg[me_y]
    finish(second)
    wide = jnp.concatenate(
        [r2[e, 32 * b : 32 * b + 32, :] for e in range(4) for b in range(2)], axis=1
    )
    rows = jnp.concatenate(
        [dott(second_ref[0, l], wide) + dott(second_ref[1, l], wide) for l in range(2)], axis=1
    )
    upper, lower = split(rows)
    partial = jnp.concatenate(
        [
            dotf(first_tab[0][l], upper) + dotf(first_tab[0][l], lower) + dotf(first_tab[1][l], upper)
            for l in range(2)
        ],
        axis=1,
    )
    s_msg[...] = partial.astype(BF16).reshape(8, 16, 128)

    third = start(2, "gx", lambda p: s_msg.at[p], r3)
    waiting += third
    r3[me_x] = s_msg[me_x]
    finish(third)
    modes = jnp.sum(r3[...].astype(F32), axis=0)
    for h in range(8):
        t_msg[h] = modes[2 * h : 2 * h + 2, :]

    fourth = start(3, "gz", lambda p: t_msg.at[p], r4)
    waiting += fourth
    r4[me_z] = t_msg[me_z]
    finish(fourth)
    mode_rows = lax.broadcasted_iota(jnp.int32, (16, 128), 0)
    lanes16 = lax.broadcasted_iota(jnp.int32, (16, 128), 1)
    own = mode_rows == lanes16 // 8
    expanded = jnp.concatenate(
        [
            jnp.concatenate(
                [
                    jnp.where(own, jnp.broadcast_to(r4[s, a : a + 1, :], (16, 128)), 0.0)
                    for s in range(8)
                ],
                axis=1,
            )
            for a in range(2)
        ],
        axis=0,
    ).astype(BF16)
    product = dotf(expanded, mixing[...])
    sign = jnp.where(lanes16 < 64, -1.0, 1.0)
    mixed = product[0:16] + pltpu.roll(product[16:32], 64, 1) * sign
    first_place = (me_x + me_y + me_z) == 0
    mixed = jnp.where((mode_rows == 0) & first_place, 0.0, mixed)
    spread = jnp.where(own, 1.0, 0.0).astype(BF16)
    tall = lax.dot_general(
        mixed.astype(BF16), spread, (((0,), (0,)), ((), ())), preferred_element_type=F32
    )
    tall_rows = lax.broadcasted_iota(jnp.int32, (128, 128), 0)
    tall_lanes = lax.broadcasted_iota(jnp.int32, (128, 128), 1)
    tall = jnp.where(tall_rows % 8 == tall_lanes % 8, tall, 0.0).astype(BF16)
    gather = (mode_rows % 2) * 8 + mode_rows // 2 == lanes16 // 8
    turned = dotf(jnp.where(gather, 1.0, 0.0).astype(BF16), tall)
    for h in range(8):
        n_msg[h] = turned[2 * h : 2 * h + 2, :]

    fifth = start(4, "gz", lambda p: n_msg.at[p], r5)
    waiting += fifth
    r5[me_z] = n_msg[me_z]
    finish(fifth)
    g_msg[...] = jnp.concatenate([r5[h] for h in range(8)], axis=0).astype(BF16)

    sixth = start(5, "gx", lambda p: g_msg, r6)
    waiting += sixth
    r6[me_x] = g_msg[...]
    finish(sixth)
    field = r6[...].reshape(128, 128)
    along = (
        dotf(back_tab[0][0], field[:, 0:64])
        + dotf(back_tab[1][0], field[:, 0:64])
        + dotf(back_tab[0][1], field[:, 64:128])
        + dotf(back_tab[1][1], field[:, 64:128])
    )
    upper, lower = split(along.T)
    plane = (
        dotf(upper[0:32], second_ref[0, 0])
        + dotf(lower[0:32], second_ref[0, 0])
        + dotf(upper[0:32], second_ref[1, 0])
        + dotf(upper[32:64], second_ref[0, 1])
        + dotf(lower[32:64], second_ref[0, 1])
        + dotf(upper[32:64], second_ref[1, 1])
    )
    zero_rows = lax.broadcasted_iota(jnp.int32, (32, 1024), 0)
    scale = 1.0 / GRID**3
    plane = plane * jnp.where((zero_rows < 8) & (me_y == 0), scale, 2.0 * scale)
    for e in range(4):
        for b in range(2):
            part = plane[:, (2 * e + b) * 128 : (2 * e + b + 1) * 128]
            f_msg[e, 32 * b : 32 * b + 32, :] = part.astype(BF16)

    seventh = start(6, "gy", lambda p: f_msg.at[p], r7)
    waiting += seventh
    r7[me_y] = f_msg[me_y]
    wide_field = field.astype(F32)
    lane_group = tall_lanes // 32
    paired = jnp.zeros((128, 128), F32)
    for p in range(4):
        paired = jnp.where(lane_group == p, dotf(pair_ref[p], field), paired)
    low = ((tall_lanes // 8) % 4 == 0) & (me_y == 0)
    power = jnp.where(low, 0.5 * wide_field * (wide_field + paired), 2.0 * wide_field * wide_field)
    power = jnp.sum(power, axis=0, keepdims=True)
    power = power + pltpu.roll(power, 64, 1)
    power = power + pltpu.roll(power, 32, 1)
    power = power + pltpu.roll(power, 16, 1)
    power = power + pltpu.roll(power, 8, 1)
    tall_power = jnp.broadcast_to(power, (128, 128)).T
    v_msg[...] = tall_power[0:8, :] * (scale * scale)
    eighth = start(7, "gy", lambda p: v_msg, rv)
    waiting += eighth
    rv[me_y] = v_msg[...]
    finish(seventh)
    grid_part = r7[...].reshape(256, 128)
    branch = dotf(back_ref[0], grid_part) + dotf(back_ref[1], grid_part)
    finish(eighth)
    variance = (rv[0] + rv[1]) + (rv[2] + rv[3])
    inverse = 1.0 / jnp.sqrt(variance + NORM_FLOOR)
    branch = branch.reshape(64, 8, 128) * inverse[None]
    b_msg[...] = branch.reshape(8, 64, 128).astype(BF16)

    ninth = start(8, "gz", lambda p: b_msg.at[p], r8)
    waiting += ninth
    r8[me_z] = b_msg[me_z]
    finish(ninth)
    for z in range(8):
        normed = r8[:, 8 * z : 8 * z + 8, :].astype(F32).reshape(64, 128)
        out_ref[:, z, :] = gelu(normed + skip[z]).T
    for copy in waiting:
        copy.wait_send()


def spectral_layer(latent, skip_t, weight, third, back, second, first, firstt, pair):
    vmem = pl.BlockSpec(memory_space=pltpu.VMEM)
    return pl.pallas_call(
        spectral_kernel,
        out_shape=jax.ShapeDtypeStruct((128, 8, 64), F32),
        in_specs=[vmem] * 9,
        out_specs=vmem,
        scratch_shapes=[
            pltpu.VMEM((8, 64, 128), BF16),
            pltpu.VMEM((4, 64, 128), BF16),
            pltpu.VMEM((4, 64, 128), BF16),
            pltpu.VMEM((8, 16, 128), BF16),
            pltpu.VMEM((8, 16, 128), BF16),
            pltpu.VMEM((8, 2, 128), F32),
            pltpu.VMEM((8, 2, 128), F32),
            pltpu.VMEM((1024, 128), BF16),
            pltpu.VMEM((8, 2, 128), F32),
            pltpu.VMEM((8, 2, 128), F32),
            pltpu.VMEM((16, 128), BF16),
            pltpu.VMEM((8, 16, 128), BF16),
            pltpu.VMEM((4, 64, 128), BF16),
            pltpu.VMEM((8, 128), F32),
            pltpu.VMEM((4, 64, 128), BF16),
            pltpu.VMEM((4, 8, 128), F32),
            pltpu.VMEM((8, 64, 128), BF16),
            pltpu.VMEM((8, 64, 128), BF16),
            pltpu.VMEM((8, 64, 128), F32),
            pltpu.SemaphoreType.DMA((9, 8)),
            pltpu.SemaphoreType.DMA((9, 8)),
        ],
        compiler_params=pltpu.CompilerParams(collective_id=0, has_side_effects=True),
    )(latent, skip_t, weight, third, back, second, first, firstt, pair)


def body(point_data, neighbours, counts, kernel_in, kernel_mid, kernel_out, spectral, skip_weight):
    cells_x, cells_y, cells_z = neighbours.shape[1:4]
    made = halo(
        point_data[0],
        neighbours.reshape(-1, NB),
        jnp.transpose(counts[0], (2, 0, 1)).reshape(1, -1),
    )
    latent = encode(*made, kernel_in, kernel_mid, kernel_out)
    third = third_table()
    by_place = first_table()
    out = spectral_layer(
        latent,
        skip_weight,
        spectral.reshape(2, 16, 64, 64),
        jnp.asarray(halves(third)),
        jnp.asarray(halves(third.T)),
        jnp.asarray(halves(second_table())),
        jnp.asarray(placed(by_place)),
        jnp.asarray(placed(np.swapaxes(by_place, 2, 3))),
        jnp.asarray(pair_table().astype(ml_dtypes.bfloat16)),
    )
    return out.reshape(1, cells_x, cells_y, cells_z, -1)


def solution(mesh):
    in_specs = (
        P(None, None, ("gx", "gy", "gz")),
        P(None, "gx", "gy", "gz", None),
        P(None, "gx", "gy", "gz"),
        P(),
        P(),
        P(),
        P(None, "gz", "gx", "gy", None, None),
        P(),
    )
    out_specs = P(None, "gx", "gy", "gz", None)
    return jax.shard_map(body, mesh=mesh, in_specs=in_specs, out_specs=out_specs, check_vma=False)
```

```python
import functools
import math

import jax
import jax.numpy as jnp
import ml_dtypes
import numpy as np
from jax import lax
from jax.experimental import pallas as pl
from jax.experimental.pallas import tpu as pltpu
from jax.sharding import PartitionSpec as P

GRID = 64
MODES = 16
NB = 32
NORM_FLOOR = 1.0
GX, GY, GZ = 8, 4, 8
F32 = jnp.float32
BF16 = jnp.bfloat16
MESH = pl.DeviceIdType.MESH


def gelu(v):
    inner = v * (0.7978845608028654 + 0.035677408136300125 * (v * v))
    half = 0.5 * v
    return half + half * jnp.tanh(inner)


def twice_gelu(v):
    if not GELU16:
        return v + v * jnp.tanh(v * (0.7978845608028654 + 0.035677408136300125 * (v * v)))
    v = v.astype(BF16)
    inner = v * (BF16(0.7978845608028654) + BF16(0.035677408136300125) * (v * v))
    return v + v * jnp.tanh(inner)


SLOTS = 4
ROWS = 176
FOUR, SIX = 108, 162
GELU16 = True
OFFSETS = [(dx, dy, dz) for dx in (-1, 0, 1) for dy in (-1, 0, 1) for dz in (-1, 0, 1)]


def regroup(back):
    row = lax.broadcasted_iota(jnp.int32, (512, 512), 1 if back else 0)
    column = lax.broadcasted_iota(jnp.int32, (512, 512), 0 if back else 1)
    wanted = ((row >> 1) & 7) * 64 + (row >> 4) * 2 + (row & 1)
    return jnp.where(wanted == column, 1.0, 0.0).astype(BF16)


def halo_kernel(
    points_ref, near_ref, counts_ref, table_ref, slots_ref, blocks_ref, info_ref, rank_ref,
    main, send, recv,
):
    me_x = lax.axis_index("gx")
    me_y = lax.axis_index("gy")
    me_z = lax.axis_index("gz")

    def device(offset):
        dx, dy, dz = offset
        return {
            "gx": lax.rem(me_x + dx + GX, GX),
            "gy": lax.rem(me_y + dy + GY, GY),
            "gz": lax.rem(me_z + dz + GZ, GZ),
        }

    barrier = pltpu.get_barrier_semaphore()
    peers = [o for o in OFFSETS if o != (0, 0, 0)]
    for offset in peers:
        pl.semaphore_signal(barrier, inc=1, device_id=device(offset), device_id_type=MESH)

    main[13] = jnp.concatenate([points_ref[d] for d in range(6)] + [jnp.zeros((2, 512), F32)], axis=0).astype(BF16)
    pl.semaphore_wait(barrier, len(peers))
    copies = []
    for n, offset in enumerate(peers):
        slot = 26 - OFFSETS.index(offset)
        for k, buffer in enumerate((main,)):
            copy = pltpu.make_async_remote_copy(
                src_ref=buffer.at[13],
                dst_ref=buffer.at[slot],
                send_sem=send.at[k, n],
                recv_sem=recv.at[k, n],
                device_id=device(offset),
                device_id_type=MESH,
            )
            copy.start()
            copies.append(copy)

    lane = lax.broadcasted_iota(jnp.int32, (1, 1024), 1)
    counts = jnp.concatenate([counts_ref[x].astype(F32) for x in range(8)], axis=1)
    counts = jnp.concatenate([counts[z : z + 1] for z in range(8)], axis=1)
    key = counts * 1024.0 + (1023 - lane).astype(F32)
    ones = jnp.ones((8, 128), BF16)
    rank = jnp.zeros((8, 1024), F32)
    for m in range(8):
        tall = jnp.broadcast_to(key[:, 128 * m : 128 * m + 128], (128, 128)).T
        ahead = jnp.concatenate(
            [
                jnp.where(tall > key[:, 128 * n : 128 * n + 128], 1.0, 0.0).astype(BF16)
                for n in range(8)
            ],
            axis=1,
        )
        rank = rank + jnp.dot(ones, ahead, preferred_element_type=F32)
    rank_ref[...] = rank
    near = jnp.concatenate(
        [near_ref[pl.ds(z, 128, stride=8), :].astype(F32).T for z in range(8)], axis=1
    ).astype(jnp.int32)
    owner = near >> 9
    part = near & 511
    block = ((((owner >> 5) - me_x + 1) * 3) + ((owner >> 3) & 3) - me_y + 1) * 3 + (owner & 7) - me_z + 1
    code = jnp.clip(block, 0, 26) * 2 + (part >> 8)
    place_y = (me_y * 16 + (lane & 15)).astype(F32)
    place_x = (me_x * 8 + ((lane >> 4) & 7)).astype(F32)
    place_z = (me_z * 8 + (lane >> 7)).astype(F32)
    centres = [-(place + 0.5) / GRID for place in (place_x, place_y, place_z)]
    rows = jnp.concatenate(
        [(part & 255).astype(F32), code.astype(F32), counts] + centres + [jnp.zeros((12, 1024), F32)], axis=0
    ).astype(BF16)
    order = lax.broadcasted_iota(jnp.int32, (128, 1024), 0).astype(F32)
    wide_rank = rank[0:1]
    for t in range(8):
        moved = jnp.where(order + 128.0 * t == wide_rank, 1.0, 0.0).astype(BF16)
        moved = lax.dot_general(rows, moved, (((1,), (1,)), ((), ())), preferred_element_type=F32)
        slots_ref[t] = moved[0:32].astype(jnp.int32)
        blocks_ref[t] = moved[32:64].astype(jnp.int32)
        info_ref[t] = moved[64:72]

    for copy in copies:
        copy.wait_recv()
    blocks = [main[b].astype(F32) for b in range(27)]
    rows = [block[0:4] for block in blocks] + [block[4:6] for block in blocks]
    rows.append(jnp.zeros((ROWS - SIX, 512), F32))
    rows = jnp.concatenate(rows, axis=0).astype(BF16)
    table_ref[0:ROWS, :] = rows[:, 0:256]
    table_ref[ROWS : 2 * ROWS, :] = rows[:, 256:512]
    for copy in copies:
        copy.wait_send()


def halo(points, near, counts):
    vmem = pl.BlockSpec(memory_space=pltpu.VMEM)
    return pl.pallas_call(
        halo_kernel,
        out_shape=[
            jax.ShapeDtypeStruct((2 * ROWS, 256), BF16),
            jax.ShapeDtypeStruct((8, NB, 128), jnp.int32),
            jax.ShapeDtypeStruct((8, NB, 128), jnp.int32),
            jax.ShapeDtypeStruct((8, 8, 128), F32),
            jax.ShapeDtypeStruct((8, 1024), F32),
        ],
        in_specs=[vmem] * 3,
        out_specs=[vmem] * 5,
        scratch_shapes=[
            pltpu.VMEM((27, 8, 512), BF16),
            pltpu.SemaphoreType.DMA((1, 26)),
            pltpu.SemaphoreType.DMA((1, 26)),
        ],
        compiler_params=pltpu.CompilerParams(collective_id=1, has_side_effects=True),
    )(points, near, counts)


def encoder_kernel(
    table_ref, slots_ref, blocks_ref, info_ref, rank_ref, in_ref, mid_ref, last_ref, out_ref,
    first_scr, mid_scr, last_scr, kept_scr, hidden_scr, base_scr, totals, trips,
):
    column = lax.broadcasted_iota(jnp.int32, (6, ROWS), 1)
    feature = lax.broadcasted_iota(jnp.int32, (6, ROWS), 0)
    wanted = jnp.where(column < FOUR, column % 4, 4 + column % 2)
    wanted = jnp.where(column >= SIX, column - SIX, wanted)
    chosen = jnp.where((feature == wanted) & (column < SIX + 3), 1.0, 0.0).astype(BF16)
    turn = (((0,), (0,)), ((), ()))
    first_scr[...] = lax.dot_general(in_ref[...], chosen, turn, preferred_element_type=F32).astype(BF16)
    half_mid = (mid_ref[...].astype(F32).T * 0.5).astype(BF16)
    mid_scr[...] = jnp.zeros(mid_scr.shape, BF16)
    mid_scr[0:80, 0:80] = half_mid
    mid_scr[80:160, 80:160] = half_mid
    last_scr[...] = last_ref[...]

    slot_ids = lax.broadcasted_iota(jnp.int32, (256, 128), 0).astype(jnp.int16)
    row = lax.broadcasted_iota(jnp.int32, (ROWS, 128), 0)
    row_block = jnp.where(row < FOUR, row // 4, jnp.where(row < SIX, (row - FOUR) // 2, -1)).astype(jnp.int16)
    last_rows = lax.broadcasted_iota(jnp.int32, (16, 128), 0)
    steps = 0
    for c in range(8):
        info = info_ref[c]
        trip = (jnp.max(info[0:1]).astype(jnp.int32) + SLOTS - 1) // SLOTS
        trips[c] = trip
        steps += trip
        centre = jnp.zeros((16, 128), F32)
        for d in range(3):
            centre = jnp.where(last_rows == SIX - ROWS + 16 + d, info[1 + d : 2 + d], centre)
        base_scr[c] = centre.astype(BF16)
        totals[c] = jnp.zeros((80, 128), F32)
    totals[8] = jnp.zeros((80, 128), F32)
    kept_scr[...] = jnp.zeros(kept_scr.shape, BF16)
    hidden_scr[...] = jnp.zeros(hidden_scr.shape, BF16)

    def step(n, places):
        (c0, t0), (c1, t1), (c2, t2) = places
        hidden = twice_gelu(jnp.dot(mid_scr[...], hidden_scr[...], preferred_element_type=F32))
        counts = info_ref[jnp.minimum(c2, 7), 0:1, :]
        total = totals[c2]
        for u in range(SLOTS):
            used = (SLOTS * t2 + u).astype(F32) < counts
            here = hidden[80 * (u // 2) : 80 * (u // 2) + 80, 128 * (u % 2) : 128 * (u % 2) + 128]
            total = total + jnp.where(used, here.astype(F32), 0.0)
        totals[c2] = total
        hidden = jnp.dot(first_scr[...], kept_scr[...], preferred_element_type=F32)
        hidden = twice_gelu(hidden).astype(BF16)
        for u in range(SLOTS // 2):
            hidden_scr[80 * u : 80 * u + 80, :] = hidden[:, 256 * u : 256 * u + 256]
        hot = []
        for u in range(SLOTS):
            slot = jnp.broadcast_to(slots_ref[c0, pl.ds(SLOTS * t0 + u, 1), :], (16, 128)).astype(jnp.int16)
            slot = jnp.concatenate([slot] * 16, axis=0)
            hot.append(jnp.where(slot_ids == slot, BF16(1), BF16(0)))
        found = jnp.dot(table_ref[...], jnp.concatenate(hot, axis=1), preferred_element_type=F32)
        found = found.astype(BF16)
        for u in range(SLOTS):
            code = jnp.broadcast_to(blocks_ref[c0, pl.ds(SLOTS * t0 + u, 1), :], (16, 128))
            block = (code >> 1).astype(jnp.int16)
            odd = (code & 1).astype(jnp.int16)
            same = row_block == jnp.concatenate([block] * (ROWS // 16), axis=0)
            odd = jnp.concatenate([odd] * (ROWS // 16), axis=0) == 1
            here = found[:, 128 * u : 128 * u + 128]
            here = jnp.where(odd, here[ROWS : 2 * ROWS], here[0:ROWS])
            kept_scr[0 : ROWS - 16, 128 * u : 128 * u + 128] = jnp.where(same[0 : ROWS - 16], here[0 : ROWS - 16], BF16(0))
            kept_scr[ROWS - 16 : ROWS, 128 * u : 128 * u + 128] = jnp.where(same[ROWS - 16 : ROWS], here[ROWS - 16 : ROWS], base_scr[c0])
        ended = t0 + 1 >= trips[c0]
        following = (
            jnp.minimum(jnp.where(ended, c0 + 1, c0), 7),
            jnp.where(ended, jnp.where(c0 == 7, t0, 0), t0 + 1),
        )
        return following, (c0, t0), (c1, t1)

    start = (jnp.int32(0), jnp.int32(0))
    spare = (jnp.int32(8), jnp.int32(0))
    lax.fori_loop(0, steps + 2, step, (start, spare, spare))
    last = last_scr[...]
    ordered = []
    for c in range(8):
        mean = totals[c] * (0.5 / info_ref[c, 0:1, :])
        upper = mean.astype(BF16)
        lower = (mean - upper.astype(F32)).astype(BF16)
        values = jnp.dot(last, upper, preferred_element_type=F32) + jnp.dot(
            last, lower, preferred_element_type=F32
        )
        ordered.append(values.astype(BF16))
    ordered = jnp.concatenate(ordered, axis=1)
    order = lax.broadcasted_iota(jnp.int32, (1024, 128), 0).astype(F32)
    parts = []
    for t in range(8):
        moved = jnp.where(order == rank_ref[0:1, 128 * t : 128 * t + 128], 1.0, 0.0).astype(BF16)
        parts.append(jnp.dot(ordered, moved, preferred_element_type=F32).astype(BF16))
    parts = jnp.dot(regroup(False), jnp.concatenate(parts, axis=0), preferred_element_type=F32)
    out_ref[...] = parts.astype(BF16).reshape(32, 16, 128)


def encode(table, slots, blocks, info, rank, kernel_in, kernel_mid, kernel_out):
    vmem = pl.BlockSpec(memory_space=pltpu.VMEM)
    return pl.pallas_call(
        encoder_kernel,
        out_shape=jax.ShapeDtypeStruct((32, 16, 128), BF16),
        in_specs=[vmem] * 8,
        out_specs=vmem,
        scratch_shapes=[
            pltpu.VMEM((80, ROWS), BF16),
            pltpu.VMEM((160, 160), BF16),
            pltpu.VMEM((64, 80), BF16),
            pltpu.VMEM((ROWS, 128 * SLOTS), BF16),
            pltpu.VMEM((160, 256), BF16),
            pltpu.VMEM((8, 16, 128), BF16),
            pltpu.VMEM((9, 80, 128), F32),
            pltpu.SMEM((8,), jnp.int32),
        ],
    )(table, slots, blocks, info, rank, kernel_in, kernel_mid, kernel_out)


def halves(values):
    upper = values.astype(np.float32).astype(ml_dtypes.bfloat16)
    lower = (values - upper.astype(np.float64)).astype(np.float32).astype(ml_dtypes.bfloat16)
    return np.stack([upper, lower])


def turn(frequency, position):
    angle = 2.0 * math.pi * ((frequency * position) % GRID) / GRID
    return np.cos(angle), np.sin(angle)


def centred(index):
    return np.where(index < MODES // 2, index, index - MODES)


def complex_block(cos, sin):
    return np.stack([np.stack([cos, sin], -1), np.stack([-sin, cos], -1)], -2)


@functools.lru_cache(None)
def third_table():
    cos, sin = turn(np.arange(16)[:, None], np.arange(64)[None, :])
    full = np.einsum("akz,cd->akczd", np.stack([cos, -sin]), np.eye(2))
    return full.reshape(64, 128)


@functools.lru_cache(None)
def second_table():
    j = np.arange(16)
    cos, sin = turn(centred(j)[:, None], np.arange(64)[None, :])
    both = complex_block(cos, sin).reshape(8, 2, 4, 16, 2, 2)
    full = np.einsum("gleyab,xw->lgaxebwy", both, np.eye(8))
    return full.reshape(2, 128, 1024)


@functools.lru_cache(None)
def first_table():
    i = np.arange(16)
    cos, sin = turn(centred(i)[:, None], np.arange(64)[None, :])
    both = complex_block(cos, sin).reshape(8, 2, 8, 8, 2, 2)
    return np.einsum("hltxab->tlhabx", both).reshape(8, 2, 16, 16)


def placed(values):
    return np.tile(np.moveaxis(halves(values), 0, 1), (1, 1, 1, 1, 8))


@functools.lru_cache(None)
def pair_table():
    out = np.zeros((4, 8, 8, 2, 8, 8, 2))
    for il in range(2):
        for jl in range(2):
            for h in range(8):
                for g in range(8):
                    i, j = 2 * h + il, 2 * g + jl
                    if i == 8 or j == 8:
                        continue
                    ni, nj = (16 - i) % 16, (16 - j) % 16
                    assert ni % 2 == il and nj % 2 == jl
                    for a in range(2):
                        out[2 * il + jl, g, h, a, nj // 2, ni // 2, a] = 1.0 - 2.0 * a
    return out.reshape(4, 128, 128)


def dotf(a, b):
    return jnp.dot(a, b, preferred_element_type=F32)


def dott(a, b):
    return lax.dot_general(a, b, (((1,), (1,)), ((), ())), preferred_element_type=F32)


def split(values):
    upper = values.astype(BF16)
    return upper, (values - upper.astype(F32)).astype(BF16)


def spectral_kernel(
    latent_ref, skip_ref, weight_ref, third_ref, back_ref, second_ref, first_ref, firstt_ref, pair_ref,
    out_ref,
    r1, w_msg, rw, s_msg, r3, mixing, n_msg, r5, g_msg, r6, b_msg, r8, skip, send, recv,
):
    me_x = lax.axis_index("gx")
    me_y = lax.axis_index("gy")
    me_z = lax.axis_index("gz")
    me_q = me_y * GZ + me_z
    columns = [(y, z) for y in range(GY) for z in range(GZ) if y or z]

    def across(o):
        y, z = lax.rem(me_y + o[0], GY), lax.rem(me_z + o[1], GZ)
        return o[0] * GZ + o[1], {"gy": y, "gz": z}, y * GZ + z, me_q

    def along_x(o):
        peer = lax.rem(me_x + o, GX)
        return o, {"gx": peer}, peer, me_x

    planes = [across(o) for o in columns]
    lines = [along_x(o) for o in range(1, GX)]
    barrier = pltpu.get_barrier_semaphore()
    for _, device, _, _ in planes + lines:
        pl.semaphore_signal(barrier, inc=1, device_id=device, device_id_type=MESH)
    pl.semaphore_wait(barrier, len(planes + lines))

    def start(stage, peers, source, target):
        copies = []
        for n, device, peer, me in peers:
            copy = pltpu.make_async_remote_copy(
                src_ref=source(peer),
                dst_ref=target.at[me],
                send_sem=send.at[stage, n],
                recv_sem=recv.at[stage, n],
                device_id=device,
                device_id_type=MESH,
            )
            copy.start()
            copies.append(copy)
        return copies

    def finish(copies):
        for copy in copies:
            copy.wait_recv()

    waiting = []
    rows128 = lax.broadcasted_iota(jnp.int32, (128, 128), 0)
    lanes128 = lax.broadcasted_iota(jnp.int32, (128, 128), 1)
    same = rows128 // 16 == lanes128 // 16

    def spread_blocks(ref, part, l):
        small = ref[me_x, part, l].astype(F32)
        return jnp.where(same, jnp.concatenate([small] * 8, axis=0), 0.0).astype(BF16)

    first = start(0, planes, lambda p: latent_ref.at[p], r1)
    waiting += first
    r1[me_q] = latent_ref[me_q]
    forth = regroup(False)
    for l in range(2):
        wide = jnp.concatenate(
            [weight_ref[b, 8 * l : 8 * l + 8].astype(F32).reshape(512, 64) for b in range(2)], axis=1
        ).astype(BF16)
        w_msg[:, 16 * l : 16 * l + 16, :] = dotf(forth, wide).astype(BF16).reshape(32, 16, 128)
    weights = start(1, planes, lambda p: w_msg.at[p], rw)
    waiting += weights
    rw[me_q] = w_msg[me_q]
    first_tab = [[spread_blocks(first_ref, p, l) for l in range(2)] for p in range(2)]
    back_tab = [[spread_blocks(firstt_ref, p, l) for l in range(2)] for p in range(2)]
    skip_t = skip_ref[...].astype(F32).T.astype(BF16)
    natural = dotf(regroup(True), latent_ref[...].reshape(512, 128)).astype(BF16)
    for z in range(8):
        skip[z] = dotf(skip_t, natural[64 * z : 64 * z + 64])
    finish(first)

    pieces = []
    for e in range(4):
        values = r1[8 * e : 8 * e + 8].reshape(128, 128)
        piece = dotf(third_ref[0], values) + dotf(third_ref[1], values)
        pieces += [piece[0:32], piece[32:64]]
    wide = jnp.concatenate(pieces, axis=1).astype(BF16)
    rows = jnp.concatenate(
        [dott(second_ref[0, l], wide) + dott(second_ref[1, l], wide) for l in range(2)], axis=1
    )
    upper, lower = split(rows)
    partial = jnp.concatenate(
        [
            dotf(first_tab[0][l], upper) + dotf(first_tab[0][l], lower) + dotf(first_tab[1][l], upper)
            for l in range(2)
        ],
        axis=1,
    )
    s_msg[...] = partial.astype(BF16).reshape(8, 16, 128)

    third = start(2, lines, lambda p: s_msg.at[p], r3)
    waiting += third
    r3[me_x] = s_msg[me_x]
    finish(weights)
    for h in range(8):
        parts = [
            rw[e * 8 + h, 8 * p : 8 * p + 8, :].astype(F32) for p in range(4) for e in range(4)
        ]
        mixing[h] = jnp.concatenate(parts, axis=0).astype(BF16)
    finish(third)
    modes = jnp.sum(r3[...].astype(F32), axis=0)

    rows64 = lax.broadcasted_iota(jnp.int32, (64, 128), 0)
    lanes64 = lax.broadcasted_iota(jnp.int32, (64, 128), 1)
    own = rows64 == lanes64 // 2
    spread = jnp.where(own, 1.0, 0.0).astype(BF16)
    sign = jnp.where(lanes64 < 64, -1.0, 1.0)
    pair_same = rows128 % 2 == lanes128 % 2
    fold = jnp.where((rows64 % 2) * 32 + rows64 // 2 == lanes64 // 2, 1.0, 0.0).astype(BF16)
    turned = []
    for h in range(8):
        expanded = jnp.concatenate(
            [
                jnp.where(own, jnp.broadcast_to(modes[2 * h + a : 2 * h + a + 1], (64, 128)), 0.0)
                for a in range(2)
            ],
            axis=0,
        ).astype(BF16)
        product = dotf(expanded, mixing[h])
        mixed = product[0:64] + pltpu.roll(product[64:128], 64, 1) * sign
        tall = lax.dot_general(
            mixed.astype(BF16), spread, (((0,), (0,)), ((), ())), preferred_element_type=F32
        )
        tall = jnp.where(pair_same, tall, 0.0).astype(BF16)
        turned.append(dotf(fold, tall).astype(BF16))
    n_msg[...] = dotf(forth, jnp.concatenate(turned, axis=0)).astype(BF16).reshape(32, 16, 128)

    fourth = start(3, planes, lambda p: n_msg.at[p], r5)
    waiting += fourth
    r5[me_q] = n_msg[me_q]
    finish(fourth)
    mixed = jnp.sum(r5[...].astype(F32), axis=0)
    zero_rows = lax.broadcasted_iota(jnp.int32, (16, 128), 0)
    zero_lanes = lax.broadcasted_iota(jnp.int32, (16, 128), 1)
    mixed = jnp.where((zero_rows < 2) & (zero_lanes < 2) & (me_x == 0), 0.0, mixed)
    g_msg[...] = mixed.astype(BF16)

    fifth = start(4, lines, lambda p: g_msg, r6)
    waiting += fifth
    r6[me_x] = g_msg[...]
    finish(fifth)
    field = r6[...].reshape(128, 128)
    along = (
        dotf(back_tab[0][0], field[:, 0:64])
        + dotf(back_tab[1][0], field[:, 0:64])
        + dotf(back_tab[0][1], field[:, 64:128])
        + dotf(back_tab[1][1], field[:, 64:128])
    )
    upper, lower = split(along.T)
    plane = (
        dotf(upper[0:32], second_ref[0, 0])
        + dotf(lower[0:32], second_ref[0, 0])
        + dotf(upper[0:32], second_ref[1, 0])
        + dotf(upper[32:64], second_ref[0, 1])
        + dotf(lower[32:64], second_ref[0, 1])
        + dotf(upper[32:64], second_ref[1, 1])
    )
    scale = 1.0 / GRID**3
    plane_rows = lax.broadcasted_iota(jnp.int32, (32, 1024), 0)
    plane = (plane * jnp.where(plane_rows < 2, scale, 2.0 * scale)).astype(BF16)
    wide_field = field.astype(F32)
    paired = jnp.zeros((128, 128), F32)
    for p in range(4):
        paired = jnp.where(lanes128 // 32 == p, dotf(pair_ref[p], field), paired)
    low = (lanes128 // 2) % 16 == 0
    power = jnp.where(low, 0.5 * wide_field * (wide_field + paired), 2.0 * wide_field * wide_field)
    power = jnp.sum(power, axis=0, keepdims=True)
    for shift in (64, 32, 16, 8, 4, 2):
        power = power + pltpu.roll(power, shift, 1)
    variance = jnp.broadcast_to(power, (128, 128)).T * (scale * scale)
    inverse = 1.0 / jnp.sqrt(variance + NORM_FLOOR)
    for e in range(4):
        part = jnp.concatenate(
            [plane[:, (2 * e + b) * 128 : (2 * e + b + 1) * 128] for b in range(2)], axis=0
        )
        branch = (dotf(back_ref[0], part) + dotf(back_ref[1], part)) * inverse
        b_msg[8 * e : 8 * e + 8] = branch.astype(BF16).reshape(8, 16, 128)

    sixth = start(5, planes, lambda p: b_msg.at[p], r8)
    waiting += sixth
    r8[me_q] = b_msg[me_q]
    finish(sixth)
    normed = dotf(regroup(True), r8[...].reshape(512, 128))
    for z in range(8):
        out_ref[:, z, :] = gelu(normed[64 * z : 64 * z + 64] + skip[z]).T
    for copy in waiting:
        copy.wait_send()


def spectral_layer(latent, skip_w, weight, third, back, second, first, firstt, pair):
    vmem = pl.BlockSpec(memory_space=pltpu.VMEM)
    return pl.pallas_call(
        spectral_kernel,
        out_shape=jax.ShapeDtypeStruct((128, 8, 64), F32),
        in_specs=[vmem] * 9,
        out_specs=vmem,
        scratch_shapes=[
            pltpu.VMEM((32, 16, 128), BF16),
            pltpu.VMEM((32, 32, 128), BF16),
            pltpu.VMEM((32, 32, 128), BF16),
            pltpu.VMEM((8, 16, 128), BF16),
            pltpu.VMEM((8, 16, 128), BF16),
            pltpu.VMEM((8, 128, 128), BF16),
            pltpu.VMEM((32, 16, 128), BF16),
            pltpu.VMEM((32, 16, 128), BF16),
            pltpu.VMEM((16, 128), BF16),
            pltpu.VMEM((8, 16, 128), BF16),
            pltpu.VMEM((32, 16, 128), BF16),
            pltpu.VMEM((32, 16, 128), BF16),
            pltpu.VMEM((8, 64, 128), F32),
            pltpu.SemaphoreType.DMA((6, 32)),
            pltpu.SemaphoreType.DMA((6, 32)),
        ],
        compiler_params=pltpu.CompilerParams(collective_id=0, has_side_effects=True),
    )(latent, skip_w, weight, third, back, second, first, firstt, pair)


def body(point_data, neighbours, counts, kernel_in, kernel_mid, kernel_out, spectral, skip_weight):
    cells_x, cells_y, cells_z = neighbours.shape[1:4]
    made = halo(
        jnp.transpose(point_data, (1, 0, 2)),
        neighbours.reshape(-1, NB),
        jnp.transpose(counts[0], (0, 2, 1)),
    )
    latent = encode(*made, kernel_in, kernel_mid, kernel_out.T)
    third = third_table()
    by_place = first_table()
    out = spectral_layer(
        latent,
        skip_weight,
        spectral.reshape(2, 16, 64, 64),
        jnp.asarray(halves(third)),
        jnp.asarray(halves(third.T)),
        jnp.asarray(halves(second_table())),
        jnp.asarray(placed(by_place)),
        jnp.asarray(placed(np.swapaxes(by_place, 2, 3))),
        jnp.asarray(pair_table().astype(ml_dtypes.bfloat16)),
    )
    return out.reshape(1, cells_x, cells_y, cells_z, -1)


def solution(mesh):
    in_specs = (
        P(None, None, ("gx", "gy", "gz")),
        P(None, "gx", "gy", "gz", None),
        P(None, "gx", "gy", "gz"),
        P(),
        P(),
        P(),
        P(None, "gz", "gx", "gy", None, None),
        P(),
    )
    out_specs = P(None, "gx", "gy", "gz", None)
    return jax.shard_map(body, mesh=mesh, in_specs=in_specs, out_specs=out_specs, check_vma=False)
```

```python
import functools
import math

import jax
import jax.numpy as jnp
import ml_dtypes
import numpy as np
from jax import lax
from jax.experimental import pallas as pl
from jax.experimental.pallas import tpu as pltpu
from jax.sharding import PartitionSpec as P

GRID = 64
MODES = 16
NB = 32
NORM_FLOOR = 1.0
GX, GY, GZ = 8, 4, 8
F32 = jnp.float32
BF16 = jnp.bfloat16
MESH = pl.DeviceIdType.MESH


def gelu(v):
    inner = v * (0.7978845608028654 + 0.035677408136300125 * (v * v))
    half = 0.5 * v
    return half + half * jnp.tanh(inner)


def twice_gelu(v):
    if not GELU16:
        return v + v * jnp.tanh(v * (0.7978845608028654 + 0.035677408136300125 * (v * v)))
    v = v.astype(BF16)
    inner = v * (BF16(0.7978845608028654) + BF16(0.035677408136300125) * (v * v))
    return v + v * jnp.tanh(inner)


SLOTS = 4
ROWS = 176
FOUR, SIX = 108, 162
GELU16 = True
OFFSETS = [(dx, dy, dz) for dx in (-1, 0, 1) for dy in (-1, 0, 1) for dz in (-1, 0, 1)]


def regroup(back):
    row = lax.broadcasted_iota(jnp.int32, (512, 512), 1 if back else 0)
    column = lax.broadcasted_iota(jnp.int32, (512, 512), 0 if back else 1)
    wanted = ((row >> 1) & 7) * 64 + (row >> 4) * 2 + (row & 1)
    return jnp.where(wanted == column, 1.0, 0.0).astype(BF16)


def halo_kernel(
    points_ref, near_ref, counts_ref, table_ref, slots_ref, blocks_ref, info_ref, rank_ref,
    main, send, recv,
):
    me_x = lax.axis_index("gx")
    me_y = lax.axis_index("gy")
    me_z = lax.axis_index("gz")

    def device(offset):
        dx, dy, dz = offset
        return {
            "gx": lax.rem(me_x + dx + GX, GX),
            "gy": lax.rem(me_y + dy + GY, GY),
            "gz": lax.rem(me_z + dz + GZ, GZ),
        }

    barrier = pltpu.get_barrier_semaphore()
    peers = [o for o in OFFSETS if o != (0, 0, 0)]
    for offset in peers:
        pl.semaphore_signal(barrier, inc=1, device_id=device(offset), device_id_type=MESH)

    main[13] = jnp.concatenate([points_ref[d] for d in range(6)] + [jnp.zeros((2, 512), F32)], axis=0).astype(BF16)
    pl.semaphore_wait(barrier, len(peers))
    for offset in sorted(peers, key=lambda o: -sum(abs(d) for d in o)):
        slot = 26 - OFFSETS.index(offset)
        pltpu.make_async_remote_copy(
            src_ref=main.at[13],
            dst_ref=main.at[slot],
            send_sem=send.at[0],
            recv_sem=recv.at[0],
            device_id=device(offset),
            device_id_type=MESH,
        ).start()
    everything = main.at[pl.ds(0, 26)]

    lane = lax.broadcasted_iota(jnp.int32, (1, 1024), 1)
    counts = jnp.concatenate([counts_ref[x].astype(F32) for x in range(8)], axis=1)
    counts = jnp.concatenate([counts[z : z + 1] for z in range(8)], axis=1)
    key = counts * 1024.0 + (1023 - lane).astype(F32)
    ones = jnp.ones((8, 128), BF16)
    rank = jnp.zeros((8, 1024), F32)
    for m in range(8):
        tall = jnp.broadcast_to(key[:, 128 * m : 128 * m + 128], (128, 128)).T
        ahead = jnp.concatenate(
            [
                jnp.where(tall > key[:, 128 * n : 128 * n + 128], 1.0, 0.0).astype(BF16)
                for n in range(8)
            ],
            axis=1,
        )
        rank = rank + jnp.dot(ones, ahead, preferred_element_type=F32)
    rank_ref[...] = rank
    near = jnp.concatenate(
        [near_ref[pl.ds(z, 128, stride=8), :].astype(F32).T for z in range(8)], axis=1
    ).astype(jnp.int32)
    owner = near >> 9
    part = near & 511
    block = ((((owner >> 5) - me_x + 1) * 3) + ((owner >> 3) & 3) - me_y + 1) * 3 + (owner & 7) - me_z + 1
    code = jnp.clip(block, 0, 26) * 2 + (part >> 8)
    place_y = (me_y * 16 + (lane & 15)).astype(F32)
    place_x = (me_x * 8 + ((lane >> 4) & 7)).astype(F32)
    place_z = (me_z * 8 + (lane >> 7)).astype(F32)
    centres = [-(place + 0.5) / GRID for place in (place_x, place_y, place_z)]
    rows = jnp.concatenate(
        [(part & 255).astype(F32), code.astype(F32), counts] + centres + [jnp.zeros((12, 1024), F32)], axis=0
    ).astype(BF16)
    order = lax.broadcasted_iota(jnp.int32, (128, 1024), 0).astype(F32)
    wide_rank = rank[0:1]
    for t in range(8):
        moved = jnp.where(order + 128.0 * t == wide_rank, 1.0, 0.0).astype(BF16)
        moved = lax.dot_general(rows, moved, (((1,), (1,)), ((), ())), preferred_element_type=F32)
        slots_ref[t] = moved[0:32].astype(jnp.int32)
        blocks_ref[t] = moved[32:64].astype(jnp.int32)
        info_ref[t] = moved[64:72]

    pltpu.make_async_copy(everything, everything, recv.at[0]).wait()
    blocks = [main[b].astype(F32) for b in range(27)]
    rows = [block[0:4] for block in blocks] + [block[4:6] for block in blocks]
    rows.append(jnp.zeros((ROWS - SIX, 512), F32))
    rows = jnp.concatenate(rows, axis=0).astype(BF16)
    table_ref[0:ROWS, :] = rows[:, 0:256]
    table_ref[ROWS : 2 * ROWS, :] = rows[:, 256:512]
    pltpu.make_async_copy(everything, everything, send.at[0]).wait()


def halo(points, near, counts):
    vmem = pl.BlockSpec(memory_space=pltpu.VMEM)
    return pl.pallas_call(
        halo_kernel,
        out_shape=[
            jax.ShapeDtypeStruct((2 * ROWS, 256), BF16),
            jax.ShapeDtypeStruct((8, NB, 128), jnp.int32),
            jax.ShapeDtypeStruct((8, NB, 128), jnp.int32),
            jax.ShapeDtypeStruct((8, 8, 128), F32),
            jax.ShapeDtypeStruct((8, 1024), F32),
        ],
        in_specs=[vmem] * 3,
        out_specs=[vmem] * 5,
        scratch_shapes=[
            pltpu.VMEM((27, 8, 512), BF16),
            pltpu.SemaphoreType.DMA((1,)),
            pltpu.SemaphoreType.DMA((1,)),
        ],
        compiler_params=pltpu.CompilerParams(collective_id=1, has_side_effects=True),
    )(points, near, counts)


def encoder_kernel(
    table_ref, slots_ref, blocks_ref, info_ref, rank_ref, in_ref, mid_ref, last_ref, out_ref,
    first_scr, mid_scr, last_scr, kept_scr, hidden_scr, base_scr, totals, trips,
):
    column = lax.broadcasted_iota(jnp.int32, (6, ROWS), 1)
    feature = lax.broadcasted_iota(jnp.int32, (6, ROWS), 0)
    wanted = jnp.where(column < FOUR, column % 4, 4 + column % 2)
    wanted = jnp.where(column >= SIX, column - SIX, wanted)
    chosen = jnp.where((feature == wanted) & (column < SIX + 3), 1.0, 0.0).astype(BF16)
    turn = (((0,), (0,)), ((), ()))
    first_scr[...] = lax.dot_general(in_ref[...], chosen, turn, preferred_element_type=F32).astype(BF16)
    half_mid = (mid_ref[...].astype(F32).T * 0.5).astype(BF16)
    mid_scr[...] = jnp.zeros(mid_scr.shape, BF16)
    mid_scr[0:80, 0:80] = half_mid
    mid_scr[80:160, 80:160] = half_mid
    last_scr[...] = last_ref[...]

    slot_ids = lax.broadcasted_iota(jnp.int32, (256, 128), 0).astype(jnp.int16)
    row = lax.broadcasted_iota(jnp.int32, (ROWS, 128), 0)
    row_block = jnp.where(row < FOUR, row // 4, jnp.where(row < SIX, (row - FOUR) // 2, -1)).astype(jnp.int16)
    last_rows = lax.broadcasted_iota(jnp.int32, (16, 128), 0)
    steps = 0
    for c in range(8):
        info = info_ref[c]
        trip = (jnp.max(info[0:1]).astype(jnp.int32) + SLOTS - 1) // SLOTS
        trips[c] = trip
        steps += trip
        centre = jnp.zeros((16, 128), F32)
        for d in range(3):
            centre = jnp.where(last_rows == SIX - ROWS + 16 + d, info[1 + d : 2 + d], centre)
        base_scr[c] = centre.astype(BF16)
        totals[c] = jnp.zeros((80, 128), F32)
    totals[8] = jnp.zeros((80, 128), F32)
    kept_scr[...] = jnp.zeros(kept_scr.shape, BF16)
    hidden_scr[...] = jnp.zeros(hidden_scr.shape, BF16)

    def step(n, places):
        (c0, t0), (c1, t1), (c2, t2) = places
        hidden = twice_gelu(jnp.dot(mid_scr[...], hidden_scr[...], preferred_element_type=F32))
        counts = info_ref[jnp.minimum(c2, 7), 0:1, :]
        total = totals[c2]
        for u in range(SLOTS):
            used = (SLOTS * t2 + u).astype(F32) < counts
            here = hidden[80 * (u // 2) : 80 * (u // 2) + 80, 128 * (u % 2) : 128 * (u % 2) + 128]
            total = total + jnp.where(used, here.astype(F32), 0.0)
        totals[c2] = total
        hidden = jnp.dot(first_scr[...], kept_scr[...], preferred_element_type=F32)
        hidden = twice_gelu(hidden).astype(BF16)
        for u in range(SLOTS // 2):
            hidden_scr[80 * u : 80 * u + 80, :] = hidden[:, 256 * u : 256 * u + 256]
        hot = []
        for u in range(SLOTS):
            slot = jnp.broadcast_to(slots_ref[c0, pl.ds(SLOTS * t0 + u, 1), :], (16, 128)).astype(jnp.int16)
            slot = jnp.concatenate([slot] * 16, axis=0)
            hot.append(jnp.where(slot_ids == slot, BF16(1), BF16(0)))
        found = jnp.dot(table_ref[...], jnp.concatenate(hot, axis=1), preferred_element_type=F32)
        found = found.astype(BF16)
        for u in range(SLOTS):
            code = jnp.broadcast_to(blocks_ref[c0, pl.ds(SLOTS * t0 + u, 1), :], (16, 128))
            block = (code >> 1).astype(jnp.int16)
            odd = (code & 1).astype(jnp.int16)
            same = row_block == jnp.concatenate([block] * (ROWS // 16), axis=0)
            odd = jnp.concatenate([odd] * (ROWS // 16), axis=0) == 1
            here = found[:, 128 * u : 128 * u + 128]
            here = jnp.where(odd, here[ROWS : 2 * ROWS], here[0:ROWS])
            kept_scr[0 : ROWS - 16, 128 * u : 128 * u + 128] = jnp.where(same[0 : ROWS - 16], here[0 : ROWS - 16], BF16(0))
            kept_scr[ROWS - 16 : ROWS, 128 * u : 128 * u + 128] = jnp.where(same[ROWS - 16 : ROWS], here[ROWS - 16 : ROWS], base_scr[c0])
        ended = t0 + 1 >= trips[c0]
        following = (
            jnp.minimum(jnp.where(ended, c0 + 1, c0), 7),
            jnp.where(ended, jnp.where(c0 == 7, t0, 0), t0 + 1),
        )
        return following, (c0, t0), (c1, t1)

    start = (jnp.int32(0), jnp.int32(0))
    spare = (jnp.int32(8), jnp.int32(0))
    lax.fori_loop(0, steps + 2, step, (start, spare, spare))
    last = last_scr[...]
    ordered = []
    for c in range(8):
        mean = totals[c] * (0.5 / info_ref[c, 0:1, :])
        upper = mean.astype(BF16)
        lower = (mean - upper.astype(F32)).astype(BF16)
        values = jnp.dot(last, upper, preferred_element_type=F32) + jnp.dot(
            last, lower, preferred_element_type=F32
        )
        ordered.append(values.astype(BF16))
    ordered = jnp.concatenate(ordered, axis=1)
    order = lax.broadcasted_iota(jnp.int32, (1024, 128), 0).astype(F32)
    parts = []
    for t in range(8):
        moved = jnp.where(order == rank_ref[0:1, 128 * t : 128 * t + 128], 1.0, 0.0).astype(BF16)
        parts.append(jnp.dot(ordered, moved, preferred_element_type=F32).astype(BF16))
    parts = jnp.dot(regroup(False), jnp.concatenate(parts, axis=0), preferred_element_type=F32)
    out_ref[...] = parts.astype(BF16).reshape(32, 16, 128)


def encode(table, slots, blocks, info, rank, kernel_in, kernel_mid, kernel_out):
    vmem = pl.BlockSpec(memory_space=pltpu.VMEM)
    return pl.pallas_call(
        encoder_kernel,
        out_shape=jax.ShapeDtypeStruct((32, 16, 128), BF16),
        in_specs=[vmem] * 8,
        out_specs=vmem,
        scratch_shapes=[
            pltpu.VMEM((80, ROWS), BF16),
            pltpu.VMEM((160, 160), BF16),
            pltpu.VMEM((64, 80), BF16),
            pltpu.VMEM((ROWS, 128 * SLOTS), BF16),
            pltpu.VMEM((160, 256), BF16),
            pltpu.VMEM((8, 16, 128), BF16),
            pltpu.VMEM((9, 80, 128), F32),
            pltpu.SMEM((8,), jnp.int32),
        ],
    )(table, slots, blocks, info, rank, kernel_in, kernel_mid, kernel_out)


def halves(values):
    upper = values.astype(np.float32).astype(ml_dtypes.bfloat16)
    lower = (values - upper.astype(np.float64)).astype(np.float32).astype(ml_dtypes.bfloat16)
    return np.stack([upper, lower])


def turn(frequency, position):
    angle = 2.0 * math.pi * ((frequency * position) % GRID) / GRID
    return np.cos(angle), np.sin(angle)


def centred(index):
    return np.where(index < MODES // 2, index, index - MODES)


def complex_block(cos, sin):
    return np.stack([np.stack([cos, sin], -1), np.stack([-sin, cos], -1)], -2)


@functools.lru_cache(None)
def third_table():
    cos, sin = turn(np.arange(16)[:, None], np.arange(64)[None, :])
    full = np.einsum("akz,cd->akczd", np.stack([cos, -sin]), np.eye(2))
    return full.reshape(64, 128)


@functools.lru_cache(None)
def second_table():
    j = np.arange(16)
    cos, sin = turn(centred(j)[:, None], np.arange(64)[None, :])
    both = complex_block(cos, sin).reshape(8, 2, 4, 16, 2, 2)
    full = np.einsum("gleyab,xw->lgaxebwy", both, np.eye(8))
    return full.reshape(2, 128, 1024)


@functools.lru_cache(None)
def first_table():
    i = np.arange(16)
    cos, sin = turn(centred(i)[:, None], np.arange(64)[None, :])
    both = complex_block(cos, sin).reshape(8, 2, 8, 8, 2, 2)
    return np.einsum("hltxab->tlhabx", both).reshape(8, 2, 16, 16)


def placed(values):
    return np.tile(np.moveaxis(halves(values), 0, 1), (1, 1, 1, 1, 8))


@functools.lru_cache(None)
def pair_table():
    out = np.zeros((4, 8, 8, 2, 8, 8, 2))
    for il in range(2):
        for jl in range(2):
            for h in range(8):
                for g in range(8):
                    i, j = 2 * h + il, 2 * g + jl
                    if i == 8 or j == 8:
                        continue
                    ni, nj = (16 - i) % 16, (16 - j) % 16
                    assert ni % 2 == il and nj % 2 == jl
                    for a in range(2):
                        out[2 * il + jl, g, h, a, nj // 2, ni // 2, a] = 1.0 - 2.0 * a
    return out.reshape(4, 128, 128)


def dotf(a, b):
    return jnp.dot(a, b, preferred_element_type=F32)


def dott(a, b):
    return lax.dot_general(a, b, (((1,), (1,)), ((), ())), preferred_element_type=F32)


def split(values):
    upper = values.astype(BF16)
    return upper, (values - upper.astype(F32)).astype(BF16)


def spectral_kernel(
    latent_ref, weight_any, third_any, back_any, second_any, first_any, firstt_any, pair_any,
    out_ref,
    weight_ref, third_ref, back_ref, second_ref, first_ref, firstt_ref, pair_ref,
    r1, w_msg, rw, s_msg, r3, mixing, mixed_scr, n_msg, r5, g_msg, r6, b_msg, r8, send, recv, loaded,
):
    me_x = lax.axis_index("gx")
    me_y = lax.axis_index("gy")
    me_z = lax.axis_index("gz")
    me_q = me_y * GZ + me_z
    columns = [(y, z) for y in range(GY) for z in range(GZ) if y or z]
    columns.sort(key=lambda o: -(2 * min(o[0], GY - o[0]) + min(o[1], GZ - o[1])))

    def across(o):
        y, z = lax.rem(me_y + o[0], GY), lax.rem(me_z + o[1], GZ)
        return {"gy": y, "gz": z}, y * GZ + z, me_q

    def along_x(o):
        peer = lax.rem(me_x + o, GX)
        return {"gx": peer}, peer, me_x

    planes = [across(o) for o in columns]
    lines = [along_x(o) for o in (4, 3, 5, 2, 6, 1, 7)]
    barrier = pltpu.get_barrier_semaphore()
    for device, _, _ in lines + planes:
        pl.semaphore_signal(barrier, inc=1, device_id=device, device_id_type=MESH)
    constants = (weight_any, third_any, back_any, second_any, first_any, firstt_any, pair_any)
    copies = (weight_ref, third_ref, back_ref, second_ref, first_ref, firstt_ref, pair_ref)
    loads = [pltpu.make_async_copy(c, d, loaded.at[n]) for n, (c, d) in enumerate(zip(constants, copies))]
    for load in loads:
        load.start()
    pl.semaphore_wait(barrier, len(planes + lines))

    sends = []

    def start(stage, peers, source, target):
        for device, peer, me in peers:
            pltpu.make_async_remote_copy(
                src_ref=source(peer),
                dst_ref=target.at[me],
                send_sem=send.at[stage],
                recv_sem=recv.at[stage],
                device_id=device,
                device_id_type=MESH,
            ).start()
        everything = target.at[pl.ds(0, len(peers))]
        sends.append((stage, everything))
        return stage, everything

    def finish(pending):
        stage, everything = pending
        pltpu.make_async_copy(everything, everything, recv.at[stage]).wait()

    rows128 = lax.broadcasted_iota(jnp.int32, (128, 128), 0)
    lanes128 = lax.broadcasted_iota(jnp.int32, (128, 128), 1)
    same = rows128 // 16 == lanes128 // 16

    def spread_blocks(ref, part, l):
        small = ref[me_x, part, l].astype(F32)
        return jnp.where(same, jnp.concatenate([small] * 8, axis=0), 0.0).astype(BF16)

    first = start(0, planes, lambda p: latent_ref.at[p], r1)
    r1[me_q] = latent_ref[me_q]
    loads[0].wait()
    forth = regroup(False)
    for l in range(2):
        wide = jnp.concatenate(
            [weight_ref[b, 8 * l : 8 * l + 8].astype(F32).reshape(512, 64) for b in range(2)], axis=1
        ).astype(BF16)
        w_msg[:, 16 * l : 16 * l + 16, :] = dotf(forth, wide).astype(BF16).reshape(32, 16, 128)
    weights = start(1, planes, lambda p: w_msg.at[p], rw)
    rw[me_q] = w_msg[me_q]
    for load in loads[1:]:
        load.wait()
    first_tab = [[spread_blocks(first_ref, p, l) for l in range(2)] for p in range(2)]
    back_tab = [[spread_blocks(firstt_ref, p, l) for l in range(2)] for p in range(2)]
    finish(first)

    pieces = []
    for e in range(4):
        values = r1[8 * e : 8 * e + 8].reshape(128, 128)
        piece = dotf(third_ref[0], values) + dotf(third_ref[1], values)
        pieces += [piece[0:32], piece[32:64]]
    wide = jnp.concatenate(pieces, axis=1).astype(BF16)
    rows = jnp.concatenate(
        [dott(second_ref[0, l], wide) + dott(second_ref[1, l], wide) for l in range(2)], axis=1
    )
    upper, lower = split(rows)
    partial = jnp.concatenate(
        [
            dotf(first_tab[0][l], upper) + dotf(first_tab[0][l], lower) + dotf(first_tab[1][l], upper)
            for l in range(2)
        ],
        axis=1,
    )
    s_msg[...] = partial.astype(BF16).reshape(8, 16, 128)

    third = start(2, lines, lambda p: s_msg.at[p], r3)
    r3[me_x] = s_msg[me_x]
    finish(weights)
    for h in range(8):
        parts = [
            rw[e * 8 + h, 8 * p : 8 * p + 8, :].astype(F32) for p in range(4) for e in range(4)
        ]
        mixing[h] = jnp.concatenate(parts, axis=0).T.astype(BF16)
    finish(third)
    modes = jnp.sum(r3[...].astype(F32), axis=0)

    own = rows128 // 2 == lanes128 // 2
    even = lax.broadcasted_iota(jnp.int32, (64, 128), 1) % 2 == 0
    products = []
    for h in range(8):
        expanded = jnp.concatenate(
            [
                jnp.where(own, jnp.broadcast_to(modes[2 * h + a : 2 * h + a + 1], (128, 128)), 0.0)
                for a in range(2)
            ],
            axis=0,
        ).astype(BF16)
        products.append(dott(mixing[h], expanded))
    for h, product in enumerate(products):
        mixed_scr[h, 0:64] = product[0:64, 0:128] - product[64:128, 128:256]
        mixed_scr[h, 64:128] = product[64:128, 0:128] + product[0:64, 128:256]
    turned = [
        jnp.where(even, mixed_scr[h, pl.ds(0, 64, stride=2), :], mixed_scr[h, pl.ds(1, 64, stride=2), :])
        for h in range(8)
    ]
    place = lax.broadcasted_iota(jnp.int32, (512, 512), 0)
    source = lax.broadcasted_iota(jnp.int32, (512, 512), 1)
    wanted = ((place >> 1) & 7) * 64 + (place & 1) * 32 + (place >> 4)
    order = jnp.where(wanted == source, 1.0, 0.0).astype(BF16)
    turned = jnp.concatenate(turned, axis=0).astype(BF16)
    n_msg[...] = dotf(order, turned).astype(BF16).reshape(32, 16, 128)

    fourth = start(3, planes, lambda p: n_msg.at[p], r5)
    r5[me_q] = n_msg[me_q]
    finish(fourth)
    mixed = jnp.sum(r5[...].astype(F32), axis=0)
    zero_rows = lax.broadcasted_iota(jnp.int32, (16, 128), 0)
    zero_lanes = lax.broadcasted_iota(jnp.int32, (16, 128), 1)
    mixed = jnp.where((zero_rows < 2) & (zero_lanes < 2) & (me_x == 0), 0.0, mixed)
    g_msg[...] = mixed.astype(BF16)

    fifth = start(4, lines, lambda p: g_msg, r6)
    r6[me_x] = g_msg[...]
    finish(fifth)
    field = r6[...].reshape(128, 128)
    along = (
        dotf(back_tab[0][0], field[:, 0:64])
        + dotf(back_tab[1][0], field[:, 0:64])
        + dotf(back_tab[0][1], field[:, 64:128])
        + dotf(back_tab[1][1], field[:, 64:128])
    )
    upper, lower = split(along.T)
    plane = (
        dotf(upper[0:32], second_ref[0, 0])
        + dotf(lower[0:32], second_ref[0, 0])
        + dotf(upper[0:32], second_ref[1, 0])
        + dotf(upper[32:64], second_ref[0, 1])
        + dotf(lower[32:64], second_ref[0, 1])
        + dotf(upper[32:64], second_ref[1, 1])
    )
    scale = 1.0 / GRID**3
    plane_rows = lax.broadcasted_iota(jnp.int32, (32, 1024), 0)
    plane = (plane * jnp.where(plane_rows < 2, scale, 2.0 * scale)).astype(BF16)
    wide_field = field.astype(F32)
    paired = jnp.zeros((128, 128), F32)
    for p in range(4):
        paired = jnp.where(lanes128 // 32 == p, dotf(pair_ref[p], field), paired)
    low = (lanes128 // 2) % 16 == 0
    power = jnp.where(low, 0.5 * wide_field * (wide_field + paired), 2.0 * wide_field * wide_field)
    power = jnp.sum(power, axis=0, keepdims=True)
    for shift in (64, 32, 16, 8, 4, 2):
        power = power + pltpu.roll(power, shift, 1)
    variance = jnp.broadcast_to(power, (128, 128)).T * (scale * scale)
    inverse = 1.0 / jnp.sqrt(variance + NORM_FLOOR)
    for e in range(4):
        part = jnp.concatenate(
            [plane[:, (2 * e + b) * 128 : (2 * e + b + 1) * 128] for b in range(2)], axis=0
        )
        branch = (dotf(back_ref[0], part) + dotf(back_ref[1], part)) * inverse
        b_msg[8 * e : 8 * e + 8] = branch.astype(BF16).reshape(8, 16, 128)

    sixth = start(5, planes, lambda p: b_msg.at[p], r8)
    r8[me_q] = b_msg[me_q]
    finish(sixth)
    out_ref[...] = r8[...]
    for stage, everything in sends:
        pltpu.make_async_copy(everything, everything, send.at[stage]).wait()


def final_kernel(branch_ref, latent_ref, skip_ref, out_ref):
    skip_t = skip_ref[...].astype(F32).T.astype(BF16)
    both = jnp.concatenate([branch_ref[...].reshape(512, 128), latent_ref[...].reshape(512, 128)], axis=1)
    both = dotf(regroup(True), both)
    skip = both[:, 128:256].astype(BF16)
    for z in range(8):
        cells = both[64 * z : 64 * z + 64, 0:128] + dotf(skip_t, skip[64 * z : 64 * z + 64])
        out_ref[:, z, :] = gelu(cells).T


def final(branch, latent, skip_w):
    vmem = pl.BlockSpec(memory_space=pltpu.VMEM)
    return pl.pallas_call(
        final_kernel,
        out_shape=jax.ShapeDtypeStruct((128, 8, 64), F32),
        in_specs=[vmem] * 3,
        out_specs=vmem,
    )(branch, latent, skip_w)


def spectral_layer(latent, weight, *tables):
    vmem = pl.BlockSpec(memory_space=pltpu.VMEM)
    own = [pltpu.VMEM(array.shape, array.dtype) for array in (weight,) + tables]
    return pl.pallas_call(
        spectral_kernel,
        out_shape=jax.ShapeDtypeStruct((32, 16, 128), BF16),
        in_specs=[vmem] + [pl.BlockSpec(memory_space=pl.ANY)] * 7,
        out_specs=vmem,
        scratch_shapes=own
        + [
            pltpu.VMEM((32, 16, 128), BF16),
            pltpu.VMEM((32, 32, 128), BF16),
            pltpu.VMEM((32, 32, 128), BF16),
            pltpu.VMEM((8, 16, 128), BF16),
            pltpu.VMEM((8, 16, 128), BF16),
            pltpu.VMEM((8, 128, 128), BF16),
            pltpu.VMEM((8, 128, 128), F32),
            pltpu.VMEM((32, 16, 128), BF16),
            pltpu.VMEM((32, 16, 128), BF16),
            pltpu.VMEM((16, 128), BF16),
            pltpu.VMEM((8, 16, 128), BF16),
            pltpu.VMEM((32, 16, 128), BF16),
            pltpu.VMEM((32, 16, 128), BF16),
            pltpu.SemaphoreType.DMA((6,)),
            pltpu.SemaphoreType.DMA((6,)),
            pltpu.SemaphoreType.DMA((7,)),
        ],
        compiler_params=pltpu.CompilerParams(collective_id=0, has_side_effects=True),
    )(latent, weight, *tables)


def body(point_data, neighbours, counts, kernel_in, kernel_mid, kernel_out, spectral, skip_weight):
    cells_x, cells_y, cells_z = neighbours.shape[1:4]
    made = halo(
        jnp.transpose(point_data, (1, 0, 2)),
        neighbours.reshape(-1, NB),
        jnp.transpose(counts[0], (0, 2, 1)),
    )
    latent = encode(*made, kernel_in, kernel_mid, kernel_out.T)
    third = third_table()
    by_place = first_table()
    branch = spectral_layer(
        latent,
        spectral.reshape(2, 16, 64, 64),
        jnp.asarray(halves(third)),
        jnp.asarray(halves(third.T)),
        jnp.asarray(halves(second_table())),
        jnp.asarray(placed(by_place)),
        jnp.asarray(placed(np.swapaxes(by_place, 2, 3))),
        jnp.asarray(pair_table().astype(ml_dtypes.bfloat16)),
    )
    out = final(branch, latent, skip_weight)
    return out.reshape(1, cells_x, cells_y, cells_z, -1)


def solution(mesh):
    in_specs = (
        P(None, None, ("gx", "gy", "gz")),
        P(None, "gx", "gy", "gz", None),
        P(None, "gx", "gy", "gz"),
        P(),
        P(),
        P(),
        P(None, "gz", "gx", "gy", None, None),
        P(),
    )
    out_specs = P(None, "gx", "gy", "gz", None)
    return jax.shard_map(body, mesh=mesh, in_specs=in_specs, out_specs=out_specs, check_vma=False)
```

```python
import functools
import math

import jax
import jax.numpy as jnp
import ml_dtypes
import numpy as np
from jax import lax
from jax.experimental import pallas as pl
from jax.experimental.pallas import tpu as pltpu
from jax.sharding import PartitionSpec as P

GRID = 64
MODES = 16
NB = 32
NORM_FLOOR = 1.0
GX, GY, GZ = 8, 4, 8
F32 = jnp.float32
BF16 = jnp.bfloat16
MESH = pl.DeviceIdType.MESH


def gelu(v):
    inner = v * (0.7978845608028654 + 0.035677408136300125 * (v * v))
    half = 0.5 * v
    return half + half * jnp.tanh(inner)


def twice_gelu(v):
    if not GELU16:
        return v + v * jnp.tanh(v * (0.7978845608028654 + 0.035677408136300125 * (v * v)))
    v = v.astype(BF16)
    inner = v * (BF16(0.7978845608028654) + BF16(0.035677408136300125) * (v * v))
    return v + v * jnp.tanh(inner)


SLOTS = 4
ROWS = 176
FOUR, SIX = 108, 162
GELU16 = True
OFFSETS = [(dx, dy, dz) for dx in (-1, 0, 1) for dy in (-1, 0, 1) for dz in (-1, 0, 1)]


def regroup():
    row = lax.broadcasted_iota(jnp.int32, (512, 512), 0)
    column = lax.broadcasted_iota(jnp.int32, (512, 512), 1)
    wanted = ((row >> 1) & 7) * 64 + (row >> 4) * 2 + (row & 1)
    return jnp.where(wanted == column, 1.0, 0.0).astype(BF16)


def halo_kernel(
    points_ref, near_ref, counts_ref, table_ref, slots_ref, blocks_ref, info_ref, rank_ref,
    main, send, recv,
):
    me_x = lax.axis_index("gx")
    me_y = lax.axis_index("gy")
    me_z = lax.axis_index("gz")

    def device(offset):
        dx, dy, dz = offset
        return {
            "gx": lax.rem(me_x + dx + GX, GX),
            "gy": lax.rem(me_y + dy + GY, GY),
            "gz": lax.rem(me_z + dz + GZ, GZ),
        }

    barrier = pltpu.get_barrier_semaphore()
    peers = [o for o in OFFSETS if o != (0, 0, 0)]
    for offset in peers:
        pl.semaphore_signal(barrier, inc=1, device_id=device(offset), device_id_type=MESH)

    main[13] = jnp.concatenate([points_ref[d] for d in range(6)] + [jnp.zeros((2, 512), F32)], axis=0).astype(BF16)
    pl.semaphore_wait(barrier, len(peers))
    for offset in sorted(peers, key=lambda o: -sum(abs(d) for d in o)):
        slot = 26 - OFFSETS.index(offset)
        pltpu.make_async_remote_copy(
            src_ref=main.at[13],
            dst_ref=main.at[slot],
            send_sem=send.at[0],
            recv_sem=recv.at[0],
            device_id=device(offset),
            device_id_type=MESH,
        ).start()
    everything = main.at[pl.ds(0, 26)]

    lane = lax.broadcasted_iota(jnp.int32, (1, 1024), 1)
    counts = jnp.concatenate([counts_ref[x].astype(F32) for x in range(8)], axis=1)
    counts = jnp.concatenate([counts[z : z + 1] for z in range(8)], axis=1)
    key = counts * 1024.0 + (1023 - lane).astype(F32)
    ones = jnp.ones((8, 128), BF16)
    rank = jnp.zeros((8, 1024), F32)
    for m in range(8):
        tall = jnp.broadcast_to(key[:, 128 * m : 128 * m + 128], (128, 128)).T
        ahead = jnp.concatenate(
            [
                jnp.where(tall > key[:, 128 * n : 128 * n + 128], 1.0, 0.0).astype(BF16)
                for n in range(8)
            ],
            axis=1,
        )
        rank = rank + jnp.dot(ones, ahead, preferred_element_type=F32)
    rank_ref[...] = rank
    near = jnp.concatenate(
        [near_ref[pl.ds(z, 128, stride=8), :].astype(F32).T for z in range(8)], axis=1
    ).astype(jnp.int32)
    owner = near >> 9
    part = near & 511
    block = ((((owner >> 5) - me_x + 1) * 3) + ((owner >> 3) & 3) - me_y + 1) * 3 + (owner & 7) - me_z + 1
    code = jnp.clip(block, 0, 26) * 2 + (part >> 8)
    place_y = (me_y * 16 + (lane & 15)).astype(F32)
    place_x = (me_x * 8 + ((lane >> 4) & 7)).astype(F32)
    place_z = (me_z * 8 + (lane >> 7)).astype(F32)
    centres = [-(place + 0.5) / GRID for place in (place_x, place_y, place_z)]
    rows = jnp.concatenate(
        [(part & 255).astype(F32), code.astype(F32), counts] + centres + [jnp.zeros((12, 1024), F32)], axis=0
    ).astype(BF16)
    order = lax.broadcasted_iota(jnp.int32, (128, 1024), 0).astype(F32)
    wide_rank = rank[0:1]
    for t in range(8):
        moved = jnp.where(order + 128.0 * t == wide_rank, 1.0, 0.0).astype(BF16)
        moved = lax.dot_general(rows, moved, (((1,), (1,)), ((), ())), preferred_element_type=F32)
        slots_ref[t] = moved[0:32].astype(jnp.int32)
        blocks_ref[t] = moved[32:64].astype(jnp.int32)
        info_ref[t] = moved[64:72]

    pltpu.make_async_copy(everything, everything, recv.at[0]).wait()
    blocks = [main[b].astype(F32) for b in range(27)]
    rows = [block[0:4] for block in blocks] + [block[4:6] for block in blocks]
    rows.append(jnp.zeros((ROWS - SIX, 512), F32))
    rows = jnp.concatenate(rows, axis=0).astype(BF16)
    table_ref[0:ROWS, :] = rows[:, 0:256]
    table_ref[ROWS : 2 * ROWS, :] = rows[:, 256:512]
    pltpu.make_async_copy(everything, everything, send.at[0]).wait()


def halo(points, near, counts):
    vmem = pl.BlockSpec(memory_space=pltpu.VMEM)
    return pl.pallas_call(
        halo_kernel,
        out_shape=[
            jax.ShapeDtypeStruct((2 * ROWS, 256), BF16),
            jax.ShapeDtypeStruct((8, NB, 128), jnp.int32),
            jax.ShapeDtypeStruct((8, NB, 128), jnp.int32),
            jax.ShapeDtypeStruct((8, 8, 128), F32),
            jax.ShapeDtypeStruct((8, 1024), F32),
        ],
        in_specs=[vmem] * 3,
        out_specs=[vmem] * 5,
        scratch_shapes=[
            pltpu.VMEM((27, 8, 512), BF16),
            pltpu.SemaphoreType.DMA((1,)),
            pltpu.SemaphoreType.DMA((1,)),
        ],
        compiler_params=pltpu.CompilerParams(collective_id=1, has_side_effects=True),
    )(points, near, counts)


def encoder_kernel(
    table_ref, slots_ref, blocks_ref, info_ref, in_ref, mid_ref, last_ref, out_ref,
    first_scr, mid_scr, last_scr, kept_scr, hidden_scr, base_scr, totals, trips,
):
    column = lax.broadcasted_iota(jnp.int32, (6, ROWS), 1)
    feature = lax.broadcasted_iota(jnp.int32, (6, ROWS), 0)
    wanted = jnp.where(column < FOUR, column % 4, 4 + column % 2)
    wanted = jnp.where(column >= SIX, column - SIX, wanted)
    chosen = jnp.where((feature == wanted) & (column < SIX + 3), 1.0, 0.0).astype(BF16)
    turn = (((0,), (0,)), ((), ()))
    first_scr[...] = lax.dot_general(in_ref[...], chosen, turn, preferred_element_type=F32).astype(BF16)
    half_mid = (mid_ref[...].astype(F32).T * 0.5).astype(BF16)
    mid_scr[...] = jnp.zeros(mid_scr.shape, BF16)
    mid_scr[0:80, 0:80] = half_mid
    mid_scr[80:160, 80:160] = half_mid
    last_scr[...] = last_ref[...]

    slot_ids = lax.broadcasted_iota(jnp.int32, (256, 128), 0).astype(jnp.int16)
    row = lax.broadcasted_iota(jnp.int32, (ROWS, 128), 0)
    row_block = jnp.where(row < FOUR, row // 4, jnp.where(row < SIX, (row - FOUR) // 2, -1)).astype(jnp.int16)
    last_rows = lax.broadcasted_iota(jnp.int32, (16, 128), 0)
    steps = 0
    for c in range(8):
        info = info_ref[c]
        trip = (jnp.max(info[0:1]).astype(jnp.int32) + SLOTS - 1) // SLOTS
        trips[c] = trip
        steps += trip
        centre = jnp.zeros((16, 128), F32)
        for d in range(3):
            centre = jnp.where(last_rows == SIX - ROWS + 16 + d, info[1 + d : 2 + d], centre)
        base_scr[c] = centre.astype(BF16)
        totals[c] = jnp.zeros((80, 128), F32)
    totals[8] = jnp.zeros((80, 128), F32)
    kept_scr[...] = jnp.zeros(kept_scr.shape, BF16)
    hidden_scr[...] = jnp.zeros(hidden_scr.shape, BF16)

    def step(n, places):
        (c0, t0), (c1, t1), (c2, t2) = places
        hidden = twice_gelu(jnp.dot(mid_scr[...], hidden_scr[...], preferred_element_type=F32))
        counts = info_ref[jnp.minimum(c2, 7), 0:1, :]
        total = totals[c2]
        for u in range(SLOTS):
            used = (SLOTS * t2 + u).astype(F32) < counts
            here = hidden[80 * (u // 2) : 80 * (u // 2) + 80, 128 * (u % 2) : 128 * (u % 2) + 128]
            total = total + jnp.where(used, here.astype(F32), 0.0)
        totals[c2] = total
        hidden = jnp.dot(first_scr[...], kept_scr[...], preferred_element_type=F32)
        hidden = twice_gelu(hidden).astype(BF16)
        for u in range(SLOTS // 2):
            hidden_scr[80 * u : 80 * u + 80, :] = hidden[:, 256 * u : 256 * u + 256]
        hot = []
        for u in range(SLOTS):
            slot = jnp.broadcast_to(slots_ref[c0, pl.ds(SLOTS * t0 + u, 1), :], (16, 128)).astype(jnp.int16)
            slot = jnp.concatenate([slot] * 16, axis=0)
            hot.append(jnp.where(slot_ids == slot, BF16(1), BF16(0)))
        found = jnp.dot(table_ref[...], jnp.concatenate(hot, axis=1), preferred_element_type=F32)
        found = found.astype(BF16)
        for u in range(SLOTS):
            code = jnp.broadcast_to(blocks_ref[c0, pl.ds(SLOTS * t0 + u, 1), :], (16, 128))
            block = (code >> 1).astype(jnp.int16)
            odd = (code & 1).astype(jnp.int16)
            same = row_block == jnp.concatenate([block] * (ROWS // 16), axis=0)
            odd = jnp.concatenate([odd] * (ROWS // 16), axis=0) == 1
            here = found[:, 128 * u : 128 * u + 128]
            here = jnp.where(odd, here[ROWS : 2 * ROWS], here[0:ROWS])
            kept_scr[0 : ROWS - 16, 128 * u : 128 * u + 128] = jnp.where(same[0 : ROWS - 16], here[0 : ROWS - 16], BF16(0))
            kept_scr[ROWS - 16 : ROWS, 128 * u : 128 * u + 128] = jnp.where(same[ROWS - 16 : ROWS], here[ROWS - 16 : ROWS], base_scr[c0])
        ended = t0 + 1 >= trips[c0]
        following = (
            jnp.minimum(jnp.where(ended, c0 + 1, c0), 7),
            jnp.where(ended, jnp.where(c0 == 7, t0, 0), t0 + 1),
        )
        return following, (c0, t0), (c1, t1)

    start = (jnp.int32(0), jnp.int32(0))
    spare = (jnp.int32(8), jnp.int32(0))
    lax.fori_loop(0, steps + 2, step, (start, spare, spare))
    last = last_scr[...]
    ordered = []
    for c in range(8):
        mean = totals[c] * (0.5 / info_ref[c, 0:1, :])
        upper = mean.astype(BF16)
        lower = (mean - upper.astype(F32)).astype(BF16)
        values = jnp.dot(last, upper, preferred_element_type=F32) + jnp.dot(
            last, lower, preferred_element_type=F32
        )
        ordered.append(values.astype(BF16))
    out_ref[...] = jnp.concatenate(ordered, axis=1)


def encode(table, slots, blocks, info, kernel_in, kernel_mid, kernel_out):
    vmem = pl.BlockSpec(memory_space=pltpu.VMEM)
    return pl.pallas_call(
        encoder_kernel,
        out_shape=jax.ShapeDtypeStruct((64, 1024), BF16),
        in_specs=[vmem] * 7,
        out_specs=vmem,
        scratch_shapes=[
            pltpu.VMEM((80, ROWS), BF16),
            pltpu.VMEM((160, 160), BF16),
            pltpu.VMEM((64, 80), BF16),
            pltpu.VMEM((ROWS, 128 * SLOTS), BF16),
            pltpu.VMEM((160, 256), BF16),
            pltpu.VMEM((8, 16, 128), BF16),
            pltpu.VMEM((9, 80, 128), F32),
            pltpu.SMEM((8,), jnp.int32),
        ],
    )(table, slots, blocks, info, kernel_in, kernel_mid, kernel_out)


def halves(values):
    upper = values.astype(np.float32).astype(ml_dtypes.bfloat16)
    lower = (values - upper.astype(np.float64)).astype(np.float32).astype(ml_dtypes.bfloat16)
    return np.stack([upper, lower])


def turn(frequency, position):
    angle = 2.0 * math.pi * ((frequency * position) % GRID) / GRID
    return np.cos(angle), np.sin(angle)


def centred(index):
    return np.where(index < MODES // 2, index, index - MODES)


def complex_block(cos, sin):
    return np.stack([np.stack([cos, sin], -1), np.stack([-sin, cos], -1)], -2)


@functools.lru_cache(None)
def third_table():
    cos, sin = turn(np.arange(16)[:, None], np.arange(64)[None, :])
    parts = np.stack([cos, -sin]).reshape(2, 16, 8, 8)
    full = np.einsum("akgz,cd->akcgdz", parts, np.eye(2))
    return full.reshape(64, 128)


@functools.lru_cache(None)
def second_table():
    j = np.arange(16)
    cos, sin = turn(centred(j)[:, None], np.arange(64)[None, :])
    both = complex_block(cos, sin).reshape(8, 2, 4, 16, 2, 2)
    full = np.einsum("gleyab,xw->lgaxebwy", both, np.eye(8))
    return full.reshape(2, 128, 1024)


@functools.lru_cache(None)
def first_table():
    i = np.arange(16)
    cos, sin = turn(centred(i)[:, None], np.arange(64)[None, :])
    both = complex_block(cos, sin).reshape(8, 2, 8, 8, 2, 2)
    return np.einsum("hltxab->tlhabx", both).reshape(8, 2, 16, 16)


def placed(values):
    return np.tile(np.moveaxis(halves(values), 0, 1), (1, 1, 1, 1, 8))


@functools.lru_cache(None)
def pair_table():
    out = np.zeros((4, 8, 8, 2, 8, 8, 2))
    for il in range(2):
        for jl in range(2):
            for h in range(8):
                for g in range(8):
                    i, j = 2 * h + il, 2 * g + jl
                    if i == 8 or j == 8:
                        continue
                    ni, nj = (16 - i) % 16, (16 - j) % 16
                    assert ni % 2 == il and nj % 2 == jl
                    for a in range(2):
                        out[2 * il + jl, g, h, a, nj // 2, ni // 2, a] = 1.0 - 2.0 * a
    return out.reshape(4, 128, 128)


def dotf(a, b):
    return jnp.dot(a, b, preferred_element_type=F32)


def dott(a, b):
    return lax.dot_general(a, b, (((1,), (1,)), ((), ())), preferred_element_type=F32)


def split(values):
    upper = values.astype(BF16)
    return upper, (values - upper.astype(F32)).astype(BF16)


def spectral_kernel(
    ordered_ref, rank_ref, skip_ref, weight_any, third_any, back_any, second_any, first_any, firstt_any, pair_any,
    out_ref,
    weight_ref, third_ref, back_ref, second_ref, first_ref, firstt_ref, pair_ref,
    latent, l_msg, r1, w_msg, rw, s_msg, r3, mixing, mixed_scr, n_msg, r5, g_msg, r6, b_msg, r8, ended, skip,
    send, recv, loaded,
):
    me_x = lax.axis_index("gx")
    me_y = lax.axis_index("gy")
    me_z = lax.axis_index("gz")
    me_q = me_y * GZ + me_z
    columns = [(y, z) for y in range(GY) for z in range(GZ) if y or z]
    columns.sort(key=lambda o: -(2 * min(o[0], GY - o[0]) + min(o[1], GZ - o[1])))

    def across(o):
        y, z = lax.rem(me_y + o[0], GY), lax.rem(me_z + o[1], GZ)
        return {"gy": y, "gz": z}, y * GZ + z, me_q

    def along_x(o):
        peer = lax.rem(me_x + o, GX)
        return {"gx": peer}, peer, me_x

    planes = [across(o) for o in columns]
    lines = [along_x(o) for o in (4, 3, 5, 2, 6, 1, 7)]
    barrier = pltpu.get_barrier_semaphore()
    for device, _, _ in lines + planes:
        pl.semaphore_signal(barrier, inc=1, device_id=device, device_id_type=MESH)
    constants = (weight_any, third_any, back_any, second_any, first_any, firstt_any, pair_any)
    copies = (weight_ref, third_ref, back_ref, second_ref, first_ref, firstt_ref, pair_ref)
    loads = [pltpu.make_async_copy(c, d, loaded.at[n]) for n, (c, d) in enumerate(zip(constants, copies))]
    for load in loads:
        load.start()
    order = lax.broadcasted_iota(jnp.int32, (1024, 128), 0).astype(F32)
    for z in range(8):
        moved = jnp.where(order == rank_ref[0:1, 128 * z : 128 * z + 128], 1.0, 0.0).astype(BF16)
        latent[64 * z : 64 * z + 64] = dotf(ordered_ref[...], moved)
    for q in range(32):
        both = [latent[pl.ds(2 * q + c, 8, stride=64), :] for c in range(2)]
        l_msg[q] = jnp.concatenate(both, axis=0).astype(BF16)
    pl.semaphore_wait(barrier, len(planes + lines))

    sends = []

    def start(stage, peers, source, target):
        for device, peer, me in peers:
            pltpu.make_async_remote_copy(
                src_ref=source(peer),
                dst_ref=target.at[me],
                send_sem=send.at[stage],
                recv_sem=recv.at[stage],
                device_id=device,
                device_id_type=MESH,
            ).start()
        everything = target.at[pl.ds(0, len(peers))]
        sends.append((stage, everything))
        return stage, everything

    def finish(pending):
        stage, everything = pending
        pltpu.make_async_copy(everything, everything, recv.at[stage]).wait()

    rows128 = lax.broadcasted_iota(jnp.int32, (128, 128), 0)
    lanes128 = lax.broadcasted_iota(jnp.int32, (128, 128), 1)
    same = rows128 // 16 == lanes128 // 16

    def spread_blocks(ref, part, l):
        small = ref[me_x, part, l].astype(F32)
        return jnp.where(same, jnp.concatenate([small] * 8, axis=0), 0.0).astype(BF16)

    first = start(0, planes, lambda p: l_msg.at[p], r1)
    r1[me_q] = l_msg[me_q]
    loads[0].wait()
    forth = regroup()
    for l in range(2):
        wide = jnp.concatenate(
            [weight_ref[b, 8 * l : 8 * l + 8].astype(F32).reshape(512, 64) for b in range(2)], axis=1
        ).astype(BF16)
        w_msg[:, 16 * l : 16 * l + 16, :] = dotf(forth, wide).astype(BF16).reshape(32, 16, 128)
    weights = start(1, planes, lambda p: w_msg.at[p], rw)
    rw[me_q] = w_msg[me_q]
    for load in loads[1:]:
        load.wait()
    first_tab = [[spread_blocks(first_ref, p, l) for l in range(2)] for p in range(2)]
    back_tab = [[spread_blocks(firstt_ref, p, l) for l in range(2)] for p in range(2)]
    skip_t = skip_ref[...].astype(F32).T.astype(BF16)
    for z in range(8):
        skip[z] = dotf(skip_t, latent[64 * z : 64 * z + 64].astype(BF16))
    finish(first)

    pieces = []
    for e in range(4):
        values = r1[8 * e : 8 * e + 8].reshape(128, 128)
        piece = dotf(third_ref[0], values) + dotf(third_ref[1], values)
        pieces += [piece[0:32], piece[32:64]]
    wide = jnp.concatenate(pieces, axis=1).astype(BF16)
    rows = jnp.concatenate(
        [dott(second_ref[0, l], wide) + dott(second_ref[1, l], wide) for l in range(2)], axis=1
    )
    upper, lower = split(rows)
    partial = jnp.concatenate(
        [
            dotf(first_tab[0][l], upper) + dotf(first_tab[0][l], lower) + dotf(first_tab[1][l], upper)
            for l in range(2)
        ],
        axis=1,
    )
    s_msg[...] = partial.astype(BF16).reshape(8, 16, 128)

    third = start(2, lines, lambda p: s_msg.at[p], r3)
    r3[me_x] = s_msg[me_x]
    finish(weights)
    for h in range(8):
        parts = [
            rw[e * 8 + h, 8 * p : 8 * p + 8, :].astype(F32) for p in range(4) for e in range(4)
        ]
        mixing[h] = jnp.concatenate(parts, axis=0).T.astype(BF16)
    finish(third)
    modes = jnp.sum(r3[...].astype(F32), axis=0)

    own = rows128 // 2 == lanes128 // 2
    even = lax.broadcasted_iota(jnp.int32, (64, 128), 1) % 2 == 0
    products = []
    for h in range(8):
        expanded = jnp.concatenate(
            [
                jnp.where(own, jnp.broadcast_to(modes[2 * h + a : 2 * h + a + 1], (128, 128)), 0.0)
                for a in range(2)
            ],
            axis=0,
        ).astype(BF16)
        products.append(dott(mixing[h], expanded))
    for h, product in enumerate(products):
        mixed_scr[h, 0:64] = product[0:64, 0:128] - product[64:128, 128:256]
        mixed_scr[h, 64:128] = product[64:128, 0:128] + product[0:64, 128:256]
    turned = [
        jnp.where(even, mixed_scr[h, pl.ds(0, 64, stride=2), :], mixed_scr[h, pl.ds(1, 64, stride=2), :])
        for h in range(8)
    ]
    place = lax.broadcasted_iota(jnp.int32, (512, 512), 0)
    source = lax.broadcasted_iota(jnp.int32, (512, 512), 1)
    wanted = ((place >> 1) & 7) * 64 + (place & 1) * 32 + (place >> 4)
    order = jnp.where(wanted == source, 1.0, 0.0).astype(BF16)
    turned = jnp.concatenate(turned, axis=0).astype(BF16)
    n_msg[...] = dotf(order, turned).astype(BF16).reshape(32, 16, 128)

    fourth = start(3, planes, lambda p: n_msg.at[p], r5)
    r5[me_q] = n_msg[me_q]
    finish(fourth)
    mixed = jnp.sum(r5[...].astype(F32), axis=0)
    zero_rows = lax.broadcasted_iota(jnp.int32, (16, 128), 0)
    zero_lanes = lax.broadcasted_iota(jnp.int32, (16, 128), 1)
    mixed = jnp.where((zero_rows < 2) & (zero_lanes < 2) & (me_x == 0), 0.0, mixed)
    g_msg[...] = mixed.astype(BF16)

    fifth = start(4, lines, lambda p: g_msg, r6)
    r6[me_x] = g_msg[...]
    finish(fifth)
    field = r6[...].reshape(128, 128)
    along = (
        dotf(back_tab[0][0], field[:, 0:64])
        + dotf(back_tab[1][0], field[:, 0:64])
        + dotf(back_tab[0][1], field[:, 64:128])
        + dotf(back_tab[1][1], field[:, 64:128])
    )
    upper, lower = split(along.T)
    plane = (
        dotf(upper[0:32], second_ref[0, 0])
        + dotf(lower[0:32], second_ref[0, 0])
        + dotf(upper[0:32], second_ref[1, 0])
        + dotf(upper[32:64], second_ref[0, 1])
        + dotf(lower[32:64], second_ref[0, 1])
        + dotf(upper[32:64], second_ref[1, 1])
    )
    scale = 1.0 / GRID**3
    plane_rows = lax.broadcasted_iota(jnp.int32, (32, 1024), 0)
    plane = (plane * jnp.where(plane_rows < 2, scale, 2.0 * scale)).astype(BF16)
    wide_field = field.astype(F32)
    paired = jnp.zeros((128, 128), F32)
    for p in range(4):
        paired = jnp.where(lanes128 // 32 == p, dotf(pair_ref[p], field), paired)
    low = (lanes128 // 2) % 16 == 0
    power = jnp.where(low, 0.5 * wide_field * (wide_field + paired), 2.0 * wide_field * wide_field)
    power = jnp.sum(power, axis=0, keepdims=True)
    for shift in (64, 32, 16, 8, 4, 2):
        power = power + pltpu.roll(power, shift, 1)
    lane = lax.broadcasted_iota(jnp.int32, (1, 128), 1)
    power = jnp.where(lane % 2 == (lane // 8) % 2, power, pltpu.roll(power, 1, 1))
    variance = jnp.broadcast_to(power, (128, 128)).T * (scale * scale)
    inverse = 1.0 / jnp.sqrt(variance + NORM_FLOOR)
    for e in range(4):
        part = jnp.concatenate(
            [plane[:, (2 * e + b) * 128 : (2 * e + b + 1) * 128] for b in range(2)], axis=0
        )
        branch = (dotf(back_ref[0], part) + dotf(back_ref[1], part)) * inverse
        b_msg[8 * e : 8 * e + 8] = branch.astype(BF16).reshape(8, 16, 128)

    sixth = start(5, planes, lambda p: b_msg.at[p], r8)
    r8[me_q] = b_msg[me_q]
    finish(sixth)
    ended[...] = r8[...].reshape(512, 128).astype(F32)
    for z in range(8):
        out_ref[z] = ended[pl.ds(z, 64, stride=8), :] + skip[z]
    for stage, everything in sends:
        pltpu.make_async_copy(everything, everything, send.at[stage]).wait()


def final_kernel(cells_ref, out_ref):
    for z in range(8):
        out_ref[:, z, :] = gelu(cells_ref[z]).T


def final(cells):
    vmem = pl.BlockSpec(memory_space=pltpu.VMEM)
    return pl.pallas_call(
        final_kernel, out_shape=jax.ShapeDtypeStruct((128, 8, 64), F32), in_specs=[vmem], out_specs=vmem
    )(cells)


def spectral_layer(ordered, rank, skip_w, weight, *tables):
    vmem = pl.BlockSpec(memory_space=pltpu.VMEM)
    own = [pltpu.VMEM(array.shape, array.dtype) for array in (weight,) + tables]
    return pl.pallas_call(
        spectral_kernel,
        out_shape=jax.ShapeDtypeStruct((8, 64, 128), F32),
        in_specs=[vmem] * 3 + [pl.BlockSpec(memory_space=pl.ANY)] * 7,
        out_specs=vmem,
        scratch_shapes=own
        + [
            pltpu.VMEM((512, 128), F32),
            pltpu.VMEM((32, 16, 128), BF16),
            pltpu.VMEM((32, 16, 128), BF16),
            pltpu.VMEM((32, 32, 128), BF16),
            pltpu.VMEM((32, 32, 128), BF16),
            pltpu.VMEM((8, 16, 128), BF16),
            pltpu.VMEM((8, 16, 128), BF16),
            pltpu.VMEM((8, 128, 128), BF16),
            pltpu.VMEM((8, 128, 128), F32),
            pltpu.VMEM((32, 16, 128), BF16),
            pltpu.VMEM((32, 16, 128), BF16),
            pltpu.VMEM((16, 128), BF16),
            pltpu.VMEM((8, 16, 128), BF16),
            pltpu.VMEM((32, 16, 128), BF16),
            pltpu.VMEM((32, 16, 128), BF16),
            pltpu.VMEM((512, 128), F32),
            pltpu.VMEM((8, 64, 128), F32),
            pltpu.SemaphoreType.DMA((6,)),
            pltpu.SemaphoreType.DMA((6,)),
            pltpu.SemaphoreType.DMA((7,)),
        ],
        compiler_params=pltpu.CompilerParams(collective_id=0, has_side_effects=True),
    )(ordered, rank, skip_w, weight, *tables)


def body(point_data, neighbours, counts, kernel_in, kernel_mid, kernel_out, spectral, skip_weight):
    cells_x, cells_y, cells_z = neighbours.shape[1:4]
    made = halo(
        jnp.transpose(point_data, (1, 0, 2)),
        neighbours.reshape(-1, NB),
        jnp.transpose(counts[0], (0, 2, 1)),
    )
    ordered = encode(*made[:4], kernel_in, kernel_mid, kernel_out.T)
    third = third_table()
    by_place = first_table()
    cells = spectral_layer(
        ordered,
        made[4],
        skip_weight,
        spectral.reshape(2, 16, 64, 64),
        jnp.asarray(halves(third)),
        jnp.asarray(halves(third.T)),
        jnp.asarray(halves(second_table())),
        jnp.asarray(placed(by_place)),
        jnp.asarray(placed(np.swapaxes(by_place, 2, 3))),
        jnp.asarray(pair_table().astype(ml_dtypes.bfloat16)),
    )
    out = final(cells)
    return out.reshape(1, cells_x, cells_y, cells_z, -1)


def solution(mesh):
    in_specs = (
        P(None, None, ("gx", "gy", "gz")),
        P(None, "gx", "gy", "gz", None),
        P(None, "gx", "gy", "gz"),
        P(),
        P(),
        P(),
        P(None, "gz", "gx", "gy", None, None),
        P(),
    )
    out_specs = P(None, "gx", "gy", "gz", None)
    return jax.shard_map(body, mesh=mesh, in_specs=in_specs, out_specs=out_specs, check_vma=False)
```

```python
import functools
import math

import jax
import jax.numpy as jnp
import ml_dtypes
import numpy as np
from jax import lax
from jax.experimental import pallas as pl
from jax.experimental.pallas import tpu as pltpu
from jax.sharding import PartitionSpec as P

GRID = 64
MODES = 16
NB = 32
NORM_FLOOR = 1.0
GX, GY, GZ = 8, 4, 8
F32 = jnp.float32
BF16 = jnp.bfloat16
MESH = pl.DeviceIdType.MESH


def gelu(v):
    inner = v * (0.7978845608028654 + 0.035677408136300125 * (v * v))
    half = 0.5 * v
    return half + half * jnp.tanh(inner)


def twice_gelu(v):
    if not GELU16:
        return v + v * jnp.tanh(v * (0.7978845608028654 + 0.035677408136300125 * (v * v)))
    v = v.astype(BF16)
    inner = v * (BF16(0.7978845608028654) + BF16(0.035677408136300125) * (v * v))
    return v + v * jnp.tanh(inner)


SLOTS = 4
ROWS = 176
FOUR, SIX = 108, 162
GELU16 = True
OFFSETS = [(dx, dy, dz) for dx in (-1, 0, 1) for dy in (-1, 0, 1) for dz in (-1, 0, 1)]


def regroup():
    row = lax.broadcasted_iota(jnp.int32, (512, 512), 0)
    column = lax.broadcasted_iota(jnp.int32, (512, 512), 1)
    wanted = ((row >> 1) & 7) * 64 + (row >> 4) * 2 + (row & 1)
    return jnp.where(wanted == column, 1.0, 0.0).astype(BF16)


def halo_kernel(
    points_ref, near_any, counts_ref, table_ref, slots_ref, blocks_ref, info_ref, rank_ref,
    main, near_ref, send, recv, loaded,
):
    me_x = lax.axis_index("gx")
    me_y = lax.axis_index("gy")
    me_z = lax.axis_index("gz")

    def device(offset):
        dx, dy, dz = offset
        return {
            "gx": lax.rem(me_x + dx + GX, GX),
            "gy": lax.rem(me_y + dy + GY, GY),
            "gz": lax.rem(me_z + dz + GZ, GZ),
        }

    barrier = pltpu.get_barrier_semaphore()
    peers = [o for o in OFFSETS if o != (0, 0, 0)]
    for offset in peers:
        pl.semaphore_signal(barrier, inc=1, device_id=device(offset), device_id_type=MESH)
    load = pltpu.make_async_copy(near_any, near_ref, loaded)
    load.start()

    main[13] = jnp.concatenate([points_ref[d] for d in range(6)] + [jnp.zeros((2, 512), F32)], axis=0).astype(BF16)
    pl.semaphore_wait(barrier, len(peers))
    for offset in sorted(peers, key=lambda o: -sum(abs(d) for d in o)):
        slot = 26 - OFFSETS.index(offset)
        pltpu.make_async_remote_copy(
            src_ref=main.at[13],
            dst_ref=main.at[slot],
            send_sem=send.at[0],
            recv_sem=recv.at[0],
            device_id=device(offset),
            device_id_type=MESH,
        ).start()
    everything = main.at[pl.ds(0, 26)]

    lane = lax.broadcasted_iota(jnp.int32, (1, 1024), 1)
    counts = jnp.concatenate([counts_ref[x].astype(F32) for x in range(8)], axis=1)
    counts = jnp.concatenate([counts[z : z + 1] for z in range(8)], axis=1)
    key = counts * 1024.0 + (1023 - lane).astype(F32)
    ones = jnp.ones((8, 128), BF16)
    rank = jnp.zeros((8, 1024), F32)
    for m in range(8):
        tall = jnp.broadcast_to(key[:, 128 * m : 128 * m + 128], (128, 128)).T
        ahead = jnp.concatenate(
            [
                jnp.where(tall > key[:, 128 * n : 128 * n + 128], 1.0, 0.0).astype(BF16)
                for n in range(8)
            ],
            axis=1,
        )
        rank = rank + jnp.dot(ones, ahead, preferred_element_type=F32)
    rank_ref[...] = rank
    load.wait()
    near = jnp.concatenate(
        [near_ref[pl.ds(z, 128, stride=8), :].astype(F32).T for z in range(8)], axis=1
    ).astype(jnp.int32)
    owner = near >> 9
    part = near & 511
    block = ((((owner >> 5) - me_x + 1) * 3) + ((owner >> 3) & 3) - me_y + 1) * 3 + (owner & 7) - me_z + 1
    code = jnp.clip(block, 0, 26) * 2 + (part >> 8)
    place_y = (me_y * 16 + (lane & 15)).astype(F32)
    place_x = (me_x * 8 + ((lane >> 4) & 7)).astype(F32)
    place_z = (me_z * 8 + (lane >> 7)).astype(F32)
    centres = [-(place + 0.5) / GRID for place in (place_x, place_y, place_z)]
    rows = jnp.concatenate(
        [(part & 255).astype(F32), code.astype(F32), counts] + centres + [jnp.zeros((12, 1024), F32)], axis=0
    ).astype(BF16)
    order = lax.broadcasted_iota(jnp.int32, (128, 1024), 0).astype(F32)
    wide_rank = rank[0:1]
    for t in range(8):
        moved = jnp.where(order + 128.0 * t == wide_rank, 1.0, 0.0).astype(BF16)
        moved = lax.dot_general(rows, moved, (((1,), (1,)), ((), ())), preferred_element_type=F32)
        slots_ref[t] = moved[0:32].astype(jnp.int32)
        blocks_ref[t] = moved[32:64].astype(jnp.int32)
        info_ref[t] = moved[64:72]

    pltpu.make_async_copy(everything, everything, recv.at[0]).wait()
    blocks = [main[b].astype(F32) for b in range(27)]
    rows = [block[0:4] for block in blocks] + [block[4:6] for block in blocks]
    rows.append(jnp.zeros((ROWS - SIX, 512), F32))
    rows = jnp.concatenate(rows, axis=0).astype(BF16)
    table_ref[0:ROWS, :] = rows[:, 0:256]
    table_ref[ROWS : 2 * ROWS, :] = rows[:, 256:512]
    pltpu.make_async_copy(everything, everything, send.at[0]).wait()


def halo(points, near, counts):
    vmem = pl.BlockSpec(memory_space=pltpu.VMEM)
    return pl.pallas_call(
        halo_kernel,
        out_shape=[
            jax.ShapeDtypeStruct((2 * ROWS, 256), BF16),
            jax.ShapeDtypeStruct((8, NB, 128), jnp.int32),
            jax.ShapeDtypeStruct((8, NB, 128), jnp.int32),
            jax.ShapeDtypeStruct((8, 8, 128), F32),
            jax.ShapeDtypeStruct((8, 1024), F32),
        ],
        in_specs=[vmem, pl.BlockSpec(memory_space=pl.ANY), vmem],
        out_specs=[vmem] * 5,
        scratch_shapes=[
            pltpu.VMEM((27, 8, 512), BF16),
            pltpu.VMEM((1024, NB), jnp.int32),
            pltpu.SemaphoreType.DMA((1,)),
            pltpu.SemaphoreType.DMA((1,)),
            pltpu.SemaphoreType.DMA,
        ],
        compiler_params=pltpu.CompilerParams(collective_id=1, has_side_effects=True),
    )(points, near, counts)


def encoder_kernel(
    table_ref, slots_ref, blocks_ref, info_ref, in_ref, mid_ref, last_ref, out_ref,
    first_scr, mid_scr, last_scr, kept_scr, hidden_scr, base_scr, totals, trips,
):
    column = lax.broadcasted_iota(jnp.int32, (6, ROWS), 1)
    feature = lax.broadcasted_iota(jnp.int32, (6, ROWS), 0)
    wanted = jnp.where(column < FOUR, column % 4, 4 + column % 2)
    wanted = jnp.where(column >= SIX, column - SIX, wanted)
    chosen = jnp.where((feature == wanted) & (column < SIX + 3), 1.0, 0.0).astype(BF16)
    turn = (((0,), (0,)), ((), ()))
    first_scr[...] = lax.dot_general(in_ref[...], chosen, turn, preferred_element_type=F32).astype(BF16)
    half_mid = (mid_ref[...].astype(F32).T * 0.5).astype(BF16)
    mid_scr[...] = jnp.zeros(mid_scr.shape, BF16)
    mid_scr[0:80, 0:80] = half_mid
    mid_scr[80:160, 80:160] = half_mid
    last_scr[...] = last_ref[...]

    slot_ids = lax.broadcasted_iota(jnp.int32, (256, 128), 0).astype(jnp.int16)
    row = lax.broadcasted_iota(jnp.int32, (ROWS, 128), 0)
    row_block = jnp.where(row < FOUR, row // 4, jnp.where(row < SIX, (row - FOUR) // 2, -1)).astype(jnp.int16)
    last_rows = lax.broadcasted_iota(jnp.int32, (16, 128), 0)
    steps = 0
    for c in range(8):
        info = info_ref[c]
        trip = (jnp.max(info[0:1]).astype(jnp.int32) + SLOTS - 1) // SLOTS
        trips[c] = trip
        steps += trip
        centre = jnp.zeros((16, 128), F32)
        for d in range(3):
            centre = jnp.where(last_rows == SIX - ROWS + 16 + d, info[1 + d : 2 + d], centre)
        base_scr[c] = centre.astype(BF16)
        totals[c] = jnp.zeros((80, 128), F32)
    totals[8] = jnp.zeros((80, 128), F32)
    kept_scr[...] = jnp.zeros(kept_scr.shape, BF16)
    hidden_scr[...] = jnp.zeros(hidden_scr.shape, BF16)

    def step(n, places):
        (c0, t0), (c1, t1), (c2, t2) = places
        hidden = twice_gelu(jnp.dot(mid_scr[...], hidden_scr[...], preferred_element_type=F32))
        counts = info_ref[jnp.minimum(c2, 7), 0:1, :]
        total = totals[c2]
        for u in range(SLOTS):
            used = (SLOTS * t2 + u).astype(F32) < counts
            here = hidden[80 * (u // 2) : 80 * (u // 2) + 80, 128 * (u % 2) : 128 * (u % 2) + 128]
            total = total + jnp.where(used, here.astype(F32), 0.0)
        totals[c2] = total
        hidden = jnp.dot(first_scr[...], kept_scr[...], preferred_element_type=F32)
        hidden = twice_gelu(hidden).astype(BF16)
        for u in range(SLOTS // 2):
            hidden_scr[80 * u : 80 * u + 80, :] = hidden[:, 256 * u : 256 * u + 256]
        hot = []
        for u in range(SLOTS):
            slot = jnp.broadcast_to(slots_ref[c0, pl.ds(SLOTS * t0 + u, 1), :], (16, 128)).astype(jnp.int16)
            slot = jnp.concatenate([slot] * 16, axis=0)
            hot.append(jnp.where(slot_ids == slot, BF16(1), BF16(0)))
        found = jnp.dot(table_ref[...], jnp.concatenate(hot, axis=1), preferred_element_type=F32)
        found = found.astype(BF16)
        for u in range(SLOTS):
            code = jnp.broadcast_to(blocks_ref[c0, pl.ds(SLOTS * t0 + u, 1), :], (16, 128))
            block = (code >> 1).astype(jnp.int16)
            odd = (code & 1).astype(jnp.int16)
            same = row_block == jnp.concatenate([block] * (ROWS // 16), axis=0)
            odd = jnp.concatenate([odd] * (ROWS // 16), axis=0) == 1
            here = found[:, 128 * u : 128 * u + 128]
            here = jnp.where(odd, here[ROWS : 2 * ROWS], here[0:ROWS])
            kept_scr[0 : ROWS - 16, 128 * u : 128 * u + 128] = jnp.where(same[0 : ROWS - 16], here[0 : ROWS - 16], BF16(0))
            kept_scr[ROWS - 16 : ROWS, 128 * u : 128 * u + 128] = jnp.where(same[ROWS - 16 : ROWS], here[ROWS - 16 : ROWS], base_scr[c0])
        ended = t0 + 1 >= trips[c0]
        following = (
            jnp.minimum(jnp.where(ended, c0 + 1, c0), 7),
            jnp.where(ended, jnp.where(c0 == 7, t0, 0), t0 + 1),
        )
        return following, (c0, t0), (c1, t1)

    start = (jnp.int32(0), jnp.int32(0))
    spare = (jnp.int32(8), jnp.int32(0))
    lax.fori_loop(0, steps + 2, step, (start, spare, spare))
    last = last_scr[...]
    ordered = []
    for c in range(8):
        mean = totals[c] * (0.5 / info_ref[c, 0:1, :])
        upper = mean.astype(BF16)
        lower = (mean - upper.astype(F32)).astype(BF16)
        values = jnp.dot(last, upper, preferred_element_type=F32) + jnp.dot(
            last, lower, preferred_element_type=F32
        )
        ordered.append(values.astype(BF16))
    out_ref[...] = jnp.concatenate(ordered, axis=1)


def encode(table, slots, blocks, info, kernel_in, kernel_mid, kernel_out):
    vmem = pl.BlockSpec(memory_space=pltpu.VMEM)
    return pl.pallas_call(
        encoder_kernel,
        out_shape=jax.ShapeDtypeStruct((64, 1024), BF16),
        in_specs=[vmem] * 7,
        out_specs=vmem,
        scratch_shapes=[
            pltpu.VMEM((80, ROWS), BF16),
            pltpu.VMEM((160, 160), BF16),
            pltpu.VMEM((64, 80), BF16),
            pltpu.VMEM((ROWS, 128 * SLOTS), BF16),
            pltpu.VMEM((160, 256), BF16),
            pltpu.VMEM((8, 16, 128), BF16),
            pltpu.VMEM((9, 80, 128), F32),
            pltpu.SMEM((8,), jnp.int32),
        ],
    )(table, slots, blocks, info, kernel_in, kernel_mid, kernel_out)


def halves(values):
    upper = values.astype(np.float32).astype(ml_dtypes.bfloat16)
    lower = (values - upper.astype(np.float64)).astype(np.float32).astype(ml_dtypes.bfloat16)
    return np.stack([upper, lower])


def turn(frequency, position):
    angle = 2.0 * math.pi * ((frequency * position) % GRID) / GRID
    return np.cos(angle), np.sin(angle)


def centred(index):
    return np.where(index < MODES // 2, index, index - MODES)


def complex_block(cos, sin):
    return np.stack([np.stack([cos, sin], -1), np.stack([-sin, cos], -1)], -2)


@functools.lru_cache(None)
def third_table():
    cos, sin = turn(np.arange(16)[:, None], np.arange(64)[None, :])
    parts = np.stack([cos, -sin]).reshape(2, 16, 8, 8)
    full = np.einsum("akgz,cd->akcgdz", parts, np.eye(2))
    return full.reshape(64, 128)


@functools.lru_cache(None)
def second_table():
    j = np.arange(16)
    cos, sin = turn(centred(j)[:, None], np.arange(64)[None, :])
    both = complex_block(cos, sin).reshape(8, 2, 4, 16, 2, 2)
    full = np.einsum("gleyab,xw->lgaxebwy", both, np.eye(8))
    return full.reshape(2, 128, 1024)


@functools.lru_cache(None)
def first_table():
    i = np.arange(16)
    cos, sin = turn(centred(i)[:, None], np.arange(64)[None, :])
    both = complex_block(cos, sin).reshape(8, 2, 8, 8, 2, 2)
    return np.einsum("hltxab->tlhabx", both).reshape(8, 2, 16, 16)


def placed(values):
    return np.tile(np.moveaxis(halves(values), 0, 1), (1, 1, 1, 1, 8))


@functools.lru_cache(None)
def pair_table():
    out = np.zeros((4, 8, 8, 2, 8, 8, 2))
    for il in range(2):
        for jl in range(2):
            for h in range(8):
                for g in range(8):
                    i, j = 2 * h + il, 2 * g + jl
                    if i == 8 or j == 8:
                        continue
                    ni, nj = (16 - i) % 16, (16 - j) % 16
                    assert ni % 2 == il and nj % 2 == jl
                    for a in range(2):
                        out[2 * il + jl, g, h, a, nj // 2, ni // 2, a] = 1.0 - 2.0 * a
    return out.reshape(4, 128, 128)


def dotf(a, b):
    return jnp.dot(a, b, preferred_element_type=F32)


def dott(a, b):
    return lax.dot_general(a, b, (((1,), (1,)), ((), ())), preferred_element_type=F32)


def split(values):
    upper = values.astype(BF16)
    return upper, (values - upper.astype(F32)).astype(BF16)


def spectral_kernel(
    ordered_any, rank_any, skip_ref, weight_any, third_any, back_any, second_any, first_any, firstt_any, pair_any,
    out_ref,
    weight_ref, third_ref, back_ref, second_ref, first_ref, firstt_ref, pair_ref, ordered_ref, rank_ref,
    latent, l_msg, r1, w_msg, rw, s_msg, r3, mixing, mixed_scr, n_msg, r5, g_msg, r6, b_msg, r8, ended, skip,
    send, recv, loaded,
):
    me_x = lax.axis_index("gx")
    me_y = lax.axis_index("gy")
    me_z = lax.axis_index("gz")
    me_q = me_y * GZ + me_z
    columns = [(y, z) for y in range(GY) for z in range(GZ) if y or z]
    columns.sort(key=lambda o: -(2 * min(o[0], GY - o[0]) + min(o[1], GZ - o[1])))

    def across(o):
        y, z = lax.rem(me_y + o[0], GY), lax.rem(me_z + o[1], GZ)
        return {"gy": y, "gz": z}, y * GZ + z, me_q

    def along_x(o):
        peer = lax.rem(me_x + o, GX)
        return {"gx": peer}, peer, me_x

    planes = [across(o) for o in columns]
    lines = [along_x(o) for o in (4, 3, 5, 2, 6, 1, 7)]
    barrier = pltpu.get_barrier_semaphore()
    for device, _, _ in lines + planes:
        pl.semaphore_signal(barrier, inc=1, device_id=device, device_id_type=MESH)
    constants = (weight_any, third_any, back_any, second_any, first_any, firstt_any, pair_any)
    copies = (weight_ref, third_ref, back_ref, second_ref, first_ref, firstt_ref, pair_ref)
    loads = [pltpu.make_async_copy(c, d, loaded.at[n]) for n, (c, d) in enumerate(zip(constants, copies))]
    early = [
        pltpu.make_async_copy(c, d, loaded.at[7 + n])
        for n, (c, d) in enumerate(((ordered_any, ordered_ref), (rank_any, rank_ref)))
    ]
    for load in early + loads:
        load.start()
    for load in early:
        load.wait()
    order = lax.broadcasted_iota(jnp.int32, (1024, 128), 0).astype(F32)
    for z in range(8):
        moved = jnp.where(order == rank_ref[0:1, 128 * z : 128 * z + 128], 1.0, 0.0).astype(BF16)
        latent[64 * z : 64 * z + 64] = dotf(ordered_ref[...], moved)
    for q in range(32):
        both = [latent[pl.ds(2 * q + c, 8, stride=64), :] for c in range(2)]
        l_msg[q] = jnp.concatenate(both, axis=0).astype(BF16)
    pl.semaphore_wait(barrier, len(planes + lines))

    sends = []

    def start(stage, peers, source, target):
        for device, peer, me in peers:
            pltpu.make_async_remote_copy(
                src_ref=source(peer),
                dst_ref=target.at[me],
                send_sem=send.at[stage],
                recv_sem=recv.at[stage],
                device_id=device,
                device_id_type=MESH,
            ).start()
        everything = target.at[pl.ds(0, len(peers))]
        sends.append((stage, everything))
        return stage, everything

    def finish(pending):
        stage, everything = pending
        pltpu.make_async_copy(everything, everything, recv.at[stage]).wait()

    rows128 = lax.broadcasted_iota(jnp.int32, (128, 128), 0)
    lanes128 = lax.broadcasted_iota(jnp.int32, (128, 128), 1)
    same = rows128 // 16 == lanes128 // 16

    def spread_blocks(ref, part, l):
        small = ref[me_x, part, l].astype(F32)
        return jnp.where(same, jnp.concatenate([small] * 8, axis=0), 0.0).astype(BF16)

    first = start(0, planes, lambda p: l_msg.at[p], r1)
    r1[me_q] = l_msg[me_q]
    loads[0].wait()
    forth = regroup()
    for l in range(2):
        wide = jnp.concatenate(
            [weight_ref[b, 8 * l : 8 * l + 8].astype(F32).reshape(512, 64) for b in range(2)], axis=1
        ).astype(BF16)
        w_msg[:, 16 * l : 16 * l + 16, :] = dotf(forth, wide).astype(BF16).reshape(32, 16, 128)
    weights = start(1, planes, lambda p: w_msg.at[p], rw)
    rw[me_q] = w_msg[me_q]
    for load in loads[1:]:
        load.wait()
    first_tab = [[spread_blocks(first_ref, p, l) for l in range(2)] for p in range(2)]
    back_tab = [[spread_blocks(firstt_ref, p, l) for l in range(2)] for p in range(2)]
    skip_t = skip_ref[...].astype(F32).T.astype(BF16)
    for z in range(8):
        skip[z] = dotf(skip_t, latent[64 * z : 64 * z + 64].astype(BF16))
    finish(first)

    pieces = []
    for e in range(4):
        values = r1[8 * e : 8 * e + 8].reshape(128, 128)
        piece = dotf(third_ref[0], values) + dotf(third_ref[1], values)
        pieces += [piece[0:32], piece[32:64]]
    wide = jnp.concatenate(pieces, axis=1).astype(BF16)
    rows = jnp.concatenate(
        [dott(second_ref[0, l], wide) + dott(second_ref[1, l], wide) for l in range(2)], axis=1
    )
    upper, lower = split(rows)
    partial = jnp.concatenate(
        [
            dotf(first_tab[0][l], upper) + dotf(first_tab[0][l], lower) + dotf(first_tab[1][l], upper)
            for l in range(2)
        ],
        axis=1,
    )
    s_msg[...] = partial.astype(BF16).reshape(8, 16, 128)

    third = start(2, lines, lambda p: s_msg.at[p], r3)
    r3[me_x] = s_msg[me_x]
    finish(weights)
    for h in range(8):
        parts = [
            rw[e * 8 + h, 8 * p : 8 * p + 8, :].astype(F32) for p in range(4) for e in range(4)
        ]
        mixing[h] = jnp.concatenate(parts, axis=0).T.astype(BF16)
    finish(third)
    modes = jnp.sum(r3[...].astype(F32), axis=0)

    own = rows128 // 2 == lanes128 // 2
    even = lax.broadcasted_iota(jnp.int32, (64, 128), 1) % 2 == 0
    products = []
    for h in range(8):
        expanded = jnp.concatenate(
            [
                jnp.where(own, jnp.broadcast_to(modes[2 * h + a : 2 * h + a + 1], (128, 128)), 0.0)
                for a in range(2)
            ],
            axis=0,
        ).astype(BF16)
        products.append(dott(mixing[h], expanded))
    for h, product in enumerate(products):
        mixed_scr[h, 0:64] = product[0:64, 0:128] - product[64:128, 128:256]
        mixed_scr[h, 64:128] = product[64:128, 0:128] + product[0:64, 128:256]
    turned = [
        jnp.where(even, mixed_scr[h, pl.ds(0, 64, stride=2), :], mixed_scr[h, pl.ds(1, 64, stride=2), :])
        for h in range(8)
    ]
    place = lax.broadcasted_iota(jnp.int32, (512, 512), 0)
    source = lax.broadcasted_iota(jnp.int32, (512, 512), 1)
    wanted = ((place >> 1) & 7) * 64 + (place & 1) * 32 + (place >> 4)
    order = jnp.where(wanted == source, 1.0, 0.0).astype(BF16)
    turned = jnp.concatenate(turned, axis=0).astype(BF16)
    n_msg[...] = dotf(order, turned).astype(BF16).reshape(32, 16, 128)

    fourth = start(3, planes, lambda p: n_msg.at[p], r5)
    r5[me_q] = n_msg[me_q]
    finish(fourth)
    mixed = jnp.sum(r5[...].astype(F32), axis=0)
    zero_rows = lax.broadcasted_iota(jnp.int32, (16, 128), 0)
    zero_lanes = lax.broadcasted_iota(jnp.int32, (16, 128), 1)
    mixed = jnp.where((zero_rows < 2) & (zero_lanes < 2) & (me_x == 0), 0.0, mixed)
    g_msg[...] = mixed.astype(BF16)

    fifth = start(4, lines, lambda p: g_msg, r6)
    r6[me_x] = g_msg[...]
    finish(fifth)
    field = r6[...].reshape(128, 128)
    along = (
        dotf(back_tab[0][0], field[:, 0:64])
        + dotf(back_tab[1][0], field[:, 0:64])
        + dotf(back_tab[0][1], field[:, 64:128])
        + dotf(back_tab[1][1], field[:, 64:128])
    )
    upper, lower = split(along.T)
    plane = (
        dotf(upper[0:32], second_ref[0, 0])
        + dotf(lower[0:32], second_ref[0, 0])
        + dotf(upper[0:32], second_ref[1, 0])
        + dotf(upper[32:64], second_ref[0, 1])
        + dotf(lower[32:64], second_ref[0, 1])
        + dotf(upper[32:64], second_ref[1, 1])
    )
    scale = 1.0 / GRID**3
    plane_rows = lax.broadcasted_iota(jnp.int32, (32, 1024), 0)
    plane = (plane * jnp.where(plane_rows < 2, scale, 2.0 * scale)).astype(BF16)
    wide_field = field.astype(F32)
    paired = jnp.zeros((128, 128), F32)
    for p in range(4):
        paired = jnp.where(lanes128 // 32 == p, dotf(pair_ref[p], field), paired)
    low = (lanes128 // 2) % 16 == 0
    power = jnp.where(low, 0.5 * wide_field * (wide_field + paired), 2.0 * wide_field * wide_field)
    power = jnp.sum(power, axis=0, keepdims=True)
    for shift in (64, 32, 16, 8, 4, 2):
        power = power + pltpu.roll(power, shift, 1)
    lane = lax.broadcasted_iota(jnp.int32, (1, 128), 1)
    power = jnp.where(lane % 2 == (lane // 8) % 2, power, pltpu.roll(power, 1, 1))
    variance = jnp.broadcast_to(power, (128, 128)).T * (scale * scale)
    inverse = 1.0 / jnp.sqrt(variance + NORM_FLOOR)
    for e in range(4):
        part = jnp.concatenate(
            [plane[:, (2 * e + b) * 128 : (2 * e + b + 1) * 128] for b in range(2)], axis=0
        )
        branch = (dotf(back_ref[0], part) + dotf(back_ref[1], part)) * inverse
        b_msg[8 * e : 8 * e + 8] = branch.astype(BF16).reshape(8, 16, 128)

    sixth = start(5, planes, lambda p: b_msg.at[p], r8)
    r8[me_q] = b_msg[me_q]
    finish(sixth)
    ended[...] = r8[...].reshape(512, 128).astype(F32)
    for z in range(8):
        out_ref[z] = ended[pl.ds(z, 64, stride=8), :] + skip[z]
    for stage, everything in sends:
        pltpu.make_async_copy(everything, everything, send.at[stage]).wait()


def final_kernel(cells_ref, out_ref):
    for z in range(8):
        out_ref[:, z, :] = gelu(cells_ref[z]).T


def final(cells):
    vmem = pl.BlockSpec(memory_space=pltpu.VMEM)
    return pl.pallas_call(
        final_kernel, out_shape=jax.ShapeDtypeStruct((128, 8, 64), F32), in_specs=[vmem], out_specs=vmem
    )(cells)


def spectral_layer(ordered, rank, skip_w, weight, *tables):
    vmem = pl.BlockSpec(memory_space=pltpu.VMEM)
    own = [pltpu.VMEM(array.shape, array.dtype) for array in (weight,) + tables + (ordered, rank)]
    return pl.pallas_call(
        spectral_kernel,
        out_shape=jax.ShapeDtypeStruct((8, 64, 128), F32),
        in_specs=[pl.BlockSpec(memory_space=pl.ANY)] * 2 + [vmem] + [pl.BlockSpec(memory_space=pl.ANY)] * 7,
        out_specs=vmem,
        scratch_shapes=own
        + [
            pltpu.VMEM((512, 128), F32),
            pltpu.VMEM((32, 16, 128), BF16),
            pltpu.VMEM((32, 16, 128), BF16),
            pltpu.VMEM((32, 32, 128), BF16),
            pltpu.VMEM((32, 32, 128), BF16),
            pltpu.VMEM((8, 16, 128), BF16),
            pltpu.VMEM((8, 16, 128), BF16),
            pltpu.VMEM((8, 128, 128), BF16),
            pltpu.VMEM((8, 128, 128), F32),
            pltpu.VMEM((32, 16, 128), BF16),
            pltpu.VMEM((32, 16, 128), BF16),
            pltpu.VMEM((16, 128), BF16),
            pltpu.VMEM((8, 16, 128), BF16),
            pltpu.VMEM((32, 16, 128), BF16),
            pltpu.VMEM((32, 16, 128), BF16),
            pltpu.VMEM((512, 128), F32),
            pltpu.VMEM((8, 64, 128), F32),
            pltpu.SemaphoreType.DMA((6,)),
            pltpu.SemaphoreType.DMA((6,)),
            pltpu.SemaphoreType.DMA((9,)),
        ],
        compiler_params=pltpu.CompilerParams(collective_id=0, has_side_effects=True),
    )(ordered, rank, skip_w, weight, *tables)


def body(point_data, neighbours, counts, kernel_in, kernel_mid, kernel_out, spectral, skip_weight):
    cells_x, cells_y, cells_z = neighbours.shape[1:4]
    made = halo(
        jnp.transpose(point_data, (1, 0, 2)),
        neighbours.reshape(-1, NB),
        jnp.transpose(counts[0], (0, 2, 1)),
    )
    ordered = encode(*made[:4], kernel_in, kernel_mid, kernel_out.T)
    third = third_table()
    by_place = first_table()
    cells = spectral_layer(
        ordered,
        made[4],
        skip_weight,
        spectral.reshape(2, 16, 64, 64),
        jnp.asarray(halves(third)),
        jnp.asarray(halves(third.T)),
        jnp.asarray(halves(second_table())),
        jnp.asarray(placed(by_place)),
        jnp.asarray(placed(np.swapaxes(by_place, 2, 3))),
        jnp.asarray(pair_table().astype(ml_dtypes.bfloat16)),
    )
    out = final(cells)
    return out.reshape(1, cells_x, cells_y, cells_z, -1)


def solution(mesh):
    in_specs = (
        P(None, None, ("gx", "gy", "gz")),
        P(None, "gx", "gy", "gz", None),
        P(None, "gx", "gy", "gz"),
        P(),
        P(),
        P(),
        P(None, "gz", "gx", "gy", None, None),
        P(),
    )
    out_specs = P(None, "gx", "gy", "gz", None)
    return jax.shard_map(body, mesh=mesh, in_specs=in_specs, out_specs=out_specs, check_vma=False)
```

```python
import functools
import math

import jax
import jax.numpy as jnp
import ml_dtypes
import numpy as np
from jax import lax
from jax.experimental import pallas as pl
from jax.experimental.pallas import tpu as pltpu
from jax.sharding import PartitionSpec as P

GRID = 64
LIMIT = 24 * 2**20
MODES = 16
NB = 32
NORM_FLOOR = 1.0
GX, GY, GZ = 8, 4, 8
F32 = jnp.float32
BF16 = jnp.bfloat16
MESH = pl.DeviceIdType.MESH


def gelu(v):
    inner = v * (0.7978845608028654 + 0.035677408136300125 * (v * v))
    half = 0.5 * v
    return half + half * jnp.tanh(inner)


def twice_gelu(v):
    if not GELU16:
        return v + v * jnp.tanh(v * (0.7978845608028654 + 0.035677408136300125 * (v * v)))
    v = v.astype(BF16)
    inner = v * (BF16(0.7978845608028654) + BF16(0.035677408136300125) * (v * v))
    return v + v * jnp.tanh(inner)


SLOTS = 4
ROWS = 176
FOUR, SIX = 108, 162
GELU16 = True
OFFSETS = [(dx, dy, dz) for dx in (-1, 0, 1) for dy in (-1, 0, 1) for dz in (-1, 0, 1)]


def kept(*arrays):
    return [pltpu.with_memory_space_constraint(array, pltpu.VMEM) for array in arrays]


def far(*arrays):
    return [pltpu.with_memory_space_constraint(array, pltpu.HBM) for array in arrays]


def regroup():
    row = lax.broadcasted_iota(jnp.int32, (512, 512), 0)
    column = lax.broadcasted_iota(jnp.int32, (512, 512), 1)
    wanted = ((row >> 1) & 7) * 64 + (row >> 4) * 2 + (row & 1)
    return jnp.where(wanted == column, 1.0, 0.0).astype(BF16)


def halo_kernel(
    points_ref, near_ref, counts_ref, table_ref, slots_ref, blocks_ref, info_ref, rank_ref,
    main, send, recv,
):
    me_x = lax.axis_index("gx")
    me_y = lax.axis_index("gy")
    me_z = lax.axis_index("gz")

    def device(offset):
        dx, dy, dz = offset
        return {
            "gx": lax.rem(me_x + dx + GX, GX),
            "gy": lax.rem(me_y + dy + GY, GY),
            "gz": lax.rem(me_z + dz + GZ, GZ),
        }

    barrier = pltpu.get_barrier_semaphore()
    peers = [o for o in OFFSETS if o != (0, 0, 0)]
    for offset in peers:
        pl.semaphore_signal(barrier, inc=1, device_id=device(offset), device_id_type=MESH)

    main[13] = jnp.concatenate([points_ref[d] for d in range(6)] + [jnp.zeros((2, 512), F32)], axis=0).astype(BF16)
    pl.semaphore_wait(barrier, len(peers))
    for offset in sorted(peers, key=lambda o: -sum(abs(d) for d in o)):
        slot = 26 - OFFSETS.index(offset)
        pltpu.make_async_remote_copy(
            src_ref=main.at[13],
            dst_ref=main.at[slot],
            send_sem=send.at[0],
            recv_sem=recv.at[0],
            device_id=device(offset),
            device_id_type=MESH,
        ).start()
    everything = main.at[pl.ds(0, 26)]

    lane = lax.broadcasted_iota(jnp.int32, (1, 1024), 1)
    counts = jnp.concatenate([counts_ref[x].astype(F32) for x in range(8)], axis=1)
    counts = jnp.concatenate([counts[z : z + 1] for z in range(8)], axis=1)
    key = counts * 1024.0 + (1023 - lane).astype(F32)
    ones = jnp.ones((8, 128), BF16)
    rank = jnp.zeros((8, 1024), F32)
    for m in range(8):
        tall = jnp.broadcast_to(key[:, 128 * m : 128 * m + 128], (128, 128)).T
        ahead = jnp.concatenate(
            [
                jnp.where(tall > key[:, 128 * n : 128 * n + 128], 1.0, 0.0).astype(BF16)
                for n in range(8)
            ],
            axis=1,
        )
        rank = rank + jnp.dot(ones, ahead, preferred_element_type=F32)
    rank_ref[...] = rank
    near = jnp.concatenate(
        [near_ref[pl.ds(z, 128, stride=8), :].astype(F32).T for z in range(8)], axis=1
    ).astype(jnp.int32)
    owner = near >> 9
    part = near & 511
    block = ((((owner >> 5) - me_x + 1) * 3) + ((owner >> 3) & 3) - me_y + 1) * 3 + (owner & 7) - me_z + 1
    code = jnp.clip(block, 0, 26) * 2 + (part >> 8)
    place_y = (me_y * 16 + (lane & 15)).astype(F32)
    place_x = (me_x * 8 + ((lane >> 4) & 7)).astype(F32)
    place_z = (me_z * 8 + (lane >> 7)).astype(F32)
    centres = [-(place + 0.5) / GRID for place in (place_x, place_y, place_z)]
    rows = jnp.concatenate(
        [(part & 255).astype(F32), code.astype(F32), counts] + centres + [jnp.zeros((12, 1024), F32)], axis=0
    ).astype(BF16)
    order = lax.broadcasted_iota(jnp.int32, (128, 1024), 0).astype(F32)
    wide_rank = rank[0:1]
    for t in range(8):
        moved = jnp.where(order + 128.0 * t == wide_rank, 1.0, 0.0).astype(BF16)
        moved = lax.dot_general(rows, moved, (((1,), (1,)), ((), ())), preferred_element_type=F32)
        slots_ref[t] = moved[0:32].astype(jnp.int32)
        blocks_ref[t] = moved[32:64].astype(jnp.int32)
        info_ref[t] = moved[64:72]

    pltpu.make_async_copy(everything, everything, recv.at[0]).wait()
    blocks = [main[b].astype(F32) for b in range(27)]
    rows = [block[0:4] for block in blocks] + [block[4:6] for block in blocks]
    rows.append(jnp.zeros((ROWS - SIX, 512), F32))
    rows = jnp.concatenate(rows, axis=0).astype(BF16)
    table_ref[0:ROWS, :] = rows[:, 0:256]
    table_ref[ROWS : 2 * ROWS, :] = rows[:, 256:512]
    pltpu.make_async_copy(everything, everything, send.at[0]).wait()


def halo(points, near, counts):
    vmem = pl.BlockSpec(memory_space=pltpu.VMEM)
    return pl.pallas_call(
        halo_kernel,
        out_shape=[
            pltpu.VMEM((2 * ROWS, 256), BF16),
            pltpu.VMEM((8, NB, 128), jnp.int32),
            pltpu.VMEM((8, NB, 128), jnp.int32),
            pltpu.VMEM((8, 8, 128), F32),
            pltpu.VMEM((8, 1024), F32),
        ],
        in_specs=[vmem] * 3,
        out_specs=[vmem] * 5,
        scratch_shapes=[
            pltpu.VMEM((27, 8, 512), BF16),
            pltpu.SemaphoreType.DMA((1,)),
            pltpu.SemaphoreType.DMA((1,)),
        ],
        compiler_params=pltpu.CompilerParams(collective_id=1, has_side_effects=True, vmem_limit_bytes=LIMIT),
    )(*far(points, near, counts))


def encoder_kernel(
    table_ref, slots_ref, blocks_ref, info_ref, in_ref, mid_ref, last_ref, out_ref,
    first_scr, mid_scr, last_scr, kept_scr, hidden_scr, base_scr, totals, trips,
):
    column = lax.broadcasted_iota(jnp.int32, (6, ROWS), 1)
    feature = lax.broadcasted_iota(jnp.int32, (6, ROWS), 0)
    wanted = jnp.where(column < FOUR, column % 4, 4 + column % 2)
    wanted = jnp.where(column >= SIX, column - SIX, wanted)
    chosen = jnp.where((feature == wanted) & (column < SIX + 3), 1.0, 0.0).astype(BF16)
    turn = (((0,), (0,)), ((), ()))
    first_scr[...] = lax.dot_general(in_ref[...], chosen, turn, preferred_element_type=F32).astype(BF16)
    half_mid = (mid_ref[...].astype(F32).T * 0.5).astype(BF16)
    mid_scr[...] = jnp.zeros(mid_scr.shape, BF16)
    mid_scr[0:80, 0:80] = half_mid
    mid_scr[80:160, 80:160] = half_mid
    last_scr[...] = last_ref[...]

    slot_ids = lax.broadcasted_iota(jnp.int32, (256, 128), 0).astype(jnp.int16)
    row = lax.broadcasted_iota(jnp.int32, (ROWS, 128), 0)
    row_block = jnp.where(row < FOUR, row // 4, jnp.where(row < SIX, (row - FOUR) // 2, -1)).astype(jnp.int16)
    last_rows = lax.broadcasted_iota(jnp.int32, (16, 128), 0)
    steps = 0
    for c in range(8):
        info = info_ref[c]
        trip = (jnp.max(info[0:1]).astype(jnp.int32) + SLOTS - 1) // SLOTS
        trips[c] = trip
        steps += trip
        centre = jnp.zeros((16, 128), F32)
        for d in range(3):
            centre = jnp.where(last_rows == SIX - ROWS + 16 + d, info[1 + d : 2 + d], centre)
        base_scr[c] = centre.astype(BF16)
        totals[c] = jnp.zeros((80, 128), F32)
    totals[8] = jnp.zeros((80, 128), F32)
    kept_scr[...] = jnp.zeros(kept_scr.shape, BF16)
    hidden_scr[...] = jnp.zeros(hidden_scr.shape, BF16)

    def step(n, places):
        (c0, t0), (c1, t1), (c2, t2) = places
        hidden = twice_gelu(jnp.dot(mid_scr[...], hidden_scr[...], preferred_element_type=F32))
        counts = info_ref[jnp.minimum(c2, 7), 0:1, :]
        total = totals[c2]
        for u in range(SLOTS):
            used = (SLOTS * t2 + u).astype(F32) < counts
            here = hidden[80 * (u // 2) : 80 * (u // 2) + 80, 128 * (u % 2) : 128 * (u % 2) + 128]
            total = total + jnp.where(used, here.astype(F32), 0.0)
        totals[c2] = total
        hidden = jnp.dot(first_scr[...], kept_scr[...], preferred_element_type=F32)
        hidden = twice_gelu(hidden).astype(BF16)
        for u in range(SLOTS // 2):
            hidden_scr[80 * u : 80 * u + 80, :] = hidden[:, 256 * u : 256 * u + 256]
        hot = []
        for u in range(SLOTS):
            slot = jnp.broadcast_to(slots_ref[c0, pl.ds(SLOTS * t0 + u, 1), :], (16, 128)).astype(jnp.int16)
            slot = jnp.concatenate([slot] * 16, axis=0)
            hot.append(jnp.where(slot_ids == slot, BF16(1), BF16(0)))
        found = jnp.dot(table_ref[...], jnp.concatenate(hot, axis=1), preferred_element_type=F32)
        found = found.astype(BF16)
        for u in range(SLOTS):
            code = jnp.broadcast_to(blocks_ref[c0, pl.ds(SLOTS * t0 + u, 1), :], (16, 128))
            block = (code >> 1).astype(jnp.int16)
            odd = (code & 1).astype(jnp.int16)
            same = row_block == jnp.concatenate([block] * (ROWS // 16), axis=0)
            odd = jnp.concatenate([odd] * (ROWS // 16), axis=0) == 1
            here = found[:, 128 * u : 128 * u + 128]
            here = jnp.where(odd, here[ROWS : 2 * ROWS], here[0:ROWS])
            kept_scr[0 : ROWS - 16, 128 * u : 128 * u + 128] = jnp.where(same[0 : ROWS - 16], here[0 : ROWS - 16], BF16(0))
            kept_scr[ROWS - 16 : ROWS, 128 * u : 128 * u + 128] = jnp.where(same[ROWS - 16 : ROWS], here[ROWS - 16 : ROWS], base_scr[c0])
        ended = t0 + 1 >= trips[c0]
        following = (
            jnp.minimum(jnp.where(ended, c0 + 1, c0), 7),
            jnp.where(ended, jnp.where(c0 == 7, t0, 0), t0 + 1),
        )
        return following, (c0, t0), (c1, t1)

    start = (jnp.int32(0), jnp.int32(0))
    spare = (jnp.int32(8), jnp.int32(0))
    lax.fori_loop(0, steps + 2, step, (start, spare, spare))
    last = last_scr[...]
    ordered = []
    for c in range(8):
        mean = totals[c] * (0.5 / info_ref[c, 0:1, :])
        upper = mean.astype(BF16)
        lower = (mean - upper.astype(F32)).astype(BF16)
        values = jnp.dot(last, upper, preferred_element_type=F32) + jnp.dot(
            last, lower, preferred_element_type=F32
        )
        ordered.append(values.astype(BF16))
    out_ref[...] = jnp.concatenate(ordered, axis=1)


def encode(table, slots, blocks, info, kernel_in, kernel_mid, kernel_out):
    vmem = pl.BlockSpec(memory_space=pltpu.VMEM)
    return pl.pallas_call(
        encoder_kernel,
        out_shape=pltpu.VMEM((64, 1024), BF16),
        in_specs=[vmem] * 7,
        out_specs=vmem,
        scratch_shapes=[
            pltpu.VMEM((80, ROWS), BF16),
            pltpu.VMEM((160, 160), BF16),
            pltpu.VMEM((64, 80), BF16),
            pltpu.VMEM((ROWS, 128 * SLOTS), BF16),
            pltpu.VMEM((160, 256), BF16),
            pltpu.VMEM((8, 16, 128), BF16),
            pltpu.VMEM((9, 80, 128), F32),
            pltpu.SMEM((8,), jnp.int32),
        ],
        compiler_params=pltpu.CompilerParams(vmem_limit_bytes=LIMIT),
    )(*kept(table, slots, blocks, info), *far(kernel_in, kernel_mid, kernel_out))


def halves(values):
    upper = values.astype(np.float32).astype(ml_dtypes.bfloat16)
    lower = (values - upper.astype(np.float64)).astype(np.float32).astype(ml_dtypes.bfloat16)
    return np.stack([upper, lower])


def turn(frequency, position):
    angle = 2.0 * math.pi * ((frequency * position) % GRID) / GRID
    return np.cos(angle), np.sin(angle)


def centred(index):
    return np.where(index < MODES // 2, index, index - MODES)


def complex_block(cos, sin):
    return np.stack([np.stack([cos, sin], -1), np.stack([-sin, cos], -1)], -2)


@functools.lru_cache(None)
def third_table():
    cos, sin = turn(np.arange(16)[:, None], np.arange(64)[None, :])
    parts = np.stack([cos, -sin]).reshape(2, 16, 8, 8)
    full = np.einsum("akgz,cd->akcgdz", parts, np.eye(2))
    return full.reshape(64, 128)


@functools.lru_cache(None)
def second_table():
    j = np.arange(16)
    cos, sin = turn(centred(j)[:, None], np.arange(64)[None, :])
    both = complex_block(cos, sin).reshape(8, 2, 4, 16, 2, 2)
    full = np.einsum("gleyab,xw->lgaxebwy", both, np.eye(8))
    return full.reshape(2, 128, 1024)


@functools.lru_cache(None)
def first_table():
    i = np.arange(16)
    cos, sin = turn(centred(i)[:, None], np.arange(64)[None, :])
    both = complex_block(cos, sin).reshape(8, 2, 8, 8, 2, 2)
    return np.einsum("hltxab->tlhabx", both).reshape(8, 2, 16, 16)


def placed(values):
    return np.tile(np.moveaxis(halves(values), 0, 1), (1, 1, 1, 1, 8))


@functools.lru_cache(None)
def pair_table():
    out = np.zeros((4, 8, 8, 2, 8, 8, 2))
    for il in range(2):
        for jl in range(2):
            for h in range(8):
                for g in range(8):
                    i, j = 2 * h + il, 2 * g + jl
                    if i == 8 or j == 8:
                        continue
                    ni, nj = (16 - i) % 16, (16 - j) % 16
                    assert ni % 2 == il and nj % 2 == jl
                    for a in range(2):
                        out[2 * il + jl, g, h, a, nj // 2, ni // 2, a] = 1.0 - 2.0 * a
    return out.reshape(4, 128, 128)


def dotf(a, b):
    return jnp.dot(a, b, preferred_element_type=F32)


def dott(a, b):
    return lax.dot_general(a, b, (((1,), (1,)), ((), ())), preferred_element_type=F32)


def split(values):
    upper = values.astype(BF16)
    return upper, (values - upper.astype(F32)).astype(BF16)


def spectral_kernel(
    ordered_ref, rank_ref, skip_ref, weight_any, third_any, back_any, second_any, first_any, firstt_any, pair_any,
    out_ref,
    weight_ref, third_ref, back_ref, second_ref, first_ref, firstt_ref, pair_ref,
    latent, l_msg, r1, w_msg, rw, s_msg, r3, mixing, mixed_scr, n_msg, r5, g_msg, r6, b_msg, r8, ended, skip,
    send, recv, loaded,
):
    me_x = lax.axis_index("gx")
    me_y = lax.axis_index("gy")
    me_z = lax.axis_index("gz")
    me_q = me_y * GZ + me_z
    columns = [(y, z) for y in range(GY) for z in range(GZ) if y or z]
    columns.sort(key=lambda o: -(2 * min(o[0], GY - o[0]) + min(o[1], GZ - o[1])))

    def across(o):
        y, z = lax.rem(me_y + o[0], GY), lax.rem(me_z + o[1], GZ)
        return {"gy": y, "gz": z}, y * GZ + z, me_q

    def along_x(o):
        peer = lax.rem(me_x + o, GX)
        return {"gx": peer}, peer, me_x

    planes = [across(o) for o in columns]
    lines = [along_x(o) for o in (4, 3, 5, 2, 6, 1, 7)]
    barrier = pltpu.get_barrier_semaphore()
    for device, _, _ in lines + planes:
        pl.semaphore_signal(barrier, inc=1, device_id=device, device_id_type=MESH)
    constants = (weight_any, third_any, back_any, second_any, first_any, firstt_any, pair_any)
    copies = (weight_ref, third_ref, back_ref, second_ref, first_ref, firstt_ref, pair_ref)
    loads = [pltpu.make_async_copy(c, d, loaded.at[n]) for n, (c, d) in enumerate(zip(constants, copies))]
    for load in loads:
        load.start()
    order = lax.broadcasted_iota(jnp.int32, (1024, 128), 0).astype(F32)
    for z in range(8):
        moved = jnp.where(order == rank_ref[0:1, 128 * z : 128 * z + 128], 1.0, 0.0).astype(BF16)
        latent[64 * z : 64 * z + 64] = dotf(ordered_ref[...], moved)
    for q in range(32):
        both = [latent[pl.ds(2 * q + c, 8, stride=64), :] for c in range(2)]
        l_msg[q] = jnp.concatenate(both, axis=0).astype(BF16)
    pl.semaphore_wait(barrier, len(planes + lines))

    sends = []

    def start(stage, peers, source, target):
        for device, peer, me in peers:
            pltpu.make_async_remote_copy(
                src_ref=source(peer),
                dst_ref=target.at[me],
                send_sem=send.at[stage],
                recv_sem=recv.at[stage],
                device_id=device,
                device_id_type=MESH,
            ).start()
        everything = target.at[pl.ds(0, len(peers))]
        sends.append((stage, everything))
        return stage, everything

    def finish(pending):
        stage, everything = pending
        pltpu.make_async_copy(everything, everything, recv.at[stage]).wait()

    rows128 = lax.broadcasted_iota(jnp.int32, (128, 128), 0)
    lanes128 = lax.broadcasted_iota(jnp.int32, (128, 128), 1)
    same = rows128 // 16 == lanes128 // 16

    def spread_blocks(ref, part, l):
        small = ref[me_x, part, l].astype(F32)
        return jnp.where(same, jnp.concatenate([small] * 8, axis=0), 0.0).astype(BF16)

    first = start(0, planes, lambda p: l_msg.at[p], r1)
    r1[me_q] = l_msg[me_q]
    loads[0].wait()
    forth = regroup()
    for l in range(2):
        wide = jnp.concatenate(
            [weight_ref[b, 8 * l : 8 * l + 8].astype(F32).reshape(512, 64) for b in range(2)], axis=1
        ).astype(BF16)
        w_msg[:, 16 * l : 16 * l + 16, :] = dotf(forth, wide).astype(BF16).reshape(32, 16, 128)
    weights = start(1, planes, lambda p: w_msg.at[p], rw)
    rw[me_q] = w_msg[me_q]
    for load in loads[1:]:
        load.wait()
    first_tab = [[spread_blocks(first_ref, p, l) for l in range(2)] for p in range(2)]
    back_tab = [[spread_blocks(firstt_ref, p, l) for l in range(2)] for p in range(2)]
    skip_t = skip_ref[...].astype(F32).T.astype(BF16)
    for z in range(8):
        skip[z] = dotf(skip_t, latent[64 * z : 64 * z + 64].astype(BF16))
    finish(first)

    pieces = []
    for e in range(4):
        values = r1[8 * e : 8 * e + 8].reshape(128, 128)
        piece = dotf(third_ref[0], values) + dotf(third_ref[1], values)
        pieces += [piece[0:32], piece[32:64]]
    wide = jnp.concatenate(pieces, axis=1).astype(BF16)
    rows = jnp.concatenate(
        [dott(second_ref[0, l], wide) + dott(second_ref[1, l], wide) for l in range(2)], axis=1
    )
    upper, lower = split(rows)
    partial = jnp.concatenate(
        [
            dotf(first_tab[0][l], upper) + dotf(first_tab[0][l], lower) + dotf(first_tab[1][l], upper)
            for l in range(2)
        ],
        axis=1,
    )
    s_msg[...] = partial.astype(BF16).reshape(8, 16, 128)

    third = start(2, lines, lambda p: s_msg.at[p], r3)
    r3[me_x] = s_msg[me_x]
    finish(weights)
    for h in range(8):
        parts = [
            rw[e * 8 + h, 8 * p : 8 * p + 8, :].astype(F32) for p in range(4) for e in range(4)
        ]
        mixing[h] = jnp.concatenate(parts, axis=0).T.astype(BF16)
    finish(third)
    modes = jnp.sum(r3[...].astype(F32), axis=0)

    own = rows128 // 2 == lanes128 // 2
    even = lax.broadcasted_iota(jnp.int32, (64, 128), 1) % 2 == 0
    products = []
    for h in range(8):
        expanded = jnp.concatenate(
            [
                jnp.where(own, jnp.broadcast_to(modes[2 * h + a : 2 * h + a + 1], (128, 128)), 0.0)
                for a in range(2)
            ],
            axis=0,
        ).astype(BF16)
        products.append(dott(mixing[h], expanded))
    for h, product in enumerate(products):
        mixed_scr[h, 0:64] = product[0:64, 0:128] - product[64:128, 128:256]
        mixed_scr[h, 64:128] = product[64:128, 0:128] + product[0:64, 128:256]
    turned = [
        jnp.where(even, mixed_scr[h, pl.ds(0, 64, stride=2), :], mixed_scr[h, pl.ds(1, 64, stride=2), :])
        for h in range(8)
    ]
    place = lax.broadcasted_iota(jnp.int32, (512, 512), 0)
    source = lax.broadcasted_iota(jnp.int32, (512, 512), 1)
    wanted = ((place >> 1) & 7) * 64 + (place & 1) * 32 + (place >> 4)
    order = jnp.where(wanted == source, 1.0, 0.0).astype(BF16)
    turned = jnp.concatenate(turned, axis=0).astype(BF16)
    n_msg[...] = dotf(order, turned).astype(BF16).reshape(32, 16, 128)

    fourth = start(3, planes, lambda p: n_msg.at[p], r5)
    r5[me_q] = n_msg[me_q]
    finish(fourth)
    mixed = jnp.sum(r5[...].astype(F32), axis=0)
    zero_rows = lax.broadcasted_iota(jnp.int32, (16, 128), 0)
    zero_lanes = lax.broadcasted_iota(jnp.int32, (16, 128), 1)
    mixed = jnp.where((zero_rows < 2) & (zero_lanes < 2) & (me_x == 0), 0.0, mixed)
    g_msg[...] = mixed.astype(BF16)

    fifth = start(4, lines, lambda p: g_msg, r6)
    r6[me_x] = g_msg[...]
    finish(fifth)
    field = r6[...].reshape(128, 128)
    along = (
        dotf(back_tab[0][0], field[:, 0:64])
        + dotf(back_tab[1][0], field[:, 0:64])
        + dotf(back_tab[0][1], field[:, 64:128])
        + dotf(back_tab[1][1], field[:, 64:128])
    )
    upper, lower = split(along.T)
    plane = (
        dotf(upper[0:32], second_ref[0, 0])
        + dotf(lower[0:32], second_ref[0, 0])
        + dotf(upper[0:32], second_ref[1, 0])
        + dotf(upper[32:64], second_ref[0, 1])
        + dotf(lower[32:64], second_ref[0, 1])
        + dotf(upper[32:64], second_ref[1, 1])
    )
    scale = 1.0 / GRID**3
    plane_rows = lax.broadcasted_iota(jnp.int32, (32, 1024), 0)
    plane = (plane * jnp.where(plane_rows < 2, scale, 2.0 * scale)).astype(BF16)
    wide_field = field.astype(F32)
    paired = jnp.zeros((128, 128), F32)
    for p in range(4):
        paired = jnp.where(lanes128 // 32 == p, dotf(pair_ref[p], field), paired)
    low = (lanes128 // 2) % 16 == 0
    power = jnp.where(low, 0.5 * wide_field * (wide_field + paired), 2.0 * wide_field * wide_field)
    power = jnp.sum(power, axis=0, keepdims=True)
    for shift in (64, 32, 16, 8, 4, 2):
        power = power + pltpu.roll(power, shift, 1)
    lane = lax.broadcasted_iota(jnp.int32, (1, 128), 1)
    power = jnp.where(lane % 2 == (lane // 8) % 2, power, pltpu.roll(power, 1, 1))
    variance = jnp.broadcast_to(power, (128, 128)).T * (scale * scale)
    inverse = 1.0 / jnp.sqrt(variance + NORM_FLOOR)
    for e in range(4):
        part = jnp.concatenate(
            [plane[:, (2 * e + b) * 128 : (2 * e + b + 1) * 128] for b in range(2)], axis=0
        )
        branch = (dotf(back_ref[0], part) + dotf(back_ref[1], part)) * inverse
        b_msg[8 * e : 8 * e + 8] = branch.astype(BF16).reshape(8, 16, 128)

    sixth = start(5, planes, lambda p: b_msg.at[p], r8)
    r8[me_q] = b_msg[me_q]
    finish(sixth)
    ended[...] = r8[...].reshape(512, 128).astype(F32)
    for z in range(8):
        out_ref[z] = ended[pl.ds(z, 64, stride=8), :] + skip[z]
    for stage, everything in sends:
        pltpu.make_async_copy(everything, everything, send.at[stage]).wait()


def final_kernel(cells_ref, out_ref):
    for z in range(8):
        out_ref[:, z, :] = gelu(cells_ref[z]).T


def final(cells):
    vmem = pl.BlockSpec(memory_space=pltpu.VMEM)
    return pl.pallas_call(
        final_kernel, out_shape=jax.ShapeDtypeStruct((128, 8, 64), F32), in_specs=[vmem], out_specs=vmem,
        compiler_params=pltpu.CompilerParams(vmem_limit_bytes=LIMIT),
    )(*kept(cells))


def spectral_layer(ordered, rank, skip_w, weight, *tables):
    vmem = pl.BlockSpec(memory_space=pltpu.VMEM)
    own = [pltpu.VMEM(array.shape, array.dtype) for array in (weight,) + tables]
    return pl.pallas_call(
        spectral_kernel,
        out_shape=pltpu.VMEM((8, 64, 128), F32),
        in_specs=[vmem] * 3 + [pl.BlockSpec(memory_space=pltpu.HBM)] * 7,
        out_specs=vmem,
        scratch_shapes=own
        + [
            pltpu.VMEM((512, 128), F32),
            pltpu.VMEM((32, 16, 128), BF16),
            pltpu.VMEM((32, 16, 128), BF16),
            pltpu.VMEM((32, 32, 128), BF16),
            pltpu.VMEM((32, 32, 128), BF16),
            pltpu.VMEM((8, 16, 128), BF16),
            pltpu.VMEM((8, 16, 128), BF16),
            pltpu.VMEM((8, 128, 128), BF16),
            pltpu.VMEM((8, 128, 128), F32),
            pltpu.VMEM((32, 16, 128), BF16),
            pltpu.VMEM((32, 16, 128), BF16),
            pltpu.VMEM((16, 128), BF16),
            pltpu.VMEM((8, 16, 128), BF16),
            pltpu.VMEM((32, 16, 128), BF16),
            pltpu.VMEM((32, 16, 128), BF16),
            pltpu.VMEM((512, 128), F32),
            pltpu.VMEM((8, 64, 128), F32),
            pltpu.SemaphoreType.DMA((6,)),
            pltpu.SemaphoreType.DMA((6,)),
            pltpu.SemaphoreType.DMA((7,)),
        ],
        compiler_params=pltpu.CompilerParams(collective_id=0, has_side_effects=True, vmem_limit_bytes=LIMIT),
    )(*kept(ordered, rank), *far(skip_w, weight, *tables))


def body(point_data, neighbours, counts, kernel_in, kernel_mid, kernel_out, spectral, skip_weight):
    cells_x, cells_y, cells_z = neighbours.shape[1:4]
    made = halo(
        jnp.transpose(point_data, (1, 0, 2)),
        neighbours.reshape(-1, NB),
        jnp.transpose(counts[0], (0, 2, 1)),
    )
    ordered = encode(*made[:4], kernel_in, kernel_mid, kernel_out.T)
    third = third_table()
    by_place = first_table()
    cells = spectral_layer(
        ordered,
        made[4],
        skip_weight,
        spectral.reshape(2, 16, 64, 64),
        jnp.asarray(halves(third)),
        jnp.asarray(halves(third.T)),
        jnp.asarray(halves(second_table())),
        jnp.asarray(placed(by_place)),
        jnp.asarray(placed(np.swapaxes(by_place, 2, 3))),
        jnp.asarray(pair_table().astype(ml_dtypes.bfloat16)),
    )
    out = final(cells)
    return out.reshape(1, cells_x, cells_y, cells_z, -1)


def solution(mesh):
    in_specs = (
        P(None, None, ("gx", "gy", "gz")),
        P(None, "gx", "gy", "gz", None),
        P(None, "gx", "gy", "gz"),
        P(),
        P(),
        P(),
        P(None, "gz", "gx", "gy", None, None),
        P(),
    )
    out_specs = P(None, "gx", "gy", "gz", None)
    return jax.shard_map(body, mesh=mesh, in_specs=in_specs, out_specs=out_specs, check_vma=False)
```

```python
import functools
import math

import jax
import jax.numpy as jnp
import ml_dtypes
import numpy as np
from jax import lax
from jax.experimental import pallas as pl
from jax.experimental.pallas import tpu as pltpu
from jax.sharding import PartitionSpec as P

GRID = 64
LIMIT = 24 * 2**20
MODES = 16
NB = 32
NORM_FLOOR = 1.0
GX, GY, GZ = 8, 4, 8
F32 = jnp.float32
BF16 = jnp.bfloat16
MESH = pl.DeviceIdType.MESH


def gelu(v):
    inner = v * (0.7978845608028654 + 0.035677408136300125 * (v * v))
    half = 0.5 * v
    return half + half * jnp.tanh(inner)


def twice_gelu(v):
    if not GELU16:
        return v + v * jnp.tanh(v * (0.7978845608028654 + 0.035677408136300125 * (v * v)))
    v = v.astype(BF16)
    inner = v * (BF16(0.7978845608028654) + BF16(0.035677408136300125) * (v * v))
    return v + v * jnp.tanh(inner)


SLOTS = 4
ROWS = 176
FOUR, SIX = 108, 162
GELU16 = True
OFFSETS = [(dx, dy, dz) for dx in (-1, 0, 1) for dy in (-1, 0, 1) for dz in (-1, 0, 1)]


def kept(*arrays):
    return [pltpu.with_memory_space_constraint(array, pltpu.VMEM) for array in arrays]


def far(*arrays):
    return [pltpu.with_memory_space_constraint(array, pltpu.HBM) for array in arrays]


def regroup():
    row = lax.broadcasted_iota(jnp.int32, (512, 512), 0)
    column = lax.broadcasted_iota(jnp.int32, (512, 512), 1)
    wanted = ((row >> 1) & 7) * 64 + (row >> 4) * 2 + (row & 1)
    return jnp.where(wanted == column, 1.0, 0.0).astype(BF16)


def halo_kernel(
    points_any, near_any, counts_any, in_any, mid_any, last_any, skip_any,
    table_ref, slots_ref, blocks_ref, info_ref, rank_ref, first_out, mid_out, last_out, skip_out,
    points_ref, near_ref, counts_ref, in_ref, mid_ref, skip_ref, main, send, recv, loaded,
):
    me_x = lax.axis_index("gx")
    me_y = lax.axis_index("gy")
    me_z = lax.axis_index("gz")

    def device(offset):
        dx, dy, dz = offset
        return {
            "gx": lax.rem(me_x + dx + GX, GX),
            "gy": lax.rem(me_y + dy + GY, GY),
            "gz": lax.rem(me_z + dz + GZ, GZ),
        }

    barrier = pltpu.get_barrier_semaphore()
    peers = [o for o in OFFSETS if o != (0, 0, 0)]
    for offset in peers:
        pl.semaphore_signal(barrier, inc=1, device_id=device(offset), device_id_type=MESH)
    moves = (
        (points_any, points_ref), (counts_any, counts_ref), (near_any, near_ref), (in_any, in_ref),
        (mid_any, mid_ref), (last_any, last_out), (skip_any, skip_ref),
    )
    loads = [pltpu.make_async_copy(c, d, loaded.at[n]) for n, (c, d) in enumerate(moves)]
    for load in loads:
        load.start()
    loads[0].wait()

    main[13] = jnp.concatenate([points_ref[d] for d in range(6)] + [jnp.zeros((2, 512), F32)], axis=0).astype(BF16)
    pl.semaphore_wait(barrier, len(peers))
    for offset in sorted(peers, key=lambda o: -sum(abs(d) for d in o)):
        slot = 26 - OFFSETS.index(offset)
        pltpu.make_async_remote_copy(
            src_ref=main.at[13],
            dst_ref=main.at[slot],
            send_sem=send.at[0],
            recv_sem=recv.at[0],
            device_id=device(offset),
            device_id_type=MESH,
        ).start()
    everything = main.at[pl.ds(0, 26)]

    for load in loads[1:]:
        load.wait()
    lane = lax.broadcasted_iota(jnp.int32, (1, 1024), 1)
    counts = jnp.concatenate([counts_ref[x].astype(F32) for x in range(8)], axis=1)
    counts = jnp.concatenate([counts[z : z + 1] for z in range(8)], axis=1)
    key = counts * 1024.0 + (1023 - lane).astype(F32)
    ones = jnp.ones((8, 128), BF16)
    rank = jnp.zeros((8, 1024), F32)
    for m in range(8):
        tall = jnp.broadcast_to(key[:, 128 * m : 128 * m + 128], (128, 128)).T
        ahead = jnp.concatenate(
            [
                jnp.where(tall > key[:, 128 * n : 128 * n + 128], 1.0, 0.0).astype(BF16)
                for n in range(8)
            ],
            axis=1,
        )
        rank = rank + jnp.dot(ones, ahead, preferred_element_type=F32)
    rank_ref[...] = rank
    near = jnp.concatenate(
        [near_ref[pl.ds(z, 128, stride=8), :].astype(F32).T for z in range(8)], axis=1
    ).astype(jnp.int32)
    owner = near >> 9
    part = near & 511
    block = ((((owner >> 5) - me_x + 1) * 3) + ((owner >> 3) & 3) - me_y + 1) * 3 + (owner & 7) - me_z + 1
    code = jnp.clip(block, 0, 26) * 2 + (part >> 8)
    place_y = (me_y * 16 + (lane & 15)).astype(F32)
    place_x = (me_x * 8 + ((lane >> 4) & 7)).astype(F32)
    place_z = (me_z * 8 + (lane >> 7)).astype(F32)
    centres = [-(place + 0.5) / GRID for place in (place_x, place_y, place_z)]
    rows = jnp.concatenate(
        [(part & 255).astype(F32), code.astype(F32), counts] + centres + [jnp.zeros((12, 1024), F32)], axis=0
    ).astype(BF16)
    order = lax.broadcasted_iota(jnp.int32, (128, 1024), 0).astype(F32)
    wide_rank = rank[0:1]
    for t in range(8):
        moved = jnp.where(order + 128.0 * t == wide_rank, 1.0, 0.0).astype(BF16)
        moved = lax.dot_general(rows, moved, (((1,), (1,)), ((), ())), preferred_element_type=F32)
        slots_ref[t] = moved[0:32].astype(jnp.int32)
        blocks_ref[t] = moved[32:64].astype(jnp.int32)
        info_ref[t] = moved[64:72]

    column = lax.broadcasted_iota(jnp.int32, (6, ROWS), 1)
    feature = lax.broadcasted_iota(jnp.int32, (6, ROWS), 0)
    wanted = jnp.where(column < FOUR, column % 4, 4 + column % 2)
    wanted = jnp.where(column >= SIX, column - SIX, wanted)
    chosen = jnp.where((feature == wanted) & (column < SIX + 3), 1.0, 0.0).astype(BF16)
    turn = (((0,), (0,)), ((), ()))
    first_out[...] = lax.dot_general(in_ref[...], chosen, turn, preferred_element_type=F32).astype(BF16)
    half_mid = (mid_ref[...].astype(F32).T * 0.5).astype(BF16)
    mid_out[...] = jnp.zeros(mid_out.shape, BF16)
    mid_out[0:80, 0:80] = half_mid
    mid_out[80:160, 80:160] = half_mid

    skip_out[...] = skip_ref[...].astype(F32).T.astype(BF16)

    pltpu.make_async_copy(everything, everything, recv.at[0]).wait()
    blocks = [main[b].astype(F32) for b in range(27)]
    rows = [block[0:4] for block in blocks] + [block[4:6] for block in blocks]
    rows.append(jnp.zeros((ROWS - SIX, 512), F32))
    rows = jnp.concatenate(rows, axis=0).astype(BF16)
    table_ref[0:ROWS, :] = rows[:, 0:256]
    table_ref[ROWS : 2 * ROWS, :] = rows[:, 256:512]
    pltpu.make_async_copy(everything, everything, send.at[0]).wait()


def halo(points, near, counts, kernel_in, kernel_mid, last, skip_w):
    vmem = pl.BlockSpec(memory_space=pltpu.VMEM)
    return pl.pallas_call(
        halo_kernel,
        out_shape=[
            pltpu.VMEM((2 * ROWS, 256), BF16),
            pltpu.VMEM((8, NB, 128), jnp.int32),
            pltpu.VMEM((8, NB, 128), jnp.int32),
            pltpu.VMEM((8, 8, 128), F32),
            pltpu.VMEM((8, 1024), F32),
            pltpu.VMEM((80, ROWS), BF16),
            pltpu.VMEM((160, 160), BF16),
            pltpu.VMEM((64, 80), BF16),
            pltpu.VMEM((64, 64), BF16),
        ],
        in_specs=[pl.BlockSpec(memory_space=pl.ANY)] * 7,
        out_specs=[vmem] * 9,
        scratch_shapes=[
            pltpu.VMEM(points.shape, F32),
            pltpu.VMEM(near.shape, jnp.int32),
            pltpu.VMEM(counts.shape, jnp.int32),
            pltpu.VMEM(kernel_in.shape, BF16),
            pltpu.VMEM(kernel_mid.shape, BF16),
            pltpu.VMEM(skip_w.shape, BF16),
            pltpu.VMEM((27, 8, 512), BF16),
            pltpu.SemaphoreType.DMA((1,)),
            pltpu.SemaphoreType.DMA((1,)),
            pltpu.SemaphoreType.DMA((7,)),
        ],
        compiler_params=pltpu.CompilerParams(collective_id=1, has_side_effects=True, vmem_limit_bytes=LIMIT),
    )(*far(points, near, counts, kernel_in, kernel_mid, last, skip_w))


def encoder_kernel(
    table_ref, slots_ref, blocks_ref, info_ref, first_scr, mid_scr, last_scr, out_ref,
    kept_scr, hidden_scr, base_scr, totals, trips,
):
    slot_ids = lax.broadcasted_iota(jnp.int32, (256, 128), 0).astype(jnp.int16)
    row = lax.broadcasted_iota(jnp.int32, (ROWS, 128), 0)
    row_block = jnp.where(row < FOUR, row // 4, jnp.where(row < SIX, (row - FOUR) // 2, -1)).astype(jnp.int16)
    last_rows = lax.broadcasted_iota(jnp.int32, (16, 128), 0)
    steps = 0
    for c in range(8):
        info = info_ref[c]
        trip = (jnp.max(info[0:1]).astype(jnp.int32) + SLOTS - 1) // SLOTS
        trips[c] = trip
        steps += trip
        centre = jnp.zeros((16, 128), F32)
        for d in range(3):
            centre = jnp.where(last_rows == SIX - ROWS + 16 + d, info[1 + d : 2 + d], centre)
        base_scr[c] = centre.astype(BF16)
        totals[c] = jnp.zeros((80, 128), F32)
    totals[8] = jnp.zeros((80, 128), F32)
    kept_scr[...] = jnp.zeros(kept_scr.shape, BF16)
    hidden_scr[...] = jnp.zeros(hidden_scr.shape, BF16)

    def step(n, places):
        (c0, t0), (c1, t1), (c2, t2) = places
        hidden = twice_gelu(jnp.dot(mid_scr[...], hidden_scr[...], preferred_element_type=F32))
        counts = info_ref[jnp.minimum(c2, 7), 0:1, :]
        total = totals[c2]
        for u in range(SLOTS):
            used = (SLOTS * t2 + u).astype(F32) < counts
            here = hidden[80 * (u // 2) : 80 * (u // 2) + 80, 128 * (u % 2) : 128 * (u % 2) + 128]
            total = total + jnp.where(used, here.astype(F32), 0.0)
        totals[c2] = total
        hidden = jnp.dot(first_scr[...], kept_scr[...], preferred_element_type=F32)
        hidden = twice_gelu(hidden).astype(BF16)
        for u in range(SLOTS // 2):
            hidden_scr[80 * u : 80 * u + 80, :] = hidden[:, 256 * u : 256 * u + 256]
        hot = []
        for u in range(SLOTS):
            slot = jnp.broadcast_to(slots_ref[c0, pl.ds(SLOTS * t0 + u, 1), :], (16, 128)).astype(jnp.int16)
            slot = jnp.concatenate([slot] * 16, axis=0)
            hot.append(jnp.where(slot_ids == slot, BF16(1), BF16(0)))
        found = jnp.dot(table_ref[...], jnp.concatenate(hot, axis=1), preferred_element_type=F32)
        found = found.astype(BF16)
        for u in range(SLOTS):
            code = jnp.broadcast_to(blocks_ref[c0, pl.ds(SLOTS * t0 + u, 1), :], (16, 128))
            block = (code >> 1).astype(jnp.int16)
            odd = (code & 1).astype(jnp.int16)
            same = row_block == jnp.concatenate([block] * (ROWS // 16), axis=0)
            odd = jnp.concatenate([odd] * (ROWS // 16), axis=0) == 1
            here = found[:, 128 * u : 128 * u + 128]
            here = jnp.where(odd, here[ROWS : 2 * ROWS], here[0:ROWS])
            kept_scr[0 : ROWS - 16, 128 * u : 128 * u + 128] = jnp.where(same[0 : ROWS - 16], here[0 : ROWS - 16], BF16(0))
            kept_scr[ROWS - 16 : ROWS, 128 * u : 128 * u + 128] = jnp.where(same[ROWS - 16 : ROWS], here[ROWS - 16 : ROWS], base_scr[c0])
        ended = t0 + 1 >= trips[c0]
        following = (
            jnp.minimum(jnp.where(ended, c0 + 1, c0), 7),
            jnp.where(ended, jnp.where(c0 == 7, t0, 0), t0 + 1),
        )
        return following, (c0, t0), (c1, t1)

    start = (jnp.int32(0), jnp.int32(0))
    spare = (jnp.int32(8), jnp.int32(0))
    lax.fori_loop(0, steps + 2, step, (start, spare, spare))
    last = last_scr[...]
    ordered = []
    for c in range(8):
        mean = totals[c] * (0.5 / info_ref[c, 0:1, :])
        upper = mean.astype(BF16)
        lower = (mean - upper.astype(F32)).astype(BF16)
        values = jnp.dot(last, upper, preferred_element_type=F32) + jnp.dot(
            last, lower, preferred_element_type=F32
        )
        ordered.append(values.astype(BF16))
    out_ref[...] = jnp.concatenate(ordered, axis=1)


def encode(*made):
    vmem = pl.BlockSpec(memory_space=pltpu.VMEM)
    return pl.pallas_call(
        encoder_kernel,
        out_shape=pltpu.VMEM((64, 1024), BF16),
        in_specs=[vmem] * 7,
        out_specs=vmem,
        scratch_shapes=[
            pltpu.VMEM((ROWS, 128 * SLOTS), BF16),
            pltpu.VMEM((160, 256), BF16),
            pltpu.VMEM((8, 16, 128), BF16),
            pltpu.VMEM((9, 80, 128), F32),
            pltpu.SMEM((8,), jnp.int32),
        ],
        compiler_params=pltpu.CompilerParams(vmem_limit_bytes=LIMIT),
    )(*kept(*made))


def halves(values):
    upper = values.astype(np.float32).astype(ml_dtypes.bfloat16)
    lower = (values - upper.astype(np.float64)).astype(np.float32).astype(ml_dtypes.bfloat16)
    return np.stack([upper, lower])


def turn(frequency, position):
    angle = 2.0 * math.pi * ((frequency * position) % GRID) / GRID
    return np.cos(angle), np.sin(angle)


def centred(index):
    return np.where(index < MODES // 2, index, index - MODES)


def complex_block(cos, sin):
    return np.stack([np.stack([cos, sin], -1), np.stack([-sin, cos], -1)], -2)


@functools.lru_cache(None)
def third_table():
    cos, sin = turn(np.arange(16)[:, None], np.arange(64)[None, :])
    parts = np.stack([cos, -sin]).reshape(2, 16, 8, 8)
    full = np.einsum("akgz,cd->akcgdz", parts, np.eye(2))
    return full.reshape(64, 128)


@functools.lru_cache(None)
def second_table():
    j = np.arange(16)
    cos, sin = turn(centred(j)[:, None], np.arange(64)[None, :])
    both = complex_block(cos, sin).reshape(8, 2, 4, 16, 2, 2)
    full = np.einsum("gleyab,xw->lgaxebwy", both, np.eye(8))
    return full.reshape(2, 128, 1024)


@functools.lru_cache(None)
def first_table():
    i = np.arange(16)
    cos, sin = turn(centred(i)[:, None], np.arange(64)[None, :])
    both = complex_block(cos, sin).reshape(8, 2, 8, 8, 2, 2)
    return np.einsum("hltxab->tlhabx", both).reshape(8, 2, 16, 16)


def placed(values):
    return np.tile(np.moveaxis(halves(values), 0, 1), (1, 1, 1, 1, 8))


@functools.lru_cache(None)
def pair_table():
    out = np.zeros((4, 8, 8, 2, 8, 8, 2))
    for il in range(2):
        for jl in range(2):
            for h in range(8):
                for g in range(8):
                    i, j = 2 * h + il, 2 * g + jl
                    if i == 8 or j == 8:
                        continue
                    ni, nj = (16 - i) % 16, (16 - j) % 16
                    assert ni % 2 == il and nj % 2 == jl
                    for a in range(2):
                        out[2 * il + jl, g, h, a, nj // 2, ni // 2, a] = 1.0 - 2.0 * a
    return out.reshape(4, 128, 128)


def dotf(a, b):
    return jnp.dot(a, b, preferred_element_type=F32)


def dott(a, b):
    return lax.dot_general(a, b, (((1,), (1,)), ((), ())), preferred_element_type=F32)


def split(values):
    upper = values.astype(BF16)
    return upper, (values - upper.astype(F32)).astype(BF16)


def spectral_kernel(
    ordered_ref, rank_ref, skip_ref, weight_any, third_any, back_any, second_any, first_any, firstt_any, pair_any,
    out_ref,
    weight_ref, third_ref, back_ref, second_ref, first_ref, firstt_ref, pair_ref,
    latent, l_msg, r1, w_msg, rw, s_msg, r3, mixing, mixed_scr, n_msg, r5, g_msg, r6, b_msg, r8, ended, skip,
    send, recv, loaded,
):
    me_x = lax.axis_index("gx")
    me_y = lax.axis_index("gy")
    me_z = lax.axis_index("gz")
    me_q = me_y * GZ + me_z
    columns = [(y, z) for y in range(GY) for z in range(GZ) if y or z]
    columns.sort(key=lambda o: -(2 * min(o[0], GY - o[0]) + min(o[1], GZ - o[1])))

    def across(o):
        y, z = lax.rem(me_y + o[0], GY), lax.rem(me_z + o[1], GZ)
        return {"gy": y, "gz": z}, y * GZ + z, me_q

    def along_x(o):
        peer = lax.rem(me_x + o, GX)
        return {"gx": peer}, peer, me_x

    planes = [across(o) for o in columns]
    lines = [along_x(o) for o in (4, 3, 5, 2, 6, 1, 7)]
    barrier = pltpu.get_barrier_semaphore()
    for device, _, _ in lines + planes:
        pl.semaphore_signal(barrier, inc=1, device_id=device, device_id_type=MESH)
    constants = (weight_any, third_any, back_any, second_any, first_any, firstt_any, pair_any)
    copies = (weight_ref, third_ref, back_ref, second_ref, first_ref, firstt_ref, pair_ref)
    loads = [pltpu.make_async_copy(c, d, loaded.at[n]) for n, (c, d) in enumerate(zip(constants, copies))]
    for load in loads:
        load.start()
    order = lax.broadcasted_iota(jnp.int32, (1024, 128), 0).astype(F32)
    for z in range(8):
        moved = jnp.where(order == rank_ref[0:1, 128 * z : 128 * z + 128], 1.0, 0.0).astype(BF16)
        latent[64 * z : 64 * z + 64] = dotf(ordered_ref[...], moved)
    for q in range(32):
        both = [latent[pl.ds(2 * q + c, 8, stride=64), :] for c in range(2)]
        l_msg[q] = jnp.concatenate(both, axis=0).astype(BF16)
    pl.semaphore_wait(barrier, len(planes + lines))

    sends = []

    def start(stage, peers, source, target):
        for device, peer, me in peers:
            pltpu.make_async_remote_copy(
                src_ref=source(peer),
                dst_ref=target.at[me],
                send_sem=send.at[stage],
                recv_sem=recv.at[stage],
                device_id=device,
                device_id_type=MESH,
            ).start()
        everything = target.at[pl.ds(0, len(peers))]
        sends.append((stage, everything))
        return stage, everything

    def finish(pending):
        stage, everything = pending
        pltpu.make_async_copy(everything, everything, recv.at[stage]).wait()

    rows128 = lax.broadcasted_iota(jnp.int32, (128, 128), 0)
    lanes128 = lax.broadcasted_iota(jnp.int32, (128, 128), 1)
    same = rows128 // 16 == lanes128 // 16

    def spread_blocks(ref, part, l):
        small = ref[me_x, part, l].astype(F32)
        return jnp.where(same, jnp.concatenate([small] * 8, axis=0), 0.0).astype(BF16)

    first = start(0, planes, lambda p: l_msg.at[p], r1)
    r1[me_q] = l_msg[me_q]
    loads[0].wait()
    forth = regroup()
    for l in range(2):
        wide = jnp.concatenate(
            [weight_ref[b, 8 * l : 8 * l + 8].astype(F32).reshape(512, 64) for b in range(2)], axis=1
        ).astype(BF16)
        w_msg[:, 16 * l : 16 * l + 16, :] = dotf(forth, wide).astype(BF16).reshape(32, 16, 128)
    weights = start(1, planes, lambda p: w_msg.at[p], rw)
    rw[me_q] = w_msg[me_q]
    for load in loads[1:]:
        load.wait()
    first_tab = [[spread_blocks(first_ref, p, l) for l in range(2)] for p in range(2)]
    back_tab = [[spread_blocks(firstt_ref, p, l) for l in range(2)] for p in range(2)]
    for z in range(8):
        skip[z] = dotf(skip_ref[...], latent[64 * z : 64 * z + 64].astype(BF16))
    finish(first)

    pieces = []
    for e in range(4):
        values = r1[8 * e : 8 * e + 8].reshape(128, 128)
        piece = dotf(third_ref[0], values) + dotf(third_ref[1], values)
        pieces += [piece[0:32], piece[32:64]]
    wide = jnp.concatenate(pieces, axis=1).astype(BF16)
    rows = jnp.concatenate(
        [dott(second_ref[0, l], wide) + dott(second_ref[1, l], wide) for l in range(2)], axis=1
    )
    upper, lower = split(rows)
    partial = jnp.concatenate(
        [
            dotf(first_tab[0][l], upper) + dotf(first_tab[0][l], lower) + dotf(first_tab[1][l], upper)
            for l in range(2)
        ],
        axis=1,
    )
    s_msg[...] = partial.astype(BF16).reshape(8, 16, 128)

    third = start(2, lines, lambda p: s_msg.at[p], r3)
    r3[me_x] = s_msg[me_x]
    finish(weights)
    for h in range(8):
        parts = [
            rw[e * 8 + h, 8 * p : 8 * p + 8, :].astype(F32) for p in range(4) for e in range(4)
        ]
        mixing[h] = jnp.concatenate(parts, axis=0).T.astype(BF16)
    finish(third)
    modes = jnp.sum(r3[...].astype(F32), axis=0)

    own = rows128 // 2 == lanes128 // 2
    even = lax.broadcasted_iota(jnp.int32, (64, 128), 1) % 2 == 0
    products = []
    for h in range(8):
        expanded = jnp.concatenate(
            [
                jnp.where(own, jnp.broadcast_to(modes[2 * h + a : 2 * h + a + 1], (128, 128)), 0.0)
                for a in range(2)
            ],
            axis=0,
        ).astype(BF16)
        products.append(dott(mixing[h], expanded))
    for h, product in enumerate(products):
        mixed_scr[h, 0:64] = product[0:64, 0:128] - product[64:128, 128:256]
        mixed_scr[h, 64:128] = product[64:128, 0:128] + product[0:64, 128:256]
    turned = [
        jnp.where(even, mixed_scr[h, pl.ds(0, 64, stride=2), :], mixed_scr[h, pl.ds(1, 64, stride=2), :])
        for h in range(8)
    ]
    place = lax.broadcasted_iota(jnp.int32, (512, 512), 0)
    source = lax.broadcasted_iota(jnp.int32, (512, 512), 1)
    wanted = ((place >> 1) & 7) * 64 + (place & 1) * 32 + (place >> 4)
    order = jnp.where(wanted == source, 1.0, 0.0).astype(BF16)
    turned = jnp.concatenate(turned, axis=0).astype(BF16)
    n_msg[...] = dotf(order, turned).astype(BF16).reshape(32, 16, 128)

    fourth = start(3, planes, lambda p: n_msg.at[p], r5)
    r5[me_q] = n_msg[me_q]
    finish(fourth)
    mixed = jnp.sum(r5[...].astype(F32), axis=0)
    zero_rows = lax.broadcasted_iota(jnp.int32, (16, 128), 0)
    zero_lanes = lax.broadcasted_iota(jnp.int32, (16, 128), 1)
    mixed = jnp.where((zero_rows < 2) & (zero_lanes < 2) & (me_x == 0), 0.0, mixed)
    g_msg[...] = mixed.astype(BF16)

    fifth = start(4, lines, lambda p: g_msg, r6)
    r6[me_x] = g_msg[...]
    finish(fifth)
    field = r6[...].reshape(128, 128)
    along = (
        dotf(back_tab[0][0], field[:, 0:64])
        + dotf(back_tab[1][0], field[:, 0:64])
        + dotf(back_tab[0][1], field[:, 64:128])
        + dotf(back_tab[1][1], field[:, 64:128])
    )
    upper, lower = split(along.T)
    plane = (
        dotf(upper[0:32], second_ref[0, 0])
        + dotf(lower[0:32], second_ref[0, 0])
        + dotf(upper[0:32], second_ref[1, 0])
        + dotf(upper[32:64], second_ref[0, 1])
        + dotf(lower[32:64], second_ref[0, 1])
        + dotf(upper[32:64], second_ref[1, 1])
    )
    scale = 1.0 / GRID**3
    plane_rows = lax.broadcasted_iota(jnp.int32, (32, 1024), 0)
    plane = (plane * jnp.where(plane_rows < 2, scale, 2.0 * scale)).astype(BF16)
    wide_field = field.astype(F32)
    paired = jnp.zeros((128, 128), F32)
    for p in range(4):
        paired = jnp.where(lanes128 // 32 == p, dotf(pair_ref[p], field), paired)
    low = (lanes128 // 2) % 16 == 0
    power = jnp.where(low, 0.5 * wide_field * (wide_field + paired), 2.0 * wide_field * wide_field)
    power = jnp.sum(power, axis=0, keepdims=True)
    for shift in (64, 32, 16, 8, 4, 2):
        power = power + pltpu.roll(power, shift, 1)
    lane = lax.broadcasted_iota(jnp.int32, (1, 128), 1)
    power = jnp.where(lane % 2 == (lane // 8) % 2, power, pltpu.roll(power, 1, 1))
    variance = jnp.broadcast_to(power, (128, 128)).T * (scale * scale)
    inverse = 1.0 / jnp.sqrt(variance + NORM_FLOOR)
    for e in range(4):
        part = jnp.concatenate(
            [plane[:, (2 * e + b) * 128 : (2 * e + b + 1) * 128] for b in range(2)], axis=0
        )
        branch = (dotf(back_ref[0], part) + dotf(back_ref[1], part)) * inverse
        b_msg[8 * e : 8 * e + 8] = branch.astype(BF16).reshape(8, 16, 128)

    sixth = start(5, planes, lambda p: b_msg.at[p], r8)
    r8[me_q] = b_msg[me_q]
    finish(sixth)
    ended[...] = r8[...].reshape(512, 128).astype(F32)
    for z in range(8):
        out_ref[z] = ended[pl.ds(z, 64, stride=8), :] + skip[z]
    for stage, everything in sends:
        pltpu.make_async_copy(everything, everything, send.at[stage]).wait()


def final_kernel(cells_ref, out_ref):
    for z in range(8):
        out_ref[:, z, :] = gelu(cells_ref[z]).T


def final(cells):
    vmem = pl.BlockSpec(memory_space=pltpu.VMEM)
    return pl.pallas_call(
        final_kernel, out_shape=jax.ShapeDtypeStruct((128, 8, 64), F32), in_specs=[vmem], out_specs=vmem,
        compiler_params=pltpu.CompilerParams(vmem_limit_bytes=LIMIT),
    )(*kept(cells))


def spectral_layer(ordered, rank, skip_t, weight, *tables):
    vmem = pl.BlockSpec(memory_space=pltpu.VMEM)
    own = [pltpu.VMEM(array.shape, array.dtype) for array in (weight,) + tables]
    return pl.pallas_call(
        spectral_kernel,
        out_shape=pltpu.VMEM((8, 64, 128), F32),
        in_specs=[vmem] * 3 + [pl.BlockSpec(memory_space=pltpu.HBM)] * 7,
        out_specs=vmem,
        scratch_shapes=own
        + [
            pltpu.VMEM((512, 128), F32),
            pltpu.VMEM((32, 16, 128), BF16),
            pltpu.VMEM((32, 16, 128), BF16),
            pltpu.VMEM((32, 32, 128), BF16),
            pltpu.VMEM((32, 32, 128), BF16),
            pltpu.VMEM((8, 16, 128), BF16),
            pltpu.VMEM((8, 16, 128), BF16),
            pltpu.VMEM((8, 128, 128), BF16),
            pltpu.VMEM((8, 128, 128), F32),
            pltpu.VMEM((32, 16, 128), BF16),
            pltpu.VMEM((32, 16, 128), BF16),
            pltpu.VMEM((16, 128), BF16),
            pltpu.VMEM((8, 16, 128), BF16),
            pltpu.VMEM((32, 16, 128), BF16),
            pltpu.VMEM((32, 16, 128), BF16),
            pltpu.VMEM((512, 128), F32),
            pltpu.VMEM((8, 64, 128), F32),
            pltpu.SemaphoreType.DMA((6,)),
            pltpu.SemaphoreType.DMA((6,)),
            pltpu.SemaphoreType.DMA((7,)),
        ],
        compiler_params=pltpu.CompilerParams(collective_id=0, has_side_effects=True, vmem_limit_bytes=LIMIT),
    )(*kept(ordered, rank, skip_t), *far(weight, *tables))


def body(point_data, neighbours, counts, kernel_in, kernel_mid, kernel_out, spectral, skip_weight):
    cells_x, cells_y, cells_z = neighbours.shape[1:4]
    *made, rank, first, mid, last, skip_t = halo(
        jnp.transpose(point_data, (1, 0, 2)),
        neighbours.reshape(-1, NB),
        jnp.transpose(counts[0], (0, 2, 1)),
        kernel_in,
        kernel_mid,
        kernel_out.T,
        skip_weight,
    )
    ordered = encode(*made, first, mid, last)
    third = third_table()
    by_place = first_table()
    cells = spectral_layer(
        ordered,
        rank,
        skip_t,
        spectral.reshape(2, 16, 64, 64),
        jnp.asarray(halves(third)),
        jnp.asarray(halves(third.T)),
        jnp.asarray(halves(second_table())),
        jnp.asarray(placed(by_place)),
        jnp.asarray(placed(np.swapaxes(by_place, 2, 3))),
        jnp.asarray(pair_table().astype(ml_dtypes.bfloat16)),
    )
    out = final(cells)
    return out.reshape(1, cells_x, cells_y, cells_z, -1)


def solution(mesh):
    in_specs = (
        P(None, None, ("gx", "gy", "gz")),
        P(None, "gx", "gy", "gz", None),
        P(None, "gx", "gy", "gz"),
        P(),
        P(),
        P(),
        P(None, "gz", "gx", "gy", None, None),
        P(),
    )
    out_specs = P(None, "gx", "gy", "gz", None)
    return jax.shard_map(body, mesh=mesh, in_specs=in_specs, out_specs=out_specs, check_vma=False)
```

```python
import functools
import math

import jax
import jax.numpy as jnp
import ml_dtypes
import numpy as np
from jax import lax
from jax.experimental import pallas as pl
from jax.experimental.pallas import tpu as pltpu
from jax.sharding import PartitionSpec as P

GRID = 64
LIMIT = 24 * 2**20
MODES = 16
NB = 32
NORM_FLOOR = 1.0
GX, GY, GZ = 8, 4, 8
F32 = jnp.float32
BF16 = jnp.bfloat16
MESH = pl.DeviceIdType.MESH


def gelu(v):
    inner = v * (0.7978845608028654 + 0.035677408136300125 * (v * v))
    half = 0.5 * v
    return half + half * jnp.tanh(inner)


def twice_gelu(v):
    if not GELU16:
        return v + v * jnp.tanh(v * (0.7978845608028654 + 0.035677408136300125 * (v * v)))
    v = v.astype(BF16)
    inner = v * (BF16(0.7978845608028654) + BF16(0.035677408136300125) * (v * v))
    return v + v * jnp.tanh(inner)


SLOTS = 4
ROWS = 176
FOUR, SIX = 108, 162
GELU16 = True
OFFSETS = [(dx, dy, dz) for dx in (-1, 0, 1) for dy in (-1, 0, 1) for dz in (-1, 0, 1)]


def kept(*arrays):
    return [pltpu.with_memory_space_constraint(array, pltpu.VMEM) for array in arrays]


def far(*arrays):
    return [pltpu.with_memory_space_constraint(array, pltpu.HBM) for array in arrays]


def regroup():
    row = lax.broadcasted_iota(jnp.int32, (512, 512), 0)
    column = lax.broadcasted_iota(jnp.int32, (512, 512), 1)
    wanted = ((row >> 1) & 7) * 64 + (row >> 4) * 2 + (row & 1)
    return jnp.where(wanted == column, 1.0, 0.0).astype(BF16)


def halo_kernel(
    points_any, near_any, counts_any, in_any, mid_any, last_any, skip_any,
    table_ref, slots_ref, blocks_ref, info_ref, rank_ref, first_out, mid_out, last_out, skip_out,
    points_ref, near_ref, counts_ref, in_ref, mid_ref, skip_ref, main, send, recv, loaded,
):
    me_x = lax.axis_index("gx")
    me_y = lax.axis_index("gy")
    me_z = lax.axis_index("gz")

    def device(offset):
        dx, dy, dz = offset
        return {
            "gx": lax.rem(me_x + dx + GX, GX),
            "gy": lax.rem(me_y + dy + GY, GY),
            "gz": lax.rem(me_z + dz + GZ, GZ),
        }

    barrier = pltpu.get_barrier_semaphore()
    peers = [o for o in OFFSETS if o != (0, 0, 0)]
    for offset in peers:
        pl.semaphore_signal(barrier, inc=1, device_id=device(offset), device_id_type=MESH)
    moves = (
        (points_any, points_ref), (counts_any, counts_ref), (near_any, near_ref), (in_any, in_ref),
        (mid_any, mid_ref), (last_any, last_out), (skip_any, skip_ref),
    )
    loads = [pltpu.make_async_copy(c, d, loaded.at[n]) for n, (c, d) in enumerate(moves)]
    for load in loads:
        load.start()
    loads[0].wait()

    main[13] = jnp.concatenate([points_ref[d] for d in range(6)] + [jnp.zeros((2, 512), F32)], axis=0).astype(BF16)
    pl.semaphore_wait(barrier, len(peers))
    for offset in sorted(peers, key=lambda o: -sum(abs(d) for d in o)):
        slot = 26 - OFFSETS.index(offset)
        pltpu.make_async_remote_copy(
            src_ref=main.at[13],
            dst_ref=main.at[slot],
            send_sem=send.at[0],
            recv_sem=recv.at[0],
            device_id=device(offset),
            device_id_type=MESH,
        ).start()
    everything = main.at[pl.ds(0, 26)]

    for load in loads[1:]:
        load.wait()
    lane = lax.broadcasted_iota(jnp.int32, (1, 1024), 1)
    counts = jnp.concatenate([counts_ref[x].astype(F32) for x in range(8)], axis=1)
    counts = jnp.concatenate([counts[z : z + 1] for z in range(8)], axis=1)
    key = counts * 1024.0 + (1023 - lane).astype(F32)
    ones = jnp.ones((8, 128), BF16)
    rank = jnp.zeros((8, 1024), F32)
    for m in range(8):
        tall = jnp.broadcast_to(key[:, 128 * m : 128 * m + 128], (128, 128)).T
        ahead = jnp.concatenate(
            [
                jnp.where(tall > key[:, 128 * n : 128 * n + 128], 1.0, 0.0).astype(BF16)
                for n in range(8)
            ],
            axis=1,
        )
        rank = rank + jnp.dot(ones, ahead, preferred_element_type=F32)
    rank_ref[...] = rank
    near = jnp.concatenate(
        [near_ref[pl.ds(z, 128, stride=8), :].astype(F32).T for z in range(8)], axis=1
    ).astype(jnp.int32)
    owner = near >> 9
    part = near & 511
    block = ((((owner >> 5) - me_x + 1) * 3) + ((owner >> 3) & 3) - me_y + 1) * 3 + (owner & 7) - me_z + 1
    code = jnp.clip(block, 0, 26) * 2 + (part >> 8)
    place_y = (me_y * 16 + (lane & 15)).astype(F32)
    place_x = (me_x * 8 + ((lane >> 4) & 7)).astype(F32)
    place_z = (me_z * 8 + (lane >> 7)).astype(F32)
    centres = [-(place + 0.5) / GRID for place in (place_x, place_y, place_z)]
    rows = jnp.concatenate(
        [(part & 255).astype(F32), code.astype(F32), counts] + centres + [jnp.zeros((12, 1024), F32)], axis=0
    ).astype(BF16)
    order = lax.broadcasted_iota(jnp.int32, (128, 1024), 0).astype(F32)
    wide_rank = rank[0:1]
    for t in range(8):
        moved = jnp.where(order + 128.0 * t == wide_rank, 1.0, 0.0).astype(BF16)
        moved = lax.dot_general(rows, moved, (((1,), (1,)), ((), ())), preferred_element_type=F32)
        slots_ref[t] = moved[0:32].astype(jnp.int32)
        blocks_ref[t] = moved[32:64].astype(jnp.int32)
        info_ref[t] = moved[64:72]

    column = lax.broadcasted_iota(jnp.int32, (6, ROWS), 1)
    feature = lax.broadcasted_iota(jnp.int32, (6, ROWS), 0)
    wanted = jnp.where(column < FOUR, column % 4, 4 + column % 2)
    wanted = jnp.where(column >= SIX, column - SIX, wanted)
    chosen = jnp.where((feature == wanted) & (column < SIX + 3), 1.0, 0.0).astype(BF16)
    turn = (((0,), (0,)), ((), ()))
    first_out[...] = lax.dot_general(in_ref[...], chosen, turn, preferred_element_type=F32).astype(BF16)
    half_mid = (mid_ref[...].astype(F32).T * 0.5).astype(BF16)
    mid_out[...] = jnp.zeros(mid_out.shape, BF16)
    mid_out[0:80, 0:80] = half_mid
    mid_out[80:160, 80:160] = half_mid

    skip_out[...] = skip_ref[...].astype(F32).T.astype(BF16)

    pltpu.make_async_copy(everything, everything, recv.at[0]).wait()
    blocks = [main[b].astype(F32) for b in range(27)]
    rows = [block[0:4] for block in blocks] + [block[4:6] for block in blocks]
    rows.append(jnp.zeros((ROWS - SIX, 512), F32))
    rows = jnp.concatenate(rows, axis=0).astype(BF16)
    table_ref[0:ROWS, :] = rows[:, 0:256]
    table_ref[ROWS : 2 * ROWS, :] = rows[:, 256:512]
    pltpu.make_async_copy(everything, everything, send.at[0]).wait()


def halo(points, near, counts, kernel_in, kernel_mid, last, skip_w):
    vmem = pl.BlockSpec(memory_space=pltpu.VMEM)
    return pl.pallas_call(
        halo_kernel,
        out_shape=[
            pltpu.VMEM((2 * ROWS, 256), BF16),
            pltpu.VMEM((8, NB, 128), jnp.int32),
            pltpu.VMEM((8, NB, 128), jnp.int32),
            pltpu.VMEM((8, 8, 128), F32),
            pltpu.VMEM((8, 1024), F32),
            pltpu.VMEM((80, ROWS), BF16),
            pltpu.VMEM((160, 160), BF16),
            pltpu.VMEM((64, 80), BF16),
            pltpu.VMEM((64, 64), BF16),
        ],
        in_specs=[pl.BlockSpec(memory_space=pl.ANY)] * 7,
        out_specs=[vmem] * 9,
        scratch_shapes=[
            pltpu.VMEM(points.shape, F32),
            pltpu.VMEM(near.shape, jnp.int32),
            pltpu.VMEM(counts.shape, jnp.int32),
            pltpu.VMEM(kernel_in.shape, BF16),
            pltpu.VMEM(kernel_mid.shape, BF16),
            pltpu.VMEM(skip_w.shape, BF16),
            pltpu.VMEM((27, 8, 512), BF16),
            pltpu.SemaphoreType.DMA((1,)),
            pltpu.SemaphoreType.DMA((1,)),
            pltpu.SemaphoreType.DMA((7,)),
        ],
        compiler_params=pltpu.CompilerParams(collective_id=1, has_side_effects=True, vmem_limit_bytes=LIMIT),
    )(*far(points, near, counts, kernel_in, kernel_mid, last, skip_w))


def encoder_kernel(
    table_ref, slots_ref, blocks_ref, info_ref, first_scr, mid_scr, last_scr, out_ref,
    kept_scr, hidden_scr, base_scr, totals, trips,
):
    slot_ids = lax.broadcasted_iota(jnp.int32, (256, 128), 0).astype(jnp.int16)
    row = lax.broadcasted_iota(jnp.int32, (ROWS, 128), 0)
    row_block = jnp.where(row < FOUR, row // 4, jnp.where(row < SIX, (row - FOUR) // 2, -1)).astype(jnp.int16)
    last_rows = lax.broadcasted_iota(jnp.int32, (16, 128), 0)
    steps = 0
    for c in range(8):
        info = info_ref[c]
        trip = (jnp.max(info[0:1]).astype(jnp.int32) + SLOTS - 1) // SLOTS
        trips[c] = trip
        steps += trip
        centre = jnp.zeros((16, 128), F32)
        for d in range(3):
            centre = jnp.where(last_rows == SIX - ROWS + 16 + d, info[1 + d : 2 + d], centre)
        base_scr[c] = centre.astype(BF16)
        totals[c] = jnp.zeros((80, 128), F32)
    totals[8] = jnp.zeros((80, 128), F32)
    kept_scr[...] = jnp.zeros(kept_scr.shape, BF16)
    hidden_scr[...] = jnp.zeros(hidden_scr.shape, BF16)

    def step(n, places):
        (c0, t0), (c1, t1), (c2, t2) = places
        hidden = twice_gelu(jnp.dot(mid_scr[...], hidden_scr[...], preferred_element_type=F32))
        counts = info_ref[jnp.minimum(c2, 7), 0:1, :]
        total = totals[c2]
        for u in range(SLOTS):
            used = (SLOTS * t2 + u).astype(F32) < counts
            here = hidden[80 * (u // 2) : 80 * (u // 2) + 80, 128 * (u % 2) : 128 * (u % 2) + 128]
            total = total + jnp.where(used, here.astype(F32), 0.0)
        totals[c2] = total
        hidden = jnp.dot(first_scr[...], kept_scr[...], preferred_element_type=F32)
        hidden = twice_gelu(hidden).astype(BF16)
        for u in range(SLOTS // 2):
            hidden_scr[80 * u : 80 * u + 80, :] = hidden[:, 256 * u : 256 * u + 256]
        hot = []
        for u in range(SLOTS):
            slot = jnp.broadcast_to(slots_ref[c0, pl.ds(SLOTS * t0 + u, 1), :], (16, 128)).astype(jnp.int16)
            slot = jnp.concatenate([slot] * 16, axis=0)
            hot.append(jnp.where(slot_ids == slot, BF16(1), BF16(0)))
        found = jnp.dot(table_ref[...], jnp.concatenate(hot, axis=1), preferred_element_type=F32)
        found = found.astype(BF16)
        for u in range(SLOTS):
            code = jnp.broadcast_to(blocks_ref[c0, pl.ds(SLOTS * t0 + u, 1), :], (16, 128))
            block = (code >> 1).astype(jnp.int16)
            odd = (code & 1).astype(jnp.int16)
            same = row_block == jnp.concatenate([block] * (ROWS // 16), axis=0)
            odd = jnp.concatenate([odd] * (ROWS // 16), axis=0) == 1
            here = found[:, 128 * u : 128 * u + 128]
            here = jnp.where(odd, here[ROWS : 2 * ROWS], here[0:ROWS])
            kept_scr[0 : ROWS - 16, 128 * u : 128 * u + 128] = jnp.where(same[0 : ROWS - 16], here[0 : ROWS - 16], BF16(0))
            kept_scr[ROWS - 16 : ROWS, 128 * u : 128 * u + 128] = jnp.where(same[ROWS - 16 : ROWS], here[ROWS - 16 : ROWS], base_scr[c0])
        ended = t0 + 1 >= trips[c0]
        following = (
            jnp.minimum(jnp.where(ended, c0 + 1, c0), 7),
            jnp.where(ended, jnp.where(c0 == 7, t0, 0), t0 + 1),
        )
        return following, (c0, t0), (c1, t1)

    start = (jnp.int32(0), jnp.int32(0))
    spare = (jnp.int32(8), jnp.int32(0))
    lax.fori_loop(0, steps + 2, step, (start, spare, spare))
    last = last_scr[...]
    ordered = []
    for c in range(8):
        mean = totals[c] * (0.5 / info_ref[c, 0:1, :])
        upper = mean.astype(BF16)
        lower = (mean - upper.astype(F32)).astype(BF16)
        values = jnp.dot(last, upper, preferred_element_type=F32) + jnp.dot(
            last, lower, preferred_element_type=F32
        )
        ordered.append(values.astype(BF16))
    out_ref[...] = jnp.concatenate(ordered, axis=1)


def encode(*made):
    vmem = pl.BlockSpec(memory_space=pltpu.VMEM)
    return pl.pallas_call(
        encoder_kernel,
        out_shape=pltpu.VMEM((64, 1024), BF16),
        in_specs=[vmem] * 7,
        out_specs=vmem,
        scratch_shapes=[
            pltpu.VMEM((ROWS, 128 * SLOTS), BF16),
            pltpu.VMEM((160, 256), BF16),
            pltpu.VMEM((8, 16, 128), BF16),
            pltpu.VMEM((9, 80, 128), F32),
            pltpu.SMEM((8,), jnp.int32),
        ],
        compiler_params=pltpu.CompilerParams(vmem_limit_bytes=LIMIT),
    )(*kept(*made))


def halves(values):
    upper = values.astype(np.float32).astype(ml_dtypes.bfloat16)
    lower = (values - upper.astype(np.float64)).astype(np.float32).astype(ml_dtypes.bfloat16)
    return np.stack([upper, lower])


def turn(frequency, position):
    angle = 2.0 * math.pi * ((frequency * position) % GRID) / GRID
    return np.cos(angle), np.sin(angle)


def centred(index):
    return np.where(index < MODES // 2, index, index - MODES)


def complex_block(cos, sin):
    return np.stack([np.stack([cos, sin], -1), np.stack([-sin, cos], -1)], -2)


@functools.lru_cache(None)
def third_table():
    cos, sin = turn(np.arange(16)[:, None], np.arange(64)[None, :])
    parts = np.stack([cos, -sin]).reshape(2, 16, 8, 8)
    full = np.einsum("akgz,cd->akcgdz", parts, np.eye(2))
    return full.reshape(64, 128)


@functools.lru_cache(None)
def second_table():
    j = np.arange(16)
    cos, sin = turn(centred(j)[:, None], np.arange(64)[None, :])
    both = complex_block(cos, sin).reshape(8, 2, 4, 16, 2, 2)
    full = np.einsum("gleyab,xw->lgaxebwy", both, np.eye(8))
    return full.reshape(2, 128, 1024)


@functools.lru_cache(None)
def first_table():
    i = np.arange(16)
    cos, sin = turn(centred(i)[:, None], np.arange(64)[None, :])
    both = complex_block(cos, sin).reshape(8, 2, 8, 8, 2, 2)
    return np.einsum("hltxab->tlhabx", both).reshape(8, 2, 16, 16)


def placed(values):
    return np.tile(np.moveaxis(halves(values), 0, 1), (1, 1, 1, 1, 8))


@functools.lru_cache(None)
def pair_table():
    out = np.zeros((4, 8, 8, 2, 8, 8, 2))
    for il in range(2):
        for jl in range(2):
            for h in range(8):
                for g in range(8):
                    i, j = 2 * h + il, 2 * g + jl
                    if i == 8 or j == 8:
                        continue
                    ni, nj = (16 - i) % 16, (16 - j) % 16
                    assert ni % 2 == il and nj % 2 == jl
                    for a in range(2):
                        out[2 * il + jl, g, h, a, nj // 2, ni // 2, a] = 1.0 - 2.0 * a
    return out.reshape(4, 128, 128)


def dotf(a, b):
    return jnp.dot(a, b, preferred_element_type=F32)


def dott(a, b):
    return lax.dot_general(a, b, (((1,), (1,)), ((), ())), preferred_element_type=F32)


def split(values):
    upper = values.astype(BF16)
    return upper, (values - upper.astype(F32)).astype(BF16)


def spectral_kernel(
    ordered_ref, rank_ref, skip_ref, weight_any, third_any, back_any, second_any, first_any, firstt_any, pair_any,
    out_ref,
    weight_ref, third_ref, back_ref, second_ref, first_ref, firstt_ref, pair_ref,
    latent, l_msg, r1, w_msg, rw, s_msg, r3, mixing, mixed_scr, n_msg, r5, g_msg, r6, b_msg, r8, ended, skip,
    send, recv, loaded,
):
    me_x = lax.axis_index("gx")
    me_y = lax.axis_index("gy")
    me_z = lax.axis_index("gz")
    me_q = me_y * GZ + me_z
    columns = [(y, z) for y in range(GY) for z in range(GZ) if y or z]
    columns.sort(key=lambda o: -(2 * min(o[0], GY - o[0]) + min(o[1], GZ - o[1])))

    def across(o):
        y, z = lax.rem(me_y + o[0], GY), lax.rem(me_z + o[1], GZ)
        return {"gy": y, "gz": z}, y * GZ + z, me_q

    def along_x(o):
        peer = lax.rem(me_x + o, GX)
        return {"gx": peer}, peer, me_x

    planes = [across(o) for o in columns]
    lines = [along_x(o) for o in (4, 3, 5, 2, 6, 1, 7)]
    barrier = pltpu.get_barrier_semaphore()
    for device, _, _ in lines + planes:
        pl.semaphore_signal(barrier, inc=1, device_id=device, device_id_type=MESH)
    constants = (weight_any, third_any, back_any, second_any, first_any, firstt_any, pair_any)
    copies = (weight_ref, third_ref, back_ref, second_ref, first_ref, firstt_ref, pair_ref)
    loads = [pltpu.make_async_copy(c, d, loaded.at[n]) for n, (c, d) in enumerate(zip(constants, copies))]
    for load in loads:
        load.start()
    order = lax.broadcasted_iota(jnp.int32, (1024, 128), 0).astype(F32)
    for z in range(8):
        moved = jnp.where(order == rank_ref[0:1, 128 * z : 128 * z + 128], 1.0, 0.0).astype(BF16)
        latent[64 * z : 64 * z + 64] = dotf(ordered_ref[...], moved)
    for q in range(32):
        both = [latent[pl.ds(2 * q + c, 8, stride=64), :] for c in range(2)]
        l_msg[q] = jnp.concatenate(both, axis=0).astype(BF16)
    pl.semaphore_wait(barrier, len(planes + lines))

    sends = []

    def start(stage, peers, source, target):
        for device, peer, me in peers:
            pltpu.make_async_remote_copy(
                src_ref=source(peer),
                dst_ref=target.at[me],
                send_sem=send.at[stage],
                recv_sem=recv.at[stage],
                device_id=device,
                device_id_type=MESH,
            ).start()
        everything = target.at[pl.ds(0, len(peers))]
        sends.append((stage, everything))
        return stage, everything

    def finish(pending):
        stage, everything = pending
        pltpu.make_async_copy(everything, everything, recv.at[stage]).wait()

    rows128 = lax.broadcasted_iota(jnp.int32, (128, 128), 0)
    lanes128 = lax.broadcasted_iota(jnp.int32, (128, 128), 1)
    same = rows128 // 16 == lanes128 // 16

    def spread_blocks(ref, part, l):
        small = ref[me_x, part, l].astype(F32)
        return jnp.where(same, jnp.concatenate([small] * 8, axis=0), 0.0).astype(BF16)

    first = start(0, planes, lambda p: l_msg.at[p], r1)
    r1[me_q] = l_msg[me_q]
    loads[0].wait()
    forth = regroup()
    for l in range(2):
        wide = jnp.concatenate(
            [weight_ref[b, 8 * l : 8 * l + 8].astype(F32).reshape(512, 64) for b in range(2)], axis=1
        ).astype(BF16)
        w_msg[:, 16 * l : 16 * l + 16, :] = dotf(forth, wide).astype(BF16).reshape(32, 16, 128)
    weights = start(1, planes, lambda p: w_msg.at[p], rw)
    rw[me_q] = w_msg[me_q]
    for load in loads[1:]:
        load.wait()
    first_tab = [[spread_blocks(first_ref, p, l) for l in range(2)] for p in range(2)]
    back_tab = [[spread_blocks(firstt_ref, p, l) for l in range(2)] for p in range(2)]
    for z in range(8):
        skip[z] = dotf(skip_ref[...], latent[64 * z : 64 * z + 64].astype(BF16))
    finish(first)

    pieces = []
    for e in range(4):
        values = r1[8 * e : 8 * e + 8].reshape(128, 128)
        piece = dotf(third_ref[0], values) + dotf(third_ref[1], values)
        pieces += [piece[0:32], piece[32:64]]
    wide = jnp.concatenate(pieces, axis=1).astype(BF16)
    rows = jnp.concatenate(
        [dott(second_ref[0, l], wide) + dott(second_ref[1, l], wide) for l in range(2)], axis=1
    )
    upper, lower = split(rows)
    partial = jnp.concatenate(
        [
            dotf(first_tab[0][l], upper) + dotf(first_tab[0][l], lower) + dotf(first_tab[1][l], upper)
            for l in range(2)
        ],
        axis=1,
    )
    s_msg[...] = partial.astype(BF16).reshape(8, 16, 128)

    third = start(2, lines, lambda p: s_msg.at[p], r3)
    r3[me_x] = s_msg[me_x]
    finish(weights)
    for h in range(8):
        parts = [
            rw[e * 8 + h, 8 * p : 8 * p + 8, :].astype(F32) for p in range(4) for e in range(4)
        ]
        mixing[h] = jnp.concatenate(parts, axis=0).T.astype(BF16)
    finish(third)
    modes = jnp.sum(r3[...].astype(F32), axis=0)

    own = rows128 // 2 == lanes128 // 2
    even = lax.broadcasted_iota(jnp.int32, (64, 128), 1) % 2 == 0
    products = []
    for h in range(8):
        expanded = jnp.concatenate(
            [
                jnp.where(own, jnp.broadcast_to(modes[2 * h + a : 2 * h + a + 1], (128, 128)), 0.0)
                for a in range(2)
            ],
            axis=0,
        ).astype(BF16)
        products.append(dott(mixing[h], expanded))
    for h, product in enumerate(products):
        mixed_scr[h, 0:64] = product[0:64, 0:128] - product[64:128, 128:256]
        mixed_scr[h, 64:128] = product[64:128, 0:128] + product[0:64, 128:256]
    turned = [
        jnp.where(even, mixed_scr[h, pl.ds(0, 64, stride=2), :], mixed_scr[h, pl.ds(1, 64, stride=2), :])
        for h in range(8)
    ]
    place = lax.broadcasted_iota(jnp.int32, (512, 512), 0)
    source = lax.broadcasted_iota(jnp.int32, (512, 512), 1)
    wanted = ((place >> 1) & 7) * 64 + (place & 1) * 32 + (place >> 4)
    order = jnp.where(wanted == source, 1.0, 0.0).astype(BF16)
    turned = jnp.concatenate(turned, axis=0).astype(BF16)
    n_msg[...] = dotf(order, turned).astype(BF16).reshape(32, 16, 128)

    fourth = start(3, planes, lambda p: n_msg.at[p], r5)
    r5[me_q] = n_msg[me_q]
    finish(fourth)
    mixed = jnp.sum(r5[...].astype(F32), axis=0)
    zero_rows = lax.broadcasted_iota(jnp.int32, (16, 128), 0)
    zero_lanes = lax.broadcasted_iota(jnp.int32, (16, 128), 1)
    mixed = jnp.where((zero_rows < 2) & (zero_lanes < 2) & (me_x == 0), 0.0, mixed)
    g_msg[...] = mixed.astype(BF16)

    fifth = start(4, lines, lambda p: g_msg, r6)
    r6[me_x] = g_msg[...]
    finish(fifth)
    field = r6[...].reshape(128, 128)
    along = (
        dotf(back_tab[0][0], field[:, 0:64])
        + dotf(back_tab[1][0], field[:, 0:64])
        + dotf(back_tab[0][1], field[:, 64:128])
        + dotf(back_tab[1][1], field[:, 64:128])
    )
    upper, lower = split(along.T)
    plane = (
        dotf(upper[0:32], second_ref[0, 0])
        + dotf(lower[0:32], second_ref[0, 0])
        + dotf(upper[0:32], second_ref[1, 0])
        + dotf(upper[32:64], second_ref[0, 1])
        + dotf(lower[32:64], second_ref[0, 1])
        + dotf(upper[32:64], second_ref[1, 1])
    )
    scale = 1.0 / GRID**3
    plane_rows = lax.broadcasted_iota(jnp.int32, (32, 1024), 0)
    plane = (plane * jnp.where(plane_rows < 2, scale, 2.0 * scale)).astype(BF16)
    wide_field = field.astype(F32)
    paired = jnp.zeros((128, 128), F32)
    for p in range(4):
        paired = jnp.where(lanes128 // 32 == p, dotf(pair_ref[p], field), paired)
    low = (lanes128 // 2) % 16 == 0
    power = jnp.where(low, 0.5 * wide_field * (wide_field + paired), 2.0 * wide_field * wide_field)
    power = jnp.sum(power, axis=0, keepdims=True)
    chosen = jnp.where(lanes128 % 2 == (rows128 // 8) % 2, 1.0, 0.0).astype(BF16)
    high, low_part = split(jnp.broadcast_to(power, (128, 128)))
    variance = (dott(chosen, high) + dott(chosen, low_part)) * (scale * scale)
    inverse = 1.0 / jnp.sqrt(variance + NORM_FLOOR)
    for e in range(4):
        part = jnp.concatenate(
            [plane[:, (2 * e + b) * 128 : (2 * e + b + 1) * 128] for b in range(2)], axis=0
        )
        branch = (dotf(back_ref[0], part) + dotf(back_ref[1], part)) * inverse
        b_msg[8 * e : 8 * e + 8] = branch.astype(BF16).reshape(8, 16, 128)

    sixth = start(5, planes, lambda p: b_msg.at[p], r8)
    r8[me_q] = b_msg[me_q]
    finish(sixth)
    ended[...] = r8[...].reshape(512, 128).astype(F32)
    for z in range(8):
        out_ref[z] = ended[pl.ds(z, 64, stride=8), :] + skip[z]
    for stage, everything in sends:
        pltpu.make_async_copy(everything, everything, send.at[stage]).wait()


def final_kernel(cells_ref, out_ref):
    for z in range(8):
        out_ref[:, z, :] = gelu(cells_ref[z]).T


def final(cells):
    vmem = pl.BlockSpec(memory_space=pltpu.VMEM)
    return pl.pallas_call(
        final_kernel, out_shape=jax.ShapeDtypeStruct((128, 8, 64), F32), in_specs=[vmem], out_specs=vmem,
        compiler_params=pltpu.CompilerParams(vmem_limit_bytes=LIMIT),
    )(*kept(cells))


def spectral_layer(ordered, rank, skip_t, weight, *tables):
    vmem = pl.BlockSpec(memory_space=pltpu.VMEM)
    own = [pltpu.VMEM(array.shape, array.dtype) for array in (weight,) + tables]
    return pl.pallas_call(
        spectral_kernel,
        out_shape=pltpu.VMEM((8, 64, 128), F32),
        in_specs=[vmem] * 3 + [pl.BlockSpec(memory_space=pltpu.HBM)] * 7,
        out_specs=vmem,
        scratch_shapes=own
        + [
            pltpu.VMEM((512, 128), F32),
            pltpu.VMEM((32, 16, 128), BF16),
            pltpu.VMEM((32, 16, 128), BF16),
            pltpu.VMEM((32, 32, 128), BF16),
            pltpu.VMEM((32, 32, 128), BF16),
            pltpu.VMEM((8, 16, 128), BF16),
            pltpu.VMEM((8, 16, 128), BF16),
            pltpu.VMEM((8, 128, 128), BF16),
            pltpu.VMEM((8, 128, 128), F32),
            pltpu.VMEM((32, 16, 128), BF16),
            pltpu.VMEM((32, 16, 128), BF16),
            pltpu.VMEM((16, 128), BF16),
            pltpu.VMEM((8, 16, 128), BF16),
            pltpu.VMEM((32, 16, 128), BF16),
            pltpu.VMEM((32, 16, 128), BF16),
            pltpu.VMEM((512, 128), F32),
            pltpu.VMEM((8, 64, 128), F32),
            pltpu.SemaphoreType.DMA((6,)),
            pltpu.SemaphoreType.DMA((6,)),
            pltpu.SemaphoreType.DMA((7,)),
        ],
        compiler_params=pltpu.CompilerParams(collective_id=0, has_side_effects=True, vmem_limit_bytes=LIMIT),
    )(*kept(ordered, rank, skip_t), *far(weight, *tables))


def body(point_data, neighbours, counts, kernel_in, kernel_mid, kernel_out, spectral, skip_weight):
    cells_x, cells_y, cells_z = neighbours.shape[1:4]
    *made, rank, first, mid, last, skip_t = halo(
        jnp.transpose(point_data, (1, 0, 2)),
        neighbours.reshape(-1, NB),
        jnp.transpose(counts[0], (0, 2, 1)),
        kernel_in,
        kernel_mid,
        kernel_out.T,
        skip_weight,
    )
    ordered = encode(*made, first, mid, last)
    third = third_table()
    by_place = first_table()
    cells = spectral_layer(
        ordered,
        rank,
        skip_t,
        spectral.reshape(2, 16, 64, 64),
        jnp.asarray(halves(third)),
        jnp.asarray(halves(third.T)),
        jnp.asarray(halves(second_table())),
        jnp.asarray(placed(by_place)),
        jnp.asarray(placed(np.swapaxes(by_place, 2, 3))),
        jnp.asarray(pair_table().astype(ml_dtypes.bfloat16)),
    )
    out = final(cells)
    return out.reshape(1, cells_x, cells_y, cells_z, -1)


def solution(mesh):
    in_specs = (
        P(None, None, ("gx", "gy", "gz")),
        P(None, "gx", "gy", "gz", None),
        P(None, "gx", "gy", "gz"),
        P(),
        P(),
        P(),
        P(None, "gz", "gx", "gy", None, None),
        P(),
    )
    out_specs = P(None, "gx", "gy", "gz", None)
    return jax.shard_map(body, mesh=mesh, in_specs=in_specs, out_specs=out_specs, check_vma=False)
```
